128 devices in a mesh: dp: 1, dcp: 128 (over z, y, x, core).
Axes of the slice: x: 4, y: 4, z: 4, core: 2. Of those that a mesh axis runs over, the one named last changes fastest.
Arguments:
- q: bfloat16 [32, 128, 576], P('dp', 'dcp')
- cache: bfloat16 [32, 32, 128, 8, 576], P('dp', None, 'dcp')
- lens: int32 [32], P('dp')
Outputs:
- output: bfloat16 [32, 128, 512], P('dp', 'dcp')
All inputs are finite; a program needn't handle non-finite values.
Results may differ from the reference program's by a relative error of at most 0.00544788.
Values are sent between devices in bfloat16 or wider.
A program may use at most 1 GiB of HBM per device.

```python
import jax
import jax.numpy as jnp
from jax import lax

B = 32
S = 32768
PAGE = 8
DCP = 128
HEADS = 128
LORA = 512
ROPE = 64
NOPE = 128

R = S // (PAGE * DCP)
K = LORA + ROPE


def setup_inputs(seed: int = 0, part: int = 0) -> dict:
    key = jax.random.fold_in(jax.random.key(seed), part)
    kq, kc, kl = jax.random.split(key, 3)
    qs = 1.5 * ((NOPE + ROPE) / 2.0) ** 0.5
    scale = jnp.concatenate([jnp.full((LORA,), qs / LORA ** 0.5, jnp.float32), jnp.full((ROPE,), qs / ROPE ** 0.5, jnp.float32)])
    q = (jax.random.normal(kq, (B, HEADS, K), jnp.float32) * scale).astype(jnp.bfloat16)
    cache = jax.random.normal(kc, (B, R, DCP, PAGE, K), jnp.float32).astype(jnp.bfloat16)
    lens = jax.random.randint(kl, (B,), S // 4, S + 1, jnp.int32)
    return {'q': q, 'cache': cache, 'lens': lens}


def reference(q, cache, lens):
    c = cache.reshape(B, S, K)
    pos = jnp.arange(S)

    def one(args):
        qb, cb, lb = args
        s = jnp.dot(qb, cb.T, preferred_element_type=jnp.float32) / (NOPE + ROPE) ** 0.5
        s = jnp.where(pos[None, :] < lb, s, -jnp.inf)
        a = jax.nn.softmax(s, axis=1)
        o = jnp.dot(a, cb[:, :LORA].astype(jnp.float32), preferred_element_type=jnp.float32)
        return o.astype(jnp.bfloat16)

    return lax.map(one, (q, c, lens))
```

```python
import functools
import math

import jax
import jax.numpy as jnp
from jax import lax
from jax.experimental import pallas as pl
from jax.experimental.pallas import tpu as pltpu
from jax.sharding import PartitionSpec as P

ROPE = 64
QK_DIM = 192
SCALE2 = QK_DIM ** -0.5 * math.log2(math.e)
NEG = -3.0e38
MESH = pl.DeviceIdType.MESH
F32 = jnp.float32
BF16 = jnp.bfloat16

STRIDE = (2, 8, 32)
ORDERS = ((0, 1, 2), (1, 2, 0), (2, 0, 1))
COUNT = (6, 5, 5)
NI = 6


LAT, QW, LANES = 512, 576, 128
KS, DIRS, RING, RING_OFFS, LINE_OFFS = range(3), range(2), range(4), range(1, 4), range(1, 8)


def _perm(rows, cols, f):
    r = lax.broadcasted_iota(jnp.int32, (rows, cols), 0)
    c = lax.broadcasted_iota(jnp.int32, (rows, cols), 1)
    return f(r, c).astype(F32).astype(BF16)


def _merge_weights(lses):
    top = functools.reduce(jnp.maximum, lses)
    ws = [jnp.exp2(v - top) for v in lses]
    tot = functools.reduce(jnp.add, ws)
    inv = 1.0 / tot
    return [w * inv for w in ws], top + jnp.log2(tot)


def _kernel(lens, q_h, c_h, o_h,
            q_in, s1src, s1buf, q_all, cbuf, obuf, lrow, lcol,
            r1o, r1ol, mrg, mlse, r1d, r1dl, r1m, lse1,
            r2d, r2l, s3src, s3l, r3d, r3l, oout,
            sem_q, sem_c, sem_ps, sem_pr, s1s, s1r, s2s, s2r, s3s, s3r, sfs, sfr,
            a_s, a_r, al_s, al_r, b_s, b_r, bl_s, bl_r, c_s, c_r, cl_s, cl_r,
            e_s, e_r, el_s, el_r, sem_o):
    d = lax.axis_index('dcp')
    core = d % 2
    co = ((d // 2) % 4, (d // 8) % 4, d // 32)

    def at(axis, pos):
        return {'dcp': d + (pos - co[axis]) * STRIDE[axis]}

    def line(axis, j):
        return {'dcp': d + (j // 2 - co[axis]) * STRIDE[axis] + (j % 2 - core)}

    def rcopy(src, dst, ss, rs, dev):
        return pltpu.make_async_remote_copy(src_ref=src, dst_ref=dst, send_sem=ss, recv_sem=rs,
                                            device_id=dev, device_id_type=MESH)

    def wait_bytes(ref, sem):
        pltpu.make_async_copy(ref, ref, sem).wait()

    load_q = pltpu.make_async_copy(q_h, q_in, sem_q)
    load_q.start()

    def local_cache(s):
        return pltpu.make_async_copy(c_h.at[16 * core + s], cbuf.at[s, pl.ds(32 * core, 32)], sem_c.at[s])

    @pl.loop(0, 16)
    def _(s):
        local_cache(s).start()

    bar = pltpu.get_barrier_semaphore()
    partner = {'dcp': d + 1 - 2 * core}
    pl.semaphore_signal(bar, inc=1, device_id=partner, device_id_type=MESH)
    for a in KS:
        for off in RING_OFFS:
            for c2 in DIRS:
                pl.semaphore_signal(bar, inc=1, device_id=line(a, ((co[a] + off) % 4) * 2 + c2), device_id_type=MESH)

    lrow[...] = jnp.zeros_like(lrow)

    load_q.wait()

    def sel(r, c):
        c2, k, i = r // 24, (r // 8) % 3, r % 8
        s = 3 * i + k
        return (c == 16 * c2 + s) & (s < 16)

    qp = jnp.dot(_perm(48, 32, sel), q_in[...], preferred_element_type=F32).astype(BF16)
    s1src[...] = qp.reshape(2, 3, 8, QW)
    pl.semaphore_wait(bar, 19)

    for k in KS:
        a1 = ORDERS[k][0]
        j0 = co[a1] * 2 + core
        for off in LINE_OFFS:
            j = (j0 + off) % 8
            rcopy(s1src.at[j % 2, k], s1buf.at[k, j0], s1s.at[k, off], s1r.at[k, off], line(a1, j)).start()
        s1buf[k, j0] = s1src[core, k]

    def push_cache(s):
        return rcopy(c_h.at[16 * (1 - core) + s], cbuf.at[s, pl.ds(32 * core, 32)], sem_ps.at[s], sem_pr.at[s], partner)

    def got_cache(s):
        return rcopy(c_h.at[s], cbuf.at[s, pl.ds(32 * (1 - core), 32)], sem_ps.at[s], sem_pr.at[s], partner)

    @pl.loop(0, 16)
    def _(s):
        push_cache(s).start()

    def grp(k, off=0):
        _, a2, a3 = ORDERS[k]
        return co[a3] * 4 + (co[a2] + 4 - off) % 4

    def s2(k, i, off):
        a2 = ORDERS[k][1]
        g = grp(k)
        return rcopy(q_all.at[k, i, g], q_all.at[k, i, g], s2s.at[off - 1], s2r.at[k, i, off - 1],
                     at(a2, (co[a2] + off) % 4))

    def s2_wait(k, i, off):
        g = grp(k, off)
        rcopy(q_all.at[k, i, g], q_all.at[k, i, g], s2s.at[off - 1], s2r.at[k, i, off - 1], partner).wait_recv()

    def s3(k, i, off, dr):
        a3 = ORDERS[k][2]
        g = grp(k, off)
        return rcopy(q_all.at[k, i, g], q_all.at[k, i, g], s3s.at[dr, off], s3r.at[k, i, dr, off],
                     at(a3, (co[a3] + (1 if dr == 0 else 3)) % 4))

    def s3_src(k, off, dr, hops):
        _, a2, a3 = ORDERS[k]
        p3 = (co[a3] + (4 - hops if dr == 0 else hops)) % 4
        return p3 * 4 + (co[a2] + 4 - off) % 4

    def s3_wait(k, i, off, dr):
        g = s3_src(k, off, dr, 1)
        rcopy(q_all.at[k, i, g], q_all.at[k, i, g], s3s.at[dr, off], s3r.at[k, i, dr, off], partner).wait_recv()

    def fwd(k, i, off):
        dr = off // 2
        a3 = ORDERS[k][2]
        g = s3_src(k, off, dr, 1)
        return rcopy(q_all.at[k, i, g], q_all.at[k, i, g], sfs.at[off], sfr.at[k, i, off],
                     at(a3, (co[a3] + (1 if dr == 0 else 3)) % 4))

    def fwd_wait(k, i, off):
        g = s3_src(k, off, off // 2, 2)
        rcopy(q_all.at[k, i, g], q_all.at[k, i, g], sfs.at[off], sfr.at[k, i, off], partner).wait_recv()

    def each(f):
        @pl.loop(0, NI - 1)
        def _(i):
            for k in KS:
                f(k, i)
        f(0, NI - 1)

    tr = _perm(64, 64, lambda r, c: (r // 8 == c % 8) & (r % 8 == c // 8))
    for k in KS:
        a1 = ORDERS[k][0]
        j0 = co[a1] * 2 + core
        for off in LINE_OFFS:
            src = (j0 + 8 - off) % 8
            rcopy(s1src.at[core, k], s1buf.at[k, src], s1s.at[k, off], s1r.at[k, off], partner).wait()
        blk = jnp.dot(tr, s1buf[k].reshape(64, QW), preferred_element_type=F32).astype(BF16).reshape(8, 8, QW)
        g = grp(k)
        for i in range(COUNT[k]):
            q_all[k, i, g] = blk[i]

        @pl.loop(0, COUNT[k])
        def _(i):
            for off in (2, 1, 3):
                s2(k, i, off).start()
            for dr in DIRS:
                s3(k, i, 0, dr).start()

    def stage3(k, i):
        for off in (1, 3, 2):
            s2_wait(k, i, off)
            for dr in DIRS:
                s3(k, i, off, dr).start()

    each(stage3)

    def forward(k, i):
        for off in (0, 1, 3, 2):
            s3_wait(k, i, off, off // 2)
            fwd(k, i, off).start()

    def arrive(k, i):
        s = 3 * i + k
        local_cache(s).wait()
        got_cache(s).wait_recv()
        for off in RING:
            s3_wait(k, i, off, 1 - off // 2)
            fwd_wait(k, i, off)

    chip8 = (d // 2) * 16

    def attend(k, i):
        s = 3 * i + k
        n = lens[16 * core + s]
        cs = cbuf[s].reshape(LAT, QW)
        qs = q_all[k, i].reshape(LANES, QW)
        st = lax.dot_general(cs, qs, (((1,), (1,)), ((), ())), preferred_element_type=F32) * SCALE2
        j = lax.broadcasted_iota(jnp.int32, (LAT, LANES), 0)
        ok = (j & 7) + ((j >> 3) & 31) * 1024 + (j >> 8) * 8 + chip8 < n
        st = jnp.where(ok, st, NEG)
        m = jnp.max(st, axis=0, keepdims=True)
        p = jnp.where(ok, jnp.exp2(st - m), 0.0)
        l = jnp.sum(p, axis=0, keepdims=True)
        has = l > 0.0
        ls = jnp.where(has, l, 1.0)
        pn = (p * (1.0 / ls)).astype(BF16)
        o = lax.dot_general(pn, cs[:, :LAT], (((0,), (0,)), ((), ())), preferred_element_type=F32)
        obuf[k, i] = o.astype(BF16).reshape(16, 8, LAT)
        lrow[k, pl.ds(i, 1), :] = jnp.where(has, m + jnp.log2(ls), NEG)

    def nb(k, dr, hops=1):
        a3 = ORDERS[k][2]
        return (co[a3] + (hops if dr == 0 else 4 - hops)) % 4

    def opp(k, i, dr):
        a3 = ORDERS[k][2]
        return rcopy(obuf.at[k, i, pl.ds(nb(k, 0, 2) * 4 + 2 * dr, 2)], r1o.at[k, i, dr],
                     a_s.at[k, i, dr], a_r.at[k, i, dr], at(a3, nb(k, dr)))

    def plain(k, i, dr):
        a3 = ORDERS[k][2]
        return rcopy(obuf.at[k, i, pl.ds(nb(k, dr) * 4 + 2 * (1 - dr), 2)], r1d.at[k, i, dr, pl.ds(2 * (1 - dr), 2)],
                     b_s.at[k, i, dr, 0], b_r.at[k, i, dr, 0], at(a3, nb(k, dr)))

    def merged(k, i, dr):
        a3 = ORDERS[k][2]
        return rcopy(mrg.at[k, i, dr], r1d.at[k, i, dr, pl.ds(2 * dr, 2)],
                     b_s.at[k, i, dr, 1], b_r.at[k, i, dr, 1], at(a3, nb(k, dr)))

    def send1(k, i):
        for dr in DIRS:
            opp(k, i, dr).start()
        for dr in DIRS:
            plain(k, i, dr).start()

    for k in KS:
        forward(k, 0)
    for k in KS:
        forward(k, 1)

    @pl.loop(0, NI - 1)
    def _(i):
        for k in KS:
            arrive(k, i)
        for k in KS:
            attend(k, i)
        for k in KS:
            send1(k, i)

        @pl.when(i < NI - 3)
        def _():
            for k in KS:
                forward(k, i + 2)

        @pl.when(i == NI - 3)
        def _():
            forward(0, NI - 1)

    arrive(0, NI - 1)
    attend(0, NI - 1)
    send1(0, NI - 1)

    def opp_lse(k, dr):
        a3 = ORDERS[k][2]
        return rcopy(lcol.at[k, pl.ds(nb(k, 0, 2) * 32 + 16 * dr, 16)], r1ol.at[k, dr],
                     al_s.at[k, dr], al_r.at[k, dr], at(a3, nb(k, dr)))

    def dir_lse(k, dr):
        a3 = ORDERS[k][2]
        return rcopy(mlse.at[k, dr], r1dl.at[k, dr], bl_s.at[k, dr], bl_r.at[k, dr], at(a3, nb(k, dr)))

    for k in KS:
        lcol[k] = lrow[k].T
        for dr in DIRS:
            opp_lse(k, dr).start()

    for k in KS:
        for dr in DIRS:
            base = nb(k, dr) * 4
            opp_lse(k, dr).wait_recv()
            mine = lcol[k, pl.ds(base * 8 + 16 * dr, 16), :]
            ws, ml = _merge_weights([mine, r1ol[k, dr]])
            mlse[k, dr, 16 * dr:16 * dr + 16, :] = ml
            mlse[k, dr, 16 * (1 - dr):16 * (1 - dr) + 16, :] = lcol[k, pl.ds(base * 8 + 16 * (1 - dr), 16), :]
            dir_lse(k, dr).start()
            for i in range(COUNT[k]):
                opp(k, i, dr).wait_recv()
                a = obuf[k, i, pl.ds(base + 2 * dr, 2)].reshape(16, LAT).astype(F32)
                b = r1o[k, i, dr].reshape(16, LAT).astype(F32)
                y = a * ws[0][:, i:i + 1] + b * ws[1][:, i:i + 1]
                mrg[k, i, dr] = y.astype(BF16).reshape(2, 8, LAT)
                merged(k, i, dr).start()

    def rs2(k, off):
        a2 = ORDERS[k][1]
        p = (co[a2] + off) % 4
        return rcopy(r1m.at[k, p, pl.ds(0, COUNT[k])], r2d.at[k, off - 1, pl.ds(0, COUNT[k])],
                     c_s.at[k, off - 1], c_r.at[k, off - 1], at(a2, p))

    def rs2_lse(k, off):
        a2 = ORDERS[k][1]
        p = (co[a2] + off) % 4
        return rcopy(lse1.at[k, pl.ds(p * 8, 8)], r2l.at[k, off - 1],
                     cl_s.at[k, off - 1], cl_r.at[k, off - 1], at(a2, p))

    for k in KS:
        base = co[ORDERS[k][2]] * 4
        for dr in DIRS:
            dir_lse(k, dr).wait_recv()
        ws, l1 = _merge_weights([lcol[k, pl.ds(base * 8, 32), :], r1dl[k, 0], r1dl[k, 1]])
        lse1[k] = l1
        for off in RING_OFFS:
            rs2_lse(k, off).start()
        for i in range(COUNT[k]):
            for dr in DIRS:
                plain(k, i, dr).wait_recv()
                merged(k, i, dr).wait_recv()
            y = obuf[k, i, pl.ds(base, 4)].reshape(32, LAT).astype(F32) * ws[0][:, i:i + 1]
            for dr in DIRS:
                y = y + r1d[k, i, dr].reshape(32, LAT).astype(F32) * ws[1 + dr][:, i:i + 1]
            y = y.astype(BF16).reshape(4, 8, LAT)
            for p in RING:
                r1m[k, p, i] = y[p]
        for off in (2, 1, 3):
            rs2(k, off).start()

    def rs3(k, off):
        a1 = ORDERS[k][0]
        j0 = co[a1] * 2 + core
        j = (j0 + off) % 8
        return rcopy(s3src.at[k, j], r3d.at[k, j0], e_s.at[k, off], e_r.at[k, off], line(a1, j))

    def rs3_lse(k, off):
        a1 = ORDERS[k][0]
        j0 = co[a1] * 2 + core
        j = (j0 + off) % 8
        return rcopy(s3l.at[k, j], r3l.at[k, j0], el_s.at[k, off], el_r.at[k, off], line(a1, j))

    def got3(k, off):
        j0 = co[ORDERS[k][0]] * 2 + core
        src = (j0 + 8 - off) % 8
        rcopy(s3src.at[k, 0], r3d.at[k, src], e_s.at[k, off], e_r.at[k, off], partner).wait_recv()
        rcopy(s3l.at[k, 0], r3l.at[k, src], el_s.at[k, off], el_r.at[k, off], partner).wait_recv()

    for k in KS:
        p2 = co[ORDERS[k][1]]
        n = COUNT[k]
        for off in RING_OFFS:
            rs2_lse(k, off).wait_recv()
        ws, l2 = _merge_weights([lse1[k, pl.ds(p2 * 8, 8), :]] + [r2l[k, x] for x in KS])
        lt = l2.T[0:8, :]
        for j in range(8):
            s3l[k, j] = jnp.broadcast_to(lt[:, j:j + 1], (8, LANES))
        for off in LINE_OFFS:
            rs3_lse(k, off).start()
        for off in RING_OFFS:
            rs2(k, off).wait_recv()
        ys = []
        for i in range(n):
            y = r1m[k, p2, i].astype(F32) * ws[0][:, i:i + 1]
            for x in KS:
                y = y + r2d[k, x, i].astype(F32) * ws[1 + x][:, i:i + 1]
            ys.append(y)
        y = jnp.concatenate(ys, axis=0).astype(BF16)
        pm = _perm(64, 8 * n, lambda r, c: (c == (r % 8) * 8 + r // 8) & (r % 8 < n))
        s3src[k] = jnp.dot(pm, y, preferred_element_type=F32).astype(BF16).reshape(8, 8, LAT)
        for off in LINE_OFFS:
            rs3(k, off).start()
        j0 = co[ORDERS[k][0]] * 2 + core
        r3d[k, j0] = s3src[k, j0]
        r3l[k, j0] = s3l[k, j0]

    outs = [[None] * 3 for _ in DIRS]
    for k in KS:
        for off in LINE_OFFS:
            got3(k, off)
        for h in DIRS:
            ws, _ = _merge_weights([r3l[k, 2 * p + h] for p in RING])
            y = None
            for p in RING:
                t = r3d[k, 2 * p + h].astype(F32) * jnp.concatenate([ws[p]] * 4, axis=1)
                y = t if y is None else y + t
            outs[h][k] = y
    rows = jnp.concatenate([outs[h][k] for h in DIRS for k in KS], axis=0).astype(BF16)
    fin = _perm(32, 48, lambda r, c: r == (c // 24) * 16 + 3 * (c % 8) + (c // 8) % 3)
    fin = jnp.where(_perm(32, 48, lambda r, c: 3 * (c % 8) + (c // 8) % 3 < 16) > 0, fin, jnp.zeros_like(fin))
    oout[...] = jnp.dot(fin, rows, preferred_element_type=F32).astype(BF16)
    store = pltpu.make_async_copy(oout, o_h, sem_o)
    store.start()

    for k in KS:
        for off in LINE_OFFS:
            rs3(k, off).wait_send()
            rs3_lse(k, off).wait_send()
        for off in RING_OFFS:
            rs2(k, off).wait_send()
            rs2_lse(k, off).wait_send()
        for dr in DIRS:
            opp_lse(k, dr).wait_send()
            dir_lse(k, dr).wait_send()

    def drain(k, i):
        for dr in DIRS:
            opp(k, i, dr).wait_send()
            plain(k, i, dr).wait_send()
            merged(k, i, dr).wait_send()

    each(drain)
    whole = q_all.at[0, 0]
    for off in KS:
        wait_bytes(whole, s2s.at[off])
    for off in RING:
        for dr in DIRS:
            wait_bytes(whole, s3s.at[dr, off])
        wait_bytes(whole, sfs.at[off])

    @pl.loop(0, 16)
    def _(s):
        push_cache(s).wait_send()

    store.wait()


def solution(mesh):
    def local(q, cache, lens):
        dma = pltpu.SemaphoreType.DMA
        V = pltpu.VMEM
        anyspace = pl.BlockSpec(memory_space=pl.ANY)
        scratch = [
            V((32, QW), BF16), V((2, 3, 8, QW), BF16), V((3, 8, 8, QW), BF16), V((3, NI, 16, 8, QW), BF16),
            V((16, 64, 8, QW), BF16), V((3, NI, 16, 8, LAT), BF16), V((3, LANES, LANES), F32), V((3, LANES, LANES), F32),
            V((3, NI, 2, 2, 8, LAT), BF16), V((3, 2, 16, LANES), F32), V((3, NI, 2, 2, 8, LAT), BF16),
            V((3, 2, 32, LANES), F32), V((3, NI, 2, 4, 8, LAT), BF16), V((3, 2, 32, LANES), F32),
            V((3, 4, NI, 8, LAT), BF16), V((3, 32, LANES), F32),
            V((3, 3, NI, 8, LAT), BF16), V((3, 3, 8, LANES), F32), V((3, 8, 8, LAT), BF16), V((3, 8, 8, LANES), F32),
            V((3, 8, 8, LAT), BF16), V((3, 8, 8, LANES), F32), V((32, LAT), BF16),
            dma, dma((16,)), dma((16,)), dma((16,)), dma((3, 8)), dma((3, 8)), dma((3,)), dma((3, NI, 3)),
            dma((2, 4)), dma((3, NI, 2, 4)), dma((4,)), dma((3, NI, 4)),
            dma((3, NI, 2)), dma((3, NI, 2)), dma((3, 2)), dma((3, 2)),
            dma((3, NI, 2, 2)), dma((3, NI, 2, 2)), dma((3, 2)), dma((3, 2)),
            dma((3, 3)), dma((3, 3)), dma((3, 3)), dma((3, 3)),
            dma((3, 8)), dma((3, 8)), dma((3, 8)), dma((3, 8)), dma,
        ]
        o = pl.pallas_call(
            _kernel,
            out_shape=jax.ShapeDtypeStruct((32, LAT), BF16),
            in_specs=[pl.BlockSpec(memory_space=pltpu.SMEM), anyspace, anyspace],
            out_specs=anyspace,
            scratch_shapes=scratch,
            compiler_params=pltpu.CompilerParams(collective_id=0, has_side_effects=True,
                                                 vmem_limit_bytes=58 * 2 ** 20),
        )(lens, q.reshape(32, QW), cache.reshape(32, 32, 8, QW))
        return o.reshape(32, 1, LAT)

    return jax.shard_map(local, mesh=mesh,
                         in_specs=(P('dp', 'dcp', None), P('dp', None, 'dcp', None, None), P('dp')),
                         out_specs=P('dp', 'dcp', None), check_vma=False)
```

```python
import functools
import math

import jax
import jax.numpy as jnp
from jax import lax
from jax.experimental import pallas as pl
from jax.experimental.pallas import tpu as pltpu
from jax.sharding import PartitionSpec as P

ROPE = 64
QK_DIM = 192
SCALE2 = QK_DIM ** -0.5 * math.log2(math.e)
NEG = -3.0e38
MESH = pl.DeviceIdType.MESH
F32 = jnp.float32
BF16 = jnp.bfloat16

STRIDE = (2, 8, 32)
ORDERS = ((0, 1, 2), (1, 2, 0), (2, 0, 1))
COUNT = (6, 5, 5)
NI = 6
SPLIT, DIRECT, EARLY = 3, 2, 4


LAT, QW, LANES = 512, 576, 128
KS, DIRS, RING, RING_OFFS, LINE_OFFS = range(3), range(2), range(4), range(1, 4), range(1, 8)


def _perm(rows, cols, f):
    r = lax.broadcasted_iota(jnp.int32, (rows, cols), 0)
    c = lax.broadcasted_iota(jnp.int32, (rows, cols), 1)
    return f(r, c).astype(F32).astype(BF16)


def _merge_weights(lses):
    top = functools.reduce(jnp.maximum, lses)
    ws = [jnp.exp2(v - top) for v in lses]
    tot = functools.reduce(jnp.add, ws)
    inv = 1.0 / tot
    return [w * inv for w in ws], top + jnp.log2(tot)


def _kernel(lens, q_h, c_h, o_h,
            q_in, s1src, s1buf, q_all, cbuf, obuf, lrow, lcol, r1o, r1d, r1l, r1m, lse1,
            r2d, r2l, s3src, s3l, r3d, r3l, oout,
            sem_q, sem_o, c_s, c_r, s1_s, s1_r, s2_s, s2_r, s3_s, s3f_r, s3_r, sf_s,
            ro_s, ro_r, r1_s, r1_r, r1l_s, r1l_r, r2_s, r2_r, r2l_s, r2l_r, r3_s, r3_r, r3l_s, r3l_r):
    d = lax.axis_index('dcp')
    core = d % 2
    co = ((d // 2) % 4, (d // 8) % 4, d // 32)
    partner = {'dcp': d + 1 - 2 * core}

    def ring(axis, off):
        return {'dcp': d + ((co[axis] + off) % 4 - co[axis]) * STRIDE[axis]}

    def line(axis, j):
        return {'dcp': d + (j // 2 - co[axis]) * STRIDE[axis] + (j % 2 - core)}

    def send(src, dst, ss, rs, dev):
        pltpu.make_async_remote_copy(src_ref=src, dst_ref=dst, send_sem=ss, recv_sem=rs,
                                     device_id=dev, device_id_type=MESH).start()

    def wait(ref, sem):
        pltpu.make_async_copy(ref, ref, sem).wait()

    def ks_of(i):
        return KS if i < NI - 1 else range(1)

    load_q = pltpu.make_async_copy(q_h, q_in, sem_q)
    load_q.start()

    def cache_rows(i, half):
        n = len(ks_of(i))
        return c_h.at[pl.ds(16 * half + 3 * i, n)], cbuf.at[pl.ds(3 * i, n), pl.ds(32 * core, 32)]

    for i in range(NI):
        src, dst = cache_rows(i, core)
        pltpu.make_async_copy(src, dst, c_r.at[i]).start()

    bar = pltpu.get_barrier_semaphore()
    pl.semaphore_signal(bar, inc=1, device_id=partner, device_id_type=MESH)
    for a in KS:
        for off in RING_OFFS:
            for c2 in DIRS:
                pl.semaphore_signal(bar, inc=1, device_id=line(a, ((co[a] + off) % 4) * 2 + c2), device_id_type=MESH)
    lrow[...] = jnp.zeros_like(lrow)

    def sel(r, c):
        s = 3 * (r % 8) + (r // 8) % 3
        return (c == 16 * (r // 24) + s) & (s < 16)

    load_q.wait()
    qp = jnp.dot(_perm(48, 32, sel), q_in[...], preferred_element_type=F32).astype(BF16)
    s1src[...] = qp.reshape(2, 3, 8, QW)
    pl.semaphore_wait(bar, 19)

    def place(k):
        return co[ORDERS[k][0]] * 2 + core

    for k in KS:
        j0 = place(k)
        for off in LINE_OFFS:
            j = (j0 + off) % 8
            send(s1src.at[j % 2, k], s1buf.at[k, j0], s1_s, s1_r.at[k], line(ORDERS[k][0], j))
        s1buf[k, j0] = s1src[core, k]
    for i in range(NI):
        src, dst = cache_rows(i, 1 - core)
        send(src, dst, c_s, c_r.at[i], partner)

    def slot(k, i):
        return (k * NI + i) * 16

    def blk(k, i, off):
        _, a2, a3 = ORDERS[k]
        return q_all.at[slot(k, i) + co[a3] * 4 + (co[a2] - off) % 4]

    def copy3(k, i, off):
        b = blk(k, i, off)
        a3 = ORDERS[k][2]
        for o in (1, 3):
            fw = i >= DIRECT and off // 2 == o // 2
            send(b, b, s3_s, s3f_r.at[i] if fw else s3_r.at[i], ring(a3, o))
        if i < DIRECT:
            send(b, b, s3_s, s3_r.at[i], ring(a3, 2))

    def stage2(k, i):
        b = blk(k, i, 0)
        for off in (2, 1, 3):
            send(b, b, s2_s, s2_r.at[i], ring(ORDERS[k][1], off))
        copy3(k, i, 0)

    tr = _perm(64, 64, lambda r, c: (r // 8 == c % 8) & (r % 8 == c // 8))
    for k in KS:
        wait(s1buf.at[k, pl.ds(0, 7)], s1_r.at[k])
        rows = jnp.dot(tr, s1buf[k].reshape(64, QW), preferred_element_type=F32).astype(BF16).reshape(8, 8, QW)
        _, a2, a3 = ORDERS[k]
        for i in range(COUNT[k]):
            q_all[slot(k, i) + co[a3] * 4 + co[a2]] = rows[i]
        for i in range(EARLY):
            stage2(k, i)

    def stage3(i):
        n = len(ks_of(i))
        wait(q_all.at[pl.ds(0, 3 * n)], s2_r.at[i])
        for off in (1, 3, 2):
            for k in ks_of(i):
                copy3(k, i, off)

    def more2(i):
        for k in ks_of(i):
            stage2(k, i)

    def forward(i):
        n = len(ks_of(i))
        wait(q_all.at[pl.ds(0, 4 * n)], s3f_r.at[i])
        for off in RING:
            for k in ks_of(i):
                _, a2, a3 = ORDERS[k]
                o = 1 if off < 2 else 3
                b = q_all.at[slot(k, i) + ((co[a3] - o) % 4) * 4 + (co[a2] - off) % 4]
                send(b, b, sf_s, s3_r.at[i], ring(a3, o))

    def arrive(i):
        n = len(ks_of(i))
        wait(cbuf.at[pl.ds(0, n)], c_r.at[i])
        wait(q_all.at[pl.ds(0, (12 if i < DIRECT else 8) * n)], s3_r.at[i])

    for i in range(EARLY):
        stage3(i)
        if EARLY + i < NI:
            more2(EARLY + i)

    chip8 = (d // 2) * 16

    def attend(k, i):
        s = 3 * i + k
        n = lens[16 * core + s]
        cs = cbuf[s].reshape(LAT, QW)
        qs = q_all[pl.ds(slot(k, i), 16)].reshape(LANES, QW)
        st = lax.dot_general(cs, qs, (((1,), (1,)), ((), ())), preferred_element_type=F32) * SCALE2
        j = lax.broadcasted_iota(jnp.int32, (LAT, LANES), 0)
        ok = (j & 7) + ((j >> 3) & 31) * 1024 + (j >> 8) * 8 + chip8 < n
        st = jnp.where(ok, st, NEG)
        m = jnp.max(st, axis=0, keepdims=True)
        p = jnp.where(ok, jnp.exp2(st - m), 0.0)
        l = jnp.sum(p, axis=0, keepdims=True)
        has = l > 0.0
        ls = jnp.where(has, l, 1.0)
        pn = (p * (1.0 / ls)).astype(BF16)
        o = lax.dot_general(pn, cs[:, :LAT], (((0,), (0,)), ((), ())), preferred_element_type=F32)
        obuf[pl.ds(slot(k, i), 16)] = o.astype(BF16).reshape(16, 8, LAT)
        lrow[k, i:i + 1, :] = jnp.where(has, m + jnp.log2(ls), NEG)

    def wave(i):
        return 0 if i < SPLIT else 1

    def send1(k, i):
        a3 = ORDERS[k][2]
        w = wave(i)
        for o in RING_OFFS:
            g = slot(k, i) + ((co[a3] + o) % 4) * 4
            if o == 2 and w == 0:
                for h in DIRS:
                    send(obuf.at[pl.ds(g + 2 * h, 2)], r1o.at[k, i, h], r1_s, ro_r.at[i], ring(a3, 1 + 2 * h))
            else:
                send(obuf.at[pl.ds(g, 4)], r1d.at[k, i, o - 1], r1_s, r1_r.at[w, k], ring(a3, o))

    def relay(i):
        wait(obuf.at[pl.ds(0, 4 * len(KS))], ro_r.at[i])
        for k in KS:
            for h in DIRS:
                send(r1o.at[k, i, h], r1d.at[k, i, 1, pl.ds(2 * h, 2)], ro_s, r1_r.at[0, k], ring(ORDERS[k][2], 1 + 2 * h))

    def members(w, k):
        return range(SPLIT) if w == 0 else range(SPLIT, COUNT[k])

    def send1_lse(w):
        for k in KS:
            lcol[w, k] = lrow[k].T
            for o in RING_OFFS:
                p = (co[ORDERS[k][2]] + o) % 4
                send(lcol.at[w, k, pl.ds(p * 32, 32)], r1l.at[w, k, o - 1], r1l_s, r1l_r.at[w, k], ring(ORDERS[k][2], o))

    for i in range(NI):
        with jax.named_scope(f"arrive{i}"):
            arrive(i)
        with jax.named_scope(f"attend{i}"):
            for k in ks_of(i):
                attend(k, i)
            for k in ks_of(i):
                send1(k, i)
        with jax.named_scope(f"rest{i}"):
            if i == SPLIT - 1:
                send1_lse(0)
            if 0 < i <= SPLIT:
                relay(i - 1)
            if DIRECT <= i + 2 < NI:
                forward(i + 2)
            if EARLY + i < NI:
                stage3(EARLY + i)
            if 2 * EARLY + i < NI:
                more2(2 * EARLY + i)

    send1_lse(1)

    def merge1(w, k):
        a2, a3 = ORDERS[k][1:]
        its = members(w, k)
        wait(r1l.at[w, k], r1l_r.at[w, k])
        ws, l1 = _merge_weights([lcol[w, k, pl.ds(co[a3] * 32, 32), :]] + [r1l[w, k, x] for x in KS])
        lse1[w, k] = l1
        for o in RING_OFFS:
            p = (co[a2] + o) % 4
            send(lse1.at[w, k, pl.ds(p * 8, 8)], r2l.at[w, k, o - 1], r2l_s, r2l_r.at[w, k], ring(a2, o))
        wait(obuf.at[pl.ds(0, 12 * len(its))], r1_r.at[w, k])
        for i in its:
            y = obuf[pl.ds(slot(k, i) + co[a3] * 4, 4)].reshape(32, LAT).astype(F32) * ws[0][:, i:i + 1]
            for x in KS:
                y = y + r1d[k, i, x].reshape(32, LAT).astype(F32) * ws[1 + x][:, i:i + 1]
            y = y.astype(BF16).reshape(4, 8, LAT)
            for p in RING:
                r1m[k, p, i] = y[p]
        for o in (2, 1, 3):
            p = (co[a2] + o) % 4
            sl = pl.ds(its[0], len(its))
            send(r1m.at[k, p, sl], r2d.at[k, o - 1, sl], r2_s, r2_r.at[w, k], ring(a2, o))

    def merge2(w, k):
        a1, a2, _ = ORDERS[k]
        its = members(w, k)
        n = len(its)
        j0 = place(k)
        wait(r2l.at[w, k], r2l_r.at[w, k])
        ws, l2 = _merge_weights([lse1[w, k, pl.ds(co[a2] * 8, 8), :]] + [r2l[w, k, x] for x in KS])
        lt = l2.T[0:8, :]
        for j in range(8):
            s3l[w, k, j] = jnp.broadcast_to(lt[:, j:j + 1], (8, LANES))
        for off in LINE_OFFS:
            j = (j0 + off) % 8
            send(s3l.at[w, k, j], r3l.at[w, k, j0], r3l_s, r3l_r.at[w, k], line(a1, j))
        wait(obuf.at[pl.ds(0, 3 * n)], r2_r.at[w, k])
        ys = []
        for i in its:
            y = r1m[k, co[a2], i].astype(F32) * ws[0][:, i:i + 1]
            for x in KS:
                y = y + r2d[k, x, i].astype(F32) * ws[1 + x][:, i:i + 1]
            ys.append(y)
        y = jnp.concatenate(ys, axis=0).astype(BF16)
        lo = its[0]
        pm = _perm(64, 8 * n, lambda r, c: (c == (r % 8 - lo) * 8 + r // 8) & (r % 8 >= lo) & (r % 8 < lo + n))
        s3src[w, k] = jnp.dot(pm, y, preferred_element_type=F32).astype(BF16).reshape(8, 8, LAT)
        for off in LINE_OFFS:
            j = (j0 + off) % 8
            send(s3src.at[w, k, j], r3d.at[w, k, j0], r3_s, r3_r.at[w, k], line(a1, j))
        r3d[w, k, j0] = s3src[w, k, j0]
        r3l[w, k, j0] = s3l[w, k, j0]

    rows = {}

    def merge3(w, k):
        wait(r3l.at[w, k, pl.ds(0, 7)], r3l_r.at[w, k])
        wait(r3d.at[w, k, pl.ds(0, 7)], r3_r.at[w, k])
        for h in DIRS:
            ws, _ = _merge_weights([r3l[w, k, 2 * p + h] for p in RING])
            y = None
            for p in RING:
                t = r3d[w, k, 2 * p + h].astype(F32) * jnp.concatenate([ws[p]] * 4, axis=1)
                y = t if y is None else y + t
            rows[w, h, k] = y

    for k in KS:
        merge1(0, k)
    for k in KS:
        merge1(1, k)
    for k in KS:
        merge2(0, k)
    for k in KS:
        merge2(1, k)
    for k in KS:
        merge3(0, k)
    for k in KS:
        merge3(1, k)
    flat = jnp.concatenate([rows[w, h, k] for w in DIRS for h in DIRS for k in KS], axis=0).astype(BF16)

    def pick(r, c):
        w, h, k, i = c // 48, (c // 24) % 2, (c // 8) % 3, c % 8
        s = 3 * i + k
        return (r == 16 * h + s) & (s < 16) & ((i >= SPLIT) == (w == 1))

    oout[...] = jnp.dot(_perm(32, 96, pick), flat, preferred_element_type=F32).astype(BF16)
    store = pltpu.make_async_copy(oout, o_h, sem_o)
    store.start()

    wait(cbuf.at[pl.ds(0, 8)], c_s)
    wait(q_all.at[pl.ds(0, 21)], s1_s)
    wait(q_all.at[pl.ds(0, 48)], s2_s)
    wait(q_all.at[pl.ds(0, 128 + 4 * DIRECT * len(KS))], s3_s)
    wait(q_all.at[pl.ds(0, 4 * (16 - DIRECT * len(KS)))], sf_s)
    wait(obuf.at[pl.ds(0, 192)], r1_s)
    wait(obuf.at[pl.ds(0, 4 * len(KS) * SPLIT)], ro_s)
    wait(r1l, r1l_s)
    wait(obuf.at[pl.ds(0, 48)], r2_s)
    wait(r2l, r2l_s)
    for w in DIRS:
        for k in KS:
            wait(r3d.at[w, k, pl.ds(0, 7)], r3_s)
            wait(r3l.at[w, k, pl.ds(0, 7)], r3l_s)
    store.wait()


def solution(mesh):
    def local(q, cache, lens):
        dma = pltpu.SemaphoreType.DMA
        V = pltpu.VMEM
        anyspace = pl.BlockSpec(memory_space=pl.ANY)
        tile, qtile = (8, LAT), (8, QW)
        line = (2, 3, 8)
        scratch = [
            V((32, QW), BF16), V((2, 3) + qtile, BF16), V((3, 8) + qtile, BF16), V((288,) + qtile, BF16),
            V((16, 64) + qtile, BF16), V((288,) + tile, BF16), V((3, LANES, LANES), F32), V((2, 3, LANES, LANES), F32),
            V((3, SPLIT, 2, 2) + tile, BF16), V((3, NI, 3, 4) + tile, BF16), V((2, 3, 3, 32, LANES), F32),
            V((3, 4, NI) + tile, BF16), V((2, 3, 32, LANES), F32),
            V((3, 3, NI) + tile, BF16), V((2, 3, 3, 8, LANES), F32),
            V(line + tile, BF16), V(line + (8, LANES), F32), V(line + tile, BF16), V(line + (8, LANES), F32),
            V((32, LAT), BF16),
            dma, dma, dma, dma((NI,)), dma, dma((3,)), dma, dma((NI,)), dma, dma((NI,)), dma((NI,)), dma,
            dma, dma((SPLIT,)), dma, dma((2, 3)), dma, dma((2, 3)), dma, dma((2, 3)), dma, dma((2, 3)),
            dma, dma((2, 3)), dma, dma((2, 3)),
        ]
        o = pl.pallas_call(
            _kernel,
            out_shape=jax.ShapeDtypeStruct((32, LAT), BF16),
            in_specs=[pl.BlockSpec(memory_space=pltpu.SMEM), anyspace, anyspace],
            out_specs=anyspace,
            scratch_shapes=scratch,
            compiler_params=pltpu.CompilerParams(collective_id=0, has_side_effects=True,
                                                 vmem_limit_bytes=58 * 2 ** 20),
        )(lens, q.reshape(32, QW), cache.reshape(32, 32, 8, QW))
        return o.reshape(32, 1, LAT)

    return jax.shard_map(local, mesh=mesh,
                         in_specs=(P('dp', 'dcp', None), P('dp', None, 'dcp', None, None), P('dp')),
                         out_specs=P('dp', 'dcp', None), check_vma=False)
```

```python
import functools
import math

import jax
import jax.numpy as jnp
from jax import lax
from jax.experimental import pallas as pl
from jax.experimental.pallas import tpu as pltpu
from jax.sharding import PartitionSpec as P

ROPE = 64
QK_DIM = 192
SCALE2 = QK_DIM ** -0.5 * math.log2(math.e)
NEG = -3.0e38
MESH = pl.DeviceIdType.MESH
F32 = jnp.float32
BF16 = jnp.bfloat16

STRIDE = (2, 8, 32)
ORDERS = ((0, 1, 2), (1, 2, 0), (2, 0, 1))
COUNT = (6, 5, 5)
NI = 6
SPLIT, DIRECT, EARLY = 3, 2, 4


LAT, QW, LANES = 512, 576, 128
KS, DIRS, RING, RING_OFFS, LINE_OFFS = range(3), range(2), range(4), range(1, 4), range(1, 8)


def _perm(rows, cols, f):
    r = lax.broadcasted_iota(jnp.int32, (rows, cols), 0)
    c = lax.broadcasted_iota(jnp.int32, (rows, cols), 1)
    return f(r, c).astype(F32).astype(BF16)


def _merge_weights(lses):
    top = functools.reduce(jnp.maximum, lses)
    ws = [jnp.exp2(v - top) for v in lses]
    tot = functools.reduce(jnp.add, ws)
    inv = 1.0 / tot
    return [w * inv for w in ws], top + jnp.log2(tot)


def _kernel(lens_h, q_h, c_h, o_h,
            lens, q_in, s1src, s1buf, q_even, q_odd, cbuf, obuf, lrow, wcol, r1d, r1l, r1m, lse1,
            r2d, r2l, s3src, s3l, r3d, r3l, oout,
            sem_l, sem_q, sem_o, c_s, c_r, s1_s, s1_r, s2_s, s2_r, s3_s, s3f_r, s3_r, sf_s,
            r1_s, r1_r, r1l_s, r1l_r, r2_s, r2_r, r2l_s, r2l_r, r3_s, r3_r, r3l_s, r3l_r):
    d = lax.axis_index('dcp')
    core = d % 2
    co = ((d // 2) % 4, (d // 8) % 4, d // 32)
    partner = {'dcp': d + 1 - 2 * core}

    def ring(axis, off):
        return {'dcp': d + ((co[axis] + off) % 4 - co[axis]) * STRIDE[axis]}

    def line(axis, j):
        return {'dcp': d + (j // 2 - co[axis]) * STRIDE[axis] + (j % 2 - core)}

    def send(src, dst, ss, rs, dev):
        pltpu.make_async_remote_copy(src_ref=src, dst_ref=dst, send_sem=ss, recv_sem=rs,
                                     device_id=dev, device_id_type=MESH).start()

    def wait(ref, sem):
        pltpu.make_async_copy(ref, ref, sem).wait()

    def ks_of(i):
        return KS if i < NI - 1 else range(1)

    load_q = pltpu.make_async_copy(q_h, q_in, sem_q)
    load_q.start()
    load_l = pltpu.make_async_copy(lens_h, lens, sem_l)
    load_l.start()

    def cache_rows(i, half):
        n = len(ks_of(i))
        return c_h.at[pl.ds(16 * half + 3 * i, n)], cbuf.at[pl.ds(3 * i, n), pl.ds(32 * core, 32)]

    for i in range(NI):
        src, dst = cache_rows(i, core)
        pltpu.make_async_copy(src, dst, c_r.at[i]).start()

    bar = pltpu.get_barrier_semaphore()
    pl.semaphore_signal(bar, inc=1, device_id=partner, device_id_type=MESH)
    for a in KS:
        for off in RING_OFFS:
            for c2 in DIRS:
                pl.semaphore_signal(bar, inc=1, device_id=line(a, ((co[a] + off) % 4) * 2 + c2), device_id_type=MESH)
    lrow[...] = jnp.zeros_like(lrow)
    load_l.wait()

    def sel(r, c):
        s = 3 * (r % 8) + (r // 8) % 3
        return (c == 16 * (r // 24) + s) & (s < 16)

    load_q.wait()
    qp = jnp.dot(_perm(48, 32, sel), q_in[...], preferred_element_type=F32).astype(BF16)
    s1src[...] = qp.reshape(2, 3, 8, QW)
    pl.semaphore_wait(bar, 19)

    def place(k):
        return co[ORDERS[k][0]] * 2 + core

    for k in KS:
        j0 = place(k)
        for off in LINE_OFFS:
            j = (j0 + off) % 8
            send(s1src.at[j % 2, k], s1buf.at[k, j0], s1_s.at[k], s1_r.at[k], line(ORDERS[k][0], j))
        s1buf[k, j0] = s1src[core, k]
    for i in range(NI):
        src, dst = cache_rows(i, 1 - core)
        send(src, dst, c_s, c_r.at[i], partner)

    def q_of(i):
        return q_odd if i % 2 else q_even

    def q_slot(k, i):
        return (k * 3 + i // 2) * 16

    def slot(k, i):
        return (k * NI + i) * 16

    def blk(k, i, off):
        _, a2, a3 = ORDERS[k]
        return q_of(i).at[q_slot(k, i) + co[a3] * 4 + (co[a2] - off) % 4]

    def copy3(k, i, off):
        b = blk(k, i, off)
        a3 = ORDERS[k][2]
        for o in (1, 3):
            fw = i >= DIRECT and off // 2 == o // 2
            send(b, b, s3_s.at[i % 2], s3f_r.at[i] if fw else s3_r.at[i], ring(a3, o))
        if i < DIRECT:
            send(b, b, s3_s.at[i % 2], s3_r.at[i], ring(a3, 2))

    def stage2(k, i):
        b = blk(k, i, 0)
        for off in (2, 1, 3):
            send(b, b, s2_s.at[i % 2], s2_r.at[i], ring(ORDERS[k][1], off))
        copy3(k, i, 0)

    tr = _perm(64, 64, lambda r, c: (r // 8 == c % 8) & (r % 8 == c // 8))
    for k in KS:
        wait(s1buf.at[k, pl.ds(0, 7)], s1_r.at[k])
        rows = jnp.dot(tr, s1buf[k].reshape(64, QW), preferred_element_type=F32)
        _, a2, a3 = ORDERS[k]
        for i in range(COUNT[k]):
            y = rows[8 * i:8 * i + 8, :LAT if i % 2 else QW]
            if i % 2 == 0:
                y = jnp.concatenate([y, rows[8 * i + 8:8 * i + 16, LAT:]], axis=1)
            q_of(i)[q_slot(k, i) + co[a3] * 4 + co[a2]] = y.astype(BF16)
        for i in range(EARLY):
            stage2(k, i)

    def stage3(i):
        n = len(ks_of(i))
        wait(q_of(i).at[pl.ds(0, 3 * n)], s2_r.at[i])
        for off in (1, 3, 2):
            for k in ks_of(i):
                copy3(k, i, off)

    def more2(i):
        for k in ks_of(i):
            stage2(k, i)

    def forward(i):
        n = len(ks_of(i))
        wait(q_of(i).at[pl.ds(0, 4 * n)], s3f_r.at[i])
        for off in RING:
            for k in ks_of(i):
                _, a2, a3 = ORDERS[k]
                o = 1 if off < 2 else 3
                b = q_of(i).at[q_slot(k, i) + ((co[a3] - o) % 4) * 4 + (co[a2] - off) % 4]
                send(b, b, sf_s.at[i % 2], s3_r.at[i], ring(a3, o))

    def arrive(i):
        n = len(ks_of(i))
        wait(cbuf.at[pl.ds(0, n)], c_r.at[i])
        wait(q_of(i).at[pl.ds(0, (12 if i < DIRECT else 8) * n)], s3_r.at[i])

    for i in range(EARLY):
        stage3(i)
        if EARLY + i < NI:
            more2(EARLY + i)

    chip8 = (d // 2) * 16

    j = lax.broadcasted_iota(jnp.int32, (LAT, LANES), 0)
    pos = (j & 7) + ((j >> 3) & 31) * 1024 + (j >> 8) * 8

    def cache_of(k, i):
        return cbuf[3 * i + k].reshape(LAT, QW)

    def scores(k, i):
        cs = cache_of(k, i)
        n = pl.ds(q_slot(k, i), 16)
        lat = q_of(i)[n, :, :LAT].reshape(LANES, LAT)
        rope = q_even[n, :, LAT:].reshape(LANES, LANES)
        rope = rope[:, ROPE:] if i % 2 else rope[:, :ROPE]
        dims = (((1,), (1,)), ((), ()))
        st = lax.dot_general(cs[:, :LAT], lat, dims, preferred_element_type=F32)
        return (st + lax.dot_general(cs[:, LAT:], rope, dims, preferred_element_type=F32)) * SCALE2

    def softmax(st, k, i):
        ok = pos < lens[16 * core + 3 * i + k] - chip8
        st = jnp.where(ok, st, NEG)
        m = jnp.max(st, axis=0, keepdims=True)
        p = jnp.where(ok, jnp.exp2(st - m), 0.0)
        l = jnp.sum(p, axis=0, keepdims=True)
        has = l > 0.0
        ls = jnp.where(has, l, 1.0)
        w = wave(i)
        lrow[w, k, i - w * SPLIT:i - w * SPLIT + 1, :] = jnp.where(has, m + jnp.log2(ls), NEG)
        return (p * (1.0 / ls)).astype(BF16)

    def attend(i):
        ks = ks_of(i)
        sts = [scores(k, i) for k in ks]
        ps = [softmax(st, k, i) for st, k in zip(sts, ks)]
        outs = [lax.dot_general(p, cache_of(k, i)[:, :LAT], (((0,), (0,)), ((), ())), preferred_element_type=F32)
                for p, k in zip(ps, ks)]
        for o, k in zip(outs, ks):
            obuf[pl.ds(slot(k, i), 16)] = o.astype(BF16).reshape(16, 8, LAT)

    def wave(i):
        return 0 if i < SPLIT else 1

    def send1(k, i):
        a3 = ORDERS[k][2]
        for o in (2, 1, 3):
            b = obuf.at[pl.ds(slot(k, i) + ((co[a3] + o) % 4) * 4, 4)]
            send(b, r1d.at[k, i, o - 1], r1_s, r1_r.at[wave(i), k], ring(a3, o))

    def members(w, k):
        return range(SPLIT) if w == 0 else range(SPLIT, COUNT[k])

    def send1_lse(w):
        for k in KS:
            for o in RING_OFFS:
                send(lrow.at[w, k], r1l.at[w, k, o - 1], r1l_s, r1l_r.at[w, k], ring(ORDERS[k][2], o))

    for i in range(NI):
        with jax.named_scope(f"arrive{i}"):
            arrive(i)
        with jax.named_scope(f"attend{i}"):
            attend(i)
            for k in ks_of(i):
                send1(k, i)
        with jax.named_scope(f"rest{i}"):
            if i == SPLIT - 1:
                send1_lse(0)
            if DIRECT <= i + 2 < NI:
                forward(i + 2)
            if EARLY + i < NI:
                stage3(EARLY + i)
            if 2 * EARLY + i < NI:
                more2(2 * EARLY + i)

    send1_lse(1)

    def columns(ws, row, n):
        wcol[:, :32] = jnp.concatenate(ws, axis=0).T
        t = wcol[pl.ds(row, n), :32]
        return lambda x, i: t[:, 8 * x + i:8 * x + i + 1]

    def merge1(w, k):
        a2, a3 = ORDERS[k][1:]
        its = members(w, k)
        wait(r1l.at[w, k], r1l_r.at[w, k])
        ws, lse1[w, k] = _merge_weights([lrow[w, k]] + [r1l[w, k, x] for x in KS])
        for o in RING_OFFS:
            send(lse1.at[w, k], r2l.at[w, k, o - 1], r2l_s, r2l_r.at[w, k], ring(a2, o))
        cols = columns(ws, co[a3] * 32, 32)
        wait(obuf.at[pl.ds(0, 12 * len(its))], r1_r.at[w, k])
        for i in its:
            y = obuf[pl.ds(slot(k, i) + co[a3] * 4, 4)].reshape(32, LAT).astype(F32) * cols(0, i - its[0])
            for x in KS:
                y = y + r1d[k, i, x].reshape(32, LAT).astype(F32) * cols(1 + x, i - its[0])
            y = y.astype(BF16).reshape(4, 8, LAT)
            for p in RING:
                r1m[k, p, i] = y[p]
        for o in (2, 1, 3):
            p = (co[a2] + o) % 4
            sl = pl.ds(its[0], len(its))
            send(r1m.at[k, p, sl], r2d.at[k, o - 1, sl], r2_s, r2_r.at[w, k], ring(a2, o))

    def merge2(w, k):
        a1, a2, a3 = ORDERS[k]
        its = members(w, k)
        n = len(its)
        j0 = place(k)
        wait(r2l.at[w, k], r2l_r.at[w, k])
        ws, l2 = _merge_weights([lse1[w, k]] + [r2l[w, k, x] for x in KS])
        g = co[a3] * 4 + co[a2]
        lt = pltpu.roll(l2, ((16 - g) % 16) * 8, 1)
        cols = columns(ws, g * 8, 8)
        for j in range(8):
            s3l[w, k, j] = jnp.broadcast_to(lt[:, j:j + 1], (8, LANES))
        for off in LINE_OFFS:
            j = (j0 + off) % 8
            send(s3l.at[w, k, j], r3l.at[w, k, j0], r3l_s, r3l_r.at[w, k], line(a1, j))
        wait(obuf.at[pl.ds(0, 3 * n)], r2_r.at[w, k])
        ys = []
        for i in its:
            y = r1m[k, co[a2], i].astype(F32) * cols(0, i - its[0])
            for x in KS:
                y = y + r2d[k, x, i].astype(F32) * cols(1 + x, i - its[0])
            ys.append(y)
        y = jnp.concatenate(ys, axis=0).astype(BF16)
        pm = _perm(64, 8 * n, lambda r, c: (c == (r % 8) * 8 + r // 8) & (r % 8 < n))
        s3src[w, k] = jnp.dot(pm, y, preferred_element_type=F32).astype(BF16).reshape(8, 8, LAT)
        for off in LINE_OFFS:
            j = (j0 + off) % 8
            send(s3src.at[w, k, j], r3d.at[w, k, j0], r3_s, r3_r.at[w, k], line(a1, j))
        r3d[w, k, j0] = s3src[w, k, j0]
        r3l[w, k, j0] = s3l[w, k, j0]

    rows = {}

    def merge3(w, k):
        wait(r3l.at[w, k, pl.ds(0, 7)], r3l_r.at[w, k])
        wait(r3d.at[w, k, pl.ds(0, 7)], r3_r.at[w, k])
        for h in DIRS:
            ws, _ = _merge_weights([r3l[w, k, 2 * p + h] for p in RING])
            y = None
            for p in RING:
                t = r3d[w, k, 2 * p + h].astype(F32) * jnp.concatenate([ws[p]] * 4, axis=1)
                y = t if y is None else y + t
            rows[w, h, k] = y

    for k in KS:
        merge1(0, k)
    for k in KS:
        merge1(1, k)
    for k in KS:
        merge2(0, k)
    for k in KS:
        merge2(1, k)
    for k in KS:
        merge3(0, k)
    for k in KS:
        merge3(1, k)
    flat = jnp.concatenate([rows[w, h, k] for w in DIRS for h in DIRS for k in KS], axis=0).astype(BF16)

    def pick(r, c):
        w, h, k, i = c // 48, (c // 24) % 2, (c // 8) % 3, c % 8
        s = 3 * (i + w * SPLIT) + k
        return (r == 16 * h + s) & (s < 16) & (i < SPLIT)

    oout[...] = jnp.dot(_perm(32, 96, pick), flat, preferred_element_type=F32).astype(BF16)
    store = pltpu.make_async_copy(oout, o_h, sem_o)
    store.start()

    wait(cbuf.at[pl.ds(0, 8)], c_s)
    for k in KS:
        wait(s1buf.at[k, pl.ds(0, 7)], s1_s.at[k])
    for par in DIRS:
        its = [i for i in range(NI) for _ in ks_of(i) if i % 2 == par]
        wait(q_of(par).at[pl.ds(0, 3 * len(its))], s2_s.at[par])
        wait(q_of(par).at[pl.ds(0, sum(12 if i < DIRECT else 8 for i in its))], s3_s.at[par])
        wait(q_of(par).at[pl.ds(0, sum(0 if i < DIRECT else 4 for i in its))], sf_s.at[par])
    wait(obuf.at[pl.ds(0, 192)], r1_s)
    wait(r1l, r1l_s)
    wait(obuf.at[pl.ds(0, 48)], r2_s)
    wait(r2l, r2l_s)
    for w in DIRS:
        for k in KS:
            wait(r3d.at[w, k, pl.ds(0, 7)], r3_s)
            wait(r3l.at[w, k, pl.ds(0, 7)], r3l_s)
    store.wait()


def solution(mesh):
    def local(q, cache, lens):
        dma = pltpu.SemaphoreType.DMA
        V = pltpu.VMEM
        anyspace = pl.BlockSpec(memory_space=pl.ANY)
        tile, qtile, row = (8, LAT), (8, QW), (8, LANES)
        line = (2, 3, 8)
        scratch = [
            pltpu.SMEM((32,), jnp.int32), V((32, QW), BF16), V((2, 3) + qtile, BF16), V((3, 8) + qtile, BF16),
            V((144, 8, LAT + LANES), BF16), V((144,) + tile, BF16),
            V((16, 64) + qtile, BF16), V((288,) + tile, BF16), V((2, 3) + row, F32), V((LANES, LANES), F32),
            V((3, NI, 3, 4) + tile, BF16), V((2, 3, 3) + row, F32), V((3, 4, NI) + tile, BF16), V((2, 3) + row, F32),
            V((3, 3, NI) + tile, BF16), V((2, 3, 3) + row, F32),
            V(line + tile, BF16), V(line + row, F32), V(line + tile, BF16), V(line + row, F32),
            V((32, LAT), BF16),
            dma, dma, dma, dma, dma((NI,)), dma((3,)), dma((3,)), dma((2,)), dma((NI,)),
            dma((2,)), dma((NI,)), dma((NI,)), dma((2,)),
            dma, dma((2, 3)), dma, dma((2, 3)), dma, dma((2, 3)), dma, dma((2, 3)),
            dma, dma((2, 3)), dma, dma((2, 3)),
        ]
        o = pl.pallas_call(
            _kernel,
            out_shape=jax.ShapeDtypeStruct((32, LAT), BF16),
            in_specs=[anyspace] * 3,
            out_specs=anyspace,
            scratch_shapes=scratch,
            compiler_params=pltpu.CompilerParams(collective_id=0, has_side_effects=True,
                                                 vmem_limit_bytes=58 * 2 ** 20),
        )(lens, q.reshape(32, QW), cache.reshape(32, 32, 8, QW))
        return o.reshape(32, 1, LAT)

    return jax.shard_map(local, mesh=mesh,
                         in_specs=(P('dp', 'dcp', None), P('dp', None, 'dcp', None, None), P('dp')),
                         out_specs=P('dp', 'dcp', None), check_vma=False)
```

```python
import functools
import math

import jax
import jax.numpy as jnp
from jax import lax
from jax.experimental import pallas as pl
from jax.experimental.pallas import tpu as pltpu
from jax.sharding import PartitionSpec as P

ROPE = 64
QK_DIM = 192
SCALE2 = QK_DIM ** -0.5 * math.log2(math.e)
NEG = -3.0e38
MESH = pl.DeviceIdType.MESH
F32 = jnp.float32
BF16 = jnp.bfloat16

STRIDE = (2, 8, 32)
ORDERS = ((0, 1, 2), (1, 2, 0), (2, 0, 1))
COUNT = (6, 5, 5)
NI = 6
SPLIT, RELAYED = 3, 3


LAT, QW, LANES = 512, 576, 128
KS, DIRS, RING, RING_OFFS, LINE_OFFS = range(3), range(2), range(4), range(1, 4), range(1, 8)


def _perm(rows, cols, f):
    r = lax.broadcasted_iota(jnp.int32, (rows, cols), 0)
    c = lax.broadcasted_iota(jnp.int32, (rows, cols), 1)
    return f(r, c).astype(F32).astype(BF16)


def _merge_weights(lses):
    top = functools.reduce(jnp.maximum, lses)
    ws = [jnp.exp2(v - top) for v in lses]
    tot = functools.reduce(jnp.add, ws)
    inv = 1.0 / tot
    return [w * inv for w in ws], top + jnp.log2(tot)


def _kernel(lens_h, q_h, c_h, o_h,
            lens, q_in, s1src, s1buf, q_even, q_odd, cbuf, obuf, lrow, wcol, r1d, r1l, r1m, lse1,
            r2d, r2l, s3src, s3l, r3d, r3l, oout,
            sem_l, sem_q, sem_o, c_s, c_r, s1_s, s1_r, s2_s, s2_r, s3_s, s3f_r, s3_r, sf_s,
            r1_s, r1_r, r1l_s, r1l_r, r2_s, r2_r, r2l_s, r2l_r, r3_s, r3_r, r3l_s, r3l_r):
    d = lax.axis_index('dcp')
    core = d % 2
    co = ((d // 2) % 4, (d // 8) % 4, d // 32)
    partner = {'dcp': d + 1 - 2 * core}

    def ring(axis, off):
        return {'dcp': d + ((co[axis] + off) % 4 - co[axis]) * STRIDE[axis]}

    def line(axis, j):
        return {'dcp': d + (j // 2 - co[axis]) * STRIDE[axis] + (j % 2 - core)}

    def send(src, dst, ss, rs, dev):
        pltpu.make_async_remote_copy(src_ref=src, dst_ref=dst, send_sem=ss, recv_sem=rs,
                                     device_id=dev, device_id_type=MESH).start()

    def wait(ref, sem):
        pltpu.make_async_copy(ref, ref, sem).wait()

    def ks_of(i):
        return KS if i < NI - 1 else range(1)

    load_q = pltpu.make_async_copy(q_h, q_in, sem_q)
    load_q.start()
    load_l = pltpu.make_async_copy(lens_h, lens, sem_l)
    load_l.start()

    def cache_rows(i, half):
        n = len(ks_of(i))
        return c_h.at[pl.ds(16 * half + 3 * i, n)], cbuf.at[pl.ds(3 * i, n), pl.ds(32 * core, 32)]

    for i in range(NI):
        src, dst = cache_rows(i, core)
        pltpu.make_async_copy(src, dst, c_r.at[i]).start()

    bar = pltpu.get_barrier_semaphore()
    pl.semaphore_signal(bar, inc=1, device_id=partner, device_id_type=MESH)
    for a in KS:
        for off in RING_OFFS:
            for c2 in DIRS:
                pl.semaphore_signal(bar, inc=1, device_id=line(a, ((co[a] + off) % 4) * 2 + c2), device_id_type=MESH)
    lrow[...] = jnp.zeros_like(lrow)
    load_l.wait()

    def sel(r, c):
        s = 3 * (r % 8) + (r // 8) % 3
        return (c == 16 * (r // 24) + s) & (s < 16)

    load_q.wait()
    qp = jnp.dot(_perm(48, 32, sel), q_in[...], preferred_element_type=F32).astype(BF16)
    s1src[...] = qp.reshape(2, 3, 8, QW)
    pl.semaphore_wait(bar, 19)

    def place(k):
        return co[ORDERS[k][0]] * 2 + core

    for k in KS:
        j0 = place(k)
        for off in LINE_OFFS:
            j = (j0 + off) % 8
            send(s1src.at[j % 2, k], s1buf.at[k, j0], s1_s.at[k], s1_r.at[k], line(ORDERS[k][0], j))
        s1buf[k, j0] = s1src[core, k]
    for i in range(NI):
        src, dst = cache_rows(i, 1 - core)
        send(src, dst, c_s, c_r.at[i], partner)

    def q_of(i):
        return q_odd if i % 2 else q_even

    def q_slot(k, i):
        return (k * 3 + i // 2) * 16

    def slot(k, i):
        return (k * NI + i) * 16

    def blk(k, i, off):
        _, a2, a3 = ORDERS[k]
        return q_of(i).at[q_slot(k, i) + co[a3] * 4 + (co[a2] - off) % 4]

    def copy3(k, i, off):
        b = blk(k, i, off)
        a3 = ORDERS[k][2]
        for o in (2, 1, 3) if i < RELAYED else (1, 3):
            onward = i >= RELAYED and off // 2 == o // 2
            send(b, b, s3_s.at[i % 2], s3f_r.at[i] if onward else s3_r.at[i], ring(a3, o))

    def stage2(k, i):
        b = blk(k, i, 0)
        for off in (2, 1, 3):
            send(b, b, s2_s.at[i % 2], s2_r.at[i], ring(ORDERS[k][1], off))
        copy3(k, i, 0)

    tr = _perm(64, 64, lambda r, c: (r // 8 == c % 8) & (r % 8 == c // 8))
    for k in KS:
        wait(s1buf.at[k, pl.ds(0, 7)], s1_r.at[k])
        rows = jnp.dot(tr, s1buf[k].reshape(64, QW), preferred_element_type=F32)
        _, a2, a3 = ORDERS[k]
        for i in range(COUNT[k]):
            y = rows[8 * i:8 * i + 8, :LAT if i % 2 else QW]
            if i % 2 == 0:
                y = jnp.concatenate([y, rows[8 * i + 8:8 * i + 16, LAT:]], axis=1)
            q_of(i)[q_slot(k, i) + co[a3] * 4 + co[a2]] = y.astype(BF16)
        for i in range(COUNT[k]):
            stage2(k, i)

    def stage3(i):
        n = len(ks_of(i))
        wait(q_of(i).at[pl.ds(0, 3 * n)], s2_r.at[i])
        for off in (1, 3, 2):
            for k in ks_of(i):
                copy3(k, i, off)

    def forward(i):
        wait(q_of(i).at[pl.ds(0, 4 * len(ks_of(i)))], s3f_r.at[i])
        for off in RING:
            for k in ks_of(i):
                _, a2, a3 = ORDERS[k]
                o = 1 if off < 2 else 3
                b = q_of(i).at[q_slot(k, i) + ((co[a3] - o) % 4) * 4 + (co[a2] - off) % 4]
                send(b, b, sf_s.at[i % 2], s3_r.at[i], ring(a3, o))

    def arrive(i):
        n = len(ks_of(i))
        wait(cbuf.at[pl.ds(0, n)], c_r.at[i])
        wait(q_of(i).at[pl.ds(0, (12 if i < RELAYED else 8) * n)], s3_r.at[i])

    for i in range(NI):
        stage3(i)

    chip8 = (d // 2) * 16

    j = lax.broadcasted_iota(jnp.int32, (LAT, LANES), 0)
    pos = (j & 7) + ((j >> 3) & 31) * 1024 + (j >> 8) * 8

    def cache_of(k, i):
        return cbuf[3 * i + k].reshape(LAT, QW)

    def scores(k, i):
        cs = cache_of(k, i)
        n = pl.ds(q_slot(k, i), 16)
        lat = q_of(i)[n, :, :LAT].reshape(LANES, LAT)
        rope = q_even[n, :, LAT:].reshape(LANES, LANES)
        rope = rope[:, ROPE:] if i % 2 else rope[:, :ROPE]
        dims = (((1,), (1,)), ((), ()))
        st = lax.dot_general(cs[:, :LAT], lat, dims, preferred_element_type=F32)
        return (st + lax.dot_general(cs[:, LAT:], rope, dims, preferred_element_type=F32)) * SCALE2

    def softmax(st, k, i):
        ok = pos < lens[16 * core + 3 * i + k] - chip8
        st = jnp.where(ok, st, NEG)
        m = jnp.max(st, axis=0, keepdims=True)
        p = jnp.where(ok, jnp.exp2(st - m), 0.0)
        l = jnp.sum(p, axis=0, keepdims=True)
        has = l > 0.0
        ls = jnp.where(has, l, 1.0)
        w = wave(i)
        lrow[w, k, i - w * SPLIT:i - w * SPLIT + 1, :] = jnp.where(has, m + jnp.log2(ls), NEG)
        return (p * (1.0 / ls)).astype(BF16)

    def attend(i):
        ks = ks_of(i)
        sts = [scores(k, i) for k in ks]
        ps = [softmax(st, k, i) for st, k in zip(sts, ks)]
        outs = [lax.dot_general(p, cache_of(k, i)[:, :LAT], (((0,), (0,)), ((), ())), preferred_element_type=F32)
                for p, k in zip(ps, ks)]
        for o, k in zip(outs, ks):
            obuf[pl.ds(slot(k, i), 16)] = o.astype(BF16).reshape(16, 8, LAT)

    def wave(i):
        return 0 if i < SPLIT else 1

    def send1(k, i):
        a3 = ORDERS[k][2]
        for o in (2, 1, 3):
            b = obuf.at[pl.ds(slot(k, i) + ((co[a3] + o) % 4) * 4, 4)]
            send(b, r1d.at[k, i, o - 1], r1_s, r1_r.at[wave(i), k], ring(a3, o))

    def members(w, k):
        return range(SPLIT) if w == 0 else range(SPLIT, COUNT[k])

    def send1_lse(w):
        for k in KS:
            for o in RING_OFFS:
                send(lrow.at[w, k], r1l.at[w, k, o - 1], r1l_s, r1l_r.at[w, k], ring(ORDERS[k][2], o))

    for i in range(NI):
        with jax.named_scope(f"arrive{i}"):
            arrive(i)
        with jax.named_scope(f"attend{i}"):
            attend(i)
            for k in ks_of(i):
                send1(k, i)
        with jax.named_scope(f"rest{i}"):
            if i == SPLIT - 1:
                send1_lse(0)
            if i == 1:
                for x in range(RELAYED, NI):
                    forward(x)

    send1_lse(1)

    def columns(ws, row, n):
        wcol[:, :32] = jnp.concatenate(ws, axis=0).T
        t = wcol[pl.ds(row, n), :32]
        return lambda x, i: t[:, 8 * x + i:8 * x + i + 1]

    def merge1(w, k):
        a2, a3 = ORDERS[k][1:]
        its = members(w, k)
        wait(r1l.at[w, k], r1l_r.at[w, k])
        ws, lse1[w, k] = _merge_weights([lrow[w, k]] + [r1l[w, k, x] for x in KS])
        for o in RING_OFFS:
            send(lse1.at[w, k], r2l.at[w, k, o - 1], r2l_s, r2l_r.at[w, k], ring(a2, o))
        cols = columns(ws, co[a3] * 32, 32)
        wait(obuf.at[pl.ds(0, 12 * len(its))], r1_r.at[w, k])
        for i in its:
            y = obuf[pl.ds(slot(k, i) + co[a3] * 4, 4)].reshape(32, LAT).astype(F32) * cols(0, i - its[0])
            for x in KS:
                y = y + r1d[k, i, x].reshape(32, LAT).astype(F32) * cols(1 + x, i - its[0])
            y = y.astype(BF16).reshape(4, 8, LAT)
            for p in RING:
                r1m[k, p, i] = y[p]
        for o in (2, 1, 3):
            p = (co[a2] + o) % 4
            sl = pl.ds(its[0], len(its))
            send(r1m.at[k, p, sl], r2d.at[k, o - 1, sl], r2_s, r2_r.at[w, k], ring(a2, o))

    def merge2(w, k):
        a1, a2, a3 = ORDERS[k]
        its = members(w, k)
        n = len(its)
        j0 = place(k)
        wait(r2l.at[w, k], r2l_r.at[w, k])
        ws, l2 = _merge_weights([lse1[w, k]] + [r2l[w, k, x] for x in KS])
        g = co[a3] * 4 + co[a2]
        lt = pltpu.roll(l2, ((16 - g) % 16) * 8, 1)
        cols = columns(ws, g * 8, 8)
        for j in range(8):
            s3l[w, k, j] = jnp.broadcast_to(lt[:, j:j + 1], (8, LANES))
        for off in LINE_OFFS:
            j = (j0 + off) % 8
            send(s3l.at[w, k, j], r3l.at[w, k, j0], r3l_s, r3l_r.at[w, k], line(a1, j))
        wait(obuf.at[pl.ds(0, 3 * n)], r2_r.at[w, k])
        ys = []
        for i in its:
            y = r1m[k, co[a2], i].astype(F32) * cols(0, i - its[0])
            for x in KS:
                y = y + r2d[k, x, i].astype(F32) * cols(1 + x, i - its[0])
            ys.append(y)
        y = jnp.concatenate(ys, axis=0).astype(BF16)
        pm = _perm(64, 8 * n, lambda r, c: (c == (r % 8) * 8 + r // 8) & (r % 8 < n))
        s3src[w, k] = jnp.dot(pm, y, preferred_element_type=F32).astype(BF16).reshape(8, 8, LAT)
        for off in LINE_OFFS:
            j = (j0 + off) % 8
            send(s3src.at[w, k, j], r3d.at[w, k, j0], r3_s, r3_r.at[w, k], line(a1, j))
        r3d[w, k, j0] = s3src[w, k, j0]
        r3l[w, k, j0] = s3l[w, k, j0]

    rows = {}

    def merge3(w, k):
        wait(r3l.at[w, k, pl.ds(0, 7)], r3l_r.at[w, k])
        wait(r3d.at[w, k, pl.ds(0, 7)], r3_r.at[w, k])
        for h in DIRS:
            ws, _ = _merge_weights([r3l[w, k, 2 * p + h] for p in RING])
            y = None
            for p in RING:
                t = r3d[w, k, 2 * p + h].astype(F32) * jnp.concatenate([ws[p]] * 4, axis=1)
                y = t if y is None else y + t
            rows[w, h, k] = y

    for k in KS:
        merge1(0, k)
    for k in KS:
        merge1(1, k)
    for k in KS:
        merge2(0, k)
    wait(cbuf.at[pl.ds(0, 8)], c_s)
    for k in KS:
        wait(s1buf.at[k, pl.ds(0, 7)], s1_s.at[k])
    for par in DIRS:
        its = [i for i in range(NI) for _ in ks_of(i) if i % 2 == par]
        wait(q_of(par).at[pl.ds(0, 3 * len(its))], s2_s.at[par])
        wait(q_of(par).at[pl.ds(0, sum(12 if i < RELAYED else 8 for i in its))], s3_s.at[par])
        wait(q_of(par).at[pl.ds(0, sum(0 if i < RELAYED else 4 for i in its))], sf_s.at[par])
    for k in KS:
        merge2(1, k)
    for k in KS:
        merge3(0, k)
    wait(obuf.at[pl.ds(0, 192)], r1_s)
    wait(r1l, r1l_s)
    wait(obuf.at[pl.ds(0, 48)], r2_s)
    wait(r2l, r2l_s)
    for k in KS:
        merge3(1, k)
    flat = jnp.concatenate([rows[w, h, k] for w in DIRS for h in DIRS for k in KS], axis=0).astype(BF16)

    def pick(r, c):
        w, h, k, i = c // 48, (c // 24) % 2, (c // 8) % 3, c % 8
        s = 3 * (i + w * SPLIT) + k
        return (r == 16 * h + s) & (s < 16) & (i < SPLIT)

    oout[...] = jnp.dot(_perm(32, 96, pick), flat, preferred_element_type=F32).astype(BF16)
    store = pltpu.make_async_copy(oout, o_h, sem_o)
    store.start()

    for w in DIRS:
        for k in KS:
            wait(r3d.at[w, k, pl.ds(0, 7)], r3_s)
            wait(r3l.at[w, k, pl.ds(0, 7)], r3l_s)
    store.wait()


def solution(mesh):
    def local(q, cache, lens):
        dma = pltpu.SemaphoreType.DMA
        V = pltpu.VMEM
        anyspace = pl.BlockSpec(memory_space=pl.ANY)
        tile, qtile, row = (8, LAT), (8, QW), (8, LANES)
        line = (2, 3, 8)
        scratch = [
            pltpu.SMEM((32,), jnp.int32), V((32, QW), BF16), V((2, 3) + qtile, BF16), V((3, 8) + qtile, BF16),
            V((144, 8, LAT + LANES), BF16), V((144,) + tile, BF16),
            V((16, 64) + qtile, BF16), V((288,) + tile, BF16), V((2, 3) + row, F32), V((LANES, LANES), F32),
            V((3, NI, 3, 4) + tile, BF16), V((2, 3, 3) + row, F32), V((3, 4, NI) + tile, BF16), V((2, 3) + row, F32),
            V((3, 3, NI) + tile, BF16), V((2, 3, 3) + row, F32),
            V(line + tile, BF16), V(line + row, F32), V(line + tile, BF16), V(line + row, F32),
            V((32, LAT), BF16),
            dma, dma, dma, dma, dma((NI,)), dma((3,)), dma((3,)), dma((2,)), dma((NI,)),
            dma((2,)), dma((NI,)), dma((NI,)), dma((2,)),
            dma, dma((2, 3)), dma, dma((2, 3)), dma, dma((2, 3)), dma, dma((2, 3)),
            dma, dma((2, 3)), dma, dma((2, 3)),
        ]
        o = pl.pallas_call(
            _kernel,
            out_shape=jax.ShapeDtypeStruct((32, LAT), BF16),
            in_specs=[anyspace] * 3,
            out_specs=anyspace,
            scratch_shapes=scratch,
            compiler_params=pltpu.CompilerParams(collective_id=0, has_side_effects=True,
                                                 vmem_limit_bytes=58 * 2 ** 20),
        )(lens, q.reshape(32, QW), cache.reshape(32, 32, 8, QW))
        return o.reshape(32, 1, LAT)

    return jax.shard_map(local, mesh=mesh,
                         in_specs=(P('dp', 'dcp', None), P('dp', None, 'dcp', None, None), P('dp')),
                         out_specs=P('dp', 'dcp', None), check_vma=False)
```

```python
import functools
import math

import jax
import jax.numpy as jnp
from jax import lax
from jax.experimental import pallas as pl
from jax.experimental.pallas import tpu as pltpu
from jax.sharding import PartitionSpec as P

ROPE = 64
QK_DIM = 192
SCALE2 = QK_DIM ** -0.5 * math.log2(math.e)
NEG = -3.0e38
MESH = pl.DeviceIdType.MESH
F32 = jnp.float32
BF16 = jnp.bfloat16

STRIDE = (2, 8, 32)
ORDERS = ((0, 1, 2), (1, 2, 0), (2, 0, 1))
COUNT = (6, 5, 5)
NI = 6
SPLIT, RELAYED = 3, 3


LAT, QW, LANES = 512, 576, 128
KS, DIRS, RING, RING_OFFS, LINE_OFFS = range(3), range(2), range(4), range(1, 4), range(1, 8)


def _perm(rows, cols, f):
    r = lax.broadcasted_iota(jnp.int32, (rows, cols), 0)
    c = lax.broadcasted_iota(jnp.int32, (rows, cols), 1)
    return f(r, c).astype(F32).astype(BF16)


def _merge_weights(lses):
    top = functools.reduce(jnp.maximum, lses)
    ws = [jnp.exp2(v - top) for v in lses]
    tot = functools.reduce(jnp.add, ws)
    inv = 1.0 / tot
    return [w * inv for w in ws], top + jnp.log2(tot)


def _kernel(lens_h, q_h, c_h, o_ref,
            lens, q_in, s1src, s1buf, q_even, q_odd, cbuf, obuf, lrow, wcol, r1d, r1l, r1m, lse1,
            r2d, r2l, s3src, s3l, r3d, r3l,
            sem_l, sem_q, c_s, c_r, s1_s, s1_r, s2_s, s2_r, s3_s, s3f_r, s3_r, sf_s,
            r1_s, r1_r, r1l_s, r1l_r, r2_s, r2_r, r2l_s, r2l_r, r3_s, r3_r, r3l_s, r3l_r):
    d = lax.axis_index('dcp')
    core = d % 2
    co = ((d // 2) % 4, (d // 8) % 4, d // 32)
    partner = {'dcp': d + 1 - 2 * core}

    nxt = (1, 2, 0)
    ac = [co[n] + core * (co[nxt[n]] - co[n]) for n in KS]
    stride = [STRIDE[n] + core * (STRIDE[nxt[n]] - STRIDE[n]) for n in KS]

    def ring(axis, off):
        return {'dcp': d + ((ac[axis] + off) % 4 - ac[axis]) * stride[axis]}

    def line(axis, j):
        return {'dcp': d + (j // 2 - ac[axis]) * stride[axis] + (j % 2 - core)}

    def send(src, dst, ss, rs, dev):
        pltpu.make_async_remote_copy(src_ref=src, dst_ref=dst, send_sem=ss, recv_sem=rs,
                                     device_id=dev, device_id_type=MESH).start()

    def wait(ref, sem):
        pltpu.make_async_copy(ref, ref, sem).wait()

    def ks_of(i):
        return KS if i < NI - 1 else range(1)

    load_q = pltpu.make_async_copy(q_h, q_in, sem_q)
    load_q.start()
    load_l = pltpu.make_async_copy(lens_h, lens, sem_l)
    load_l.start()

    def cache_rows(i, half):
        n = len(ks_of(i))
        return c_h.at[pl.ds(16 * half + 3 * i, n)], cbuf.at[pl.ds(3 * i, n), pl.ds(32 * core, 32)]

    for i in range(NI):
        src, dst = cache_rows(i, core)
        pltpu.make_async_copy(src, dst, c_r.at[i]).start()

    bar = pltpu.get_barrier_semaphore()
    pl.semaphore_signal(bar, inc=1, device_id=partner, device_id_type=MESH)
    for a in KS:
        for off in RING_OFFS:
            for c2 in DIRS:
                peer = d + ((co[a] + off) % 4 - co[a]) * STRIDE[a] + c2 - core
                pl.semaphore_signal(bar, inc=1, device_id={'dcp': peer}, device_id_type=MESH)
    lrow[...] = jnp.zeros_like(lrow)
    load_l.wait()

    def sel(r, c):
        s = 3 * (r % 8) + (r // 8) % 3
        return (c == 16 * (r // 24) + s) & (s < 16)

    load_q.wait()
    qp = jnp.dot(_perm(48, 32, sel), q_in[...], preferred_element_type=F32).astype(BF16)
    s1src[...] = qp.reshape(2, 3, 8, QW)
    pl.semaphore_wait(bar, 19)

    def place(k):
        return ac[ORDERS[k][0]] * 2 + core

    for k in KS:
        n = ORDERS[k][0]
        j0 = place(k)
        oc = co[n] + co[nxt[n]] - ac[n]
        ost = STRIDE[n] + STRIDE[nxt[n]] - stride[n]
        for off in (2, 1, 3):
            send(s1src.at[core, k], s1buf.at[k, j0], s1_s.at[k], s1_r.at[k], ring(n, off))
        for off in (2, 1, 3, 0):
            peer = {'dcp': d + ((oc + off) % 4 - oc) * ost + 1 - 2 * core}
            send(s1src.at[1 - core, k], s1buf.at[k, oc * 2 + core], s1_s.at[k], s1_r.at[k], peer)
        s1buf[k, j0] = s1src[core, k]
    for i in range(NI):
        src, dst = cache_rows(i, 1 - core)
        send(src, dst, c_s, c_r.at[i], partner)

    def q_of(i):
        return q_odd if i % 2 else q_even

    def q_slot(k, i):
        return (k * 3 + i // 2) * 16

    def slot(k, i):
        return (k * NI + i) * 16

    def blk(k, i, off):
        _, a2, a3 = ORDERS[k]
        return q_of(i).at[q_slot(k, i) + ac[a3] * 4 + (ac[a2] - off) % 4]

    def copy3(k, i, off):
        b = blk(k, i, off)
        a3 = ORDERS[k][2]
        for o in (2, 1, 3) if i < RELAYED else (1, 3):
            onward = i >= RELAYED and off // 2 == o // 2
            send(b, b, s3_s.at[i % 2], s3f_r.at[i] if onward else s3_r.at[i], ring(a3, o))

    def stage2(k, i):
        b = blk(k, i, 0)
        for off in (2, 1, 3):
            send(b, b, s2_s.at[i % 2], s2_r.at[i], ring(ORDERS[k][1], off))
        copy3(k, i, 0)

    tr = _perm(64, 64, lambda r, c: (r // 8 == c % 8) & (r % 8 == c // 8))
    for k in KS:
        wait(s1buf.at[k, pl.ds(0, 7)], s1_r.at[k])
        rows = jnp.dot(tr, s1buf[k].reshape(64, QW), preferred_element_type=F32)
        _, a2, a3 = ORDERS[k]
        for i in range(COUNT[k]):
            y = rows[8 * i:8 * i + 8, :LAT if i % 2 else QW]
            if i % 2 == 0:
                y = jnp.concatenate([y, rows[8 * i + 8:8 * i + 16, LAT:]], axis=1)
            q_of(i)[q_slot(k, i) + ac[a3] * 4 + ac[a2]] = y.astype(BF16)
        stage2(k, 0)
    for i in range(1, NI):
        for k in ks_of(i):
            stage2(k, i)

    def stage3(i):
        n = len(ks_of(i))
        wait(q_of(i).at[pl.ds(0, 3 * n)], s2_r.at[i])
        for off in (1, 3, 2):
            for k in ks_of(i):
                copy3(k, i, off)

    def forward(i):
        wait(q_of(i).at[pl.ds(0, 4 * len(ks_of(i)))], s3f_r.at[i])
        for off in RING:
            for k in ks_of(i):
                _, a2, a3 = ORDERS[k]
                o = 1 if off < 2 else 3
                b = q_of(i).at[q_slot(k, i) + ((ac[a3] - o) % 4) * 4 + (ac[a2] - off) % 4]
                send(b, b, sf_s.at[i % 2], s3_r.at[i], ring(a3, o))

    def arrive(i):
        n = len(ks_of(i))
        wait(cbuf.at[pl.ds(0, n)], c_r.at[i])
        wait(q_of(i).at[pl.ds(0, (12 if i < RELAYED else 8) * n)], s3_r.at[i])

    for i in range(NI):
        stage3(i)

    chip8 = (d // 2) * 16

    j = lax.broadcasted_iota(jnp.int32, (LAT, LANES), 0)
    pos = (j & 7) + ((j >> 3) & 31) * 1024 + (j >> 8) * 8

    def cache_of(k, i):
        return cbuf[3 * i + k].reshape(LAT, QW)

    def scores(k, i):
        cs = cache_of(k, i)
        n = pl.ds(q_slot(k, i), 16)
        lat = q_of(i)[n, :, :LAT].reshape(LANES, LAT)
        rope = q_even[n, :, LAT:].reshape(LANES, LANES)
        rope = rope[:, ROPE:] if i % 2 else rope[:, :ROPE]
        dims = (((1,), (1,)), ((), ()))
        st = lax.dot_general(cs[:, :LAT], lat, dims, preferred_element_type=F32)
        return (st + lax.dot_general(cs[:, LAT:], rope, dims, preferred_element_type=F32)) * SCALE2

    def softmax(st, k, i):
        ok = pos < lens[16 * core + 3 * i + k] - chip8
        st = jnp.where(ok, st, NEG)
        m = jnp.max(st, axis=0, keepdims=True)
        p = jnp.where(ok, jnp.exp2(st - m), 0.0)
        l = jnp.sum(p, axis=0, keepdims=True)
        has = l > 0.0
        ls = jnp.where(has, l, 1.0)
        w = wave(i)
        lrow[w, k, i - w * SPLIT:i - w * SPLIT + 1, :] = jnp.where(has, m + jnp.log2(ls), NEG)
        return (p * (1.0 / ls)).astype(BF16)

    def attend(i):
        ks = ks_of(i)
        sts = [scores(k, i) for k in ks]
        ps = [softmax(st, k, i) for st, k in zip(sts, ks)]
        outs = [lax.dot_general(p, cache_of(k, i)[:, :LAT], (((0,), (0,)), ((), ())), preferred_element_type=F32)
                for p, k in zip(ps, ks)]
        for o, k in zip(outs, ks):
            obuf[pl.ds(slot(k, i), 16)] = o.astype(BF16).reshape(16, 8, LAT)

    def wave(i):
        return 0 if i < SPLIT else 1

    def send1(k, i):
        a3 = ORDERS[k][2]
        for o in (2, 1, 3):
            b = obuf.at[pl.ds(slot(k, i) + ((ac[a3] + o) % 4) * 4, 4)]
            send(b, r1d.at[k, i, o - 1], r1_s, r1_r.at[wave(i), k], ring(a3, o))

    def members(w, k):
        return range(SPLIT) if w == 0 else range(SPLIT, COUNT[k])

    def send1_lse(w):
        for k in KS:
            for o in RING_OFFS:
                send(lrow.at[w, k], r1l.at[w, k, o - 1], r1l_s, r1l_r.at[w, k], ring(ORDERS[k][2], o))

    for i in range(NI):
        with jax.named_scope(f"arrive{i}"):
            arrive(i)
        with jax.named_scope(f"attend{i}"):
            attend(i)
            for k in ks_of(i):
                send1(k, i)
        with jax.named_scope(f"rest{i}"):
            if i == SPLIT - 1:
                send1_lse(0)
            if i == 1:
                for x in range(RELAYED, NI):
                    forward(x)

    send1_lse(1)

    def columns(ws, row, n):
        wcol[:, :32] = jnp.concatenate(ws, axis=0).T
        t = wcol[pl.ds(row, n), :32]
        return lambda x, i: t[:, 8 * x + i:8 * x + i + 1]

    def merge1(w, k):
        a2, a3 = ORDERS[k][1:]
        its = members(w, k)
        wait(r1l.at[w, k], r1l_r.at[w, k])
        ws, lse1[w, k] = _merge_weights([lrow[w, k]] + [r1l[w, k, x] for x in KS])
        for o in RING_OFFS:
            send(lse1.at[w, k], r2l.at[w, k, o - 1], r2l_s, r2l_r.at[w, k], ring(a2, o))
        cols = columns(ws, ac[a3] * 32, 32)
        wait(obuf.at[pl.ds(0, 12 * len(its))], r1_r.at[w, k])
        for i in its:
            y = obuf[pl.ds(slot(k, i) + ac[a3] * 4, 4)].reshape(32, LAT).astype(F32) * cols(0, i - its[0])
            for x in KS:
                y = y + r1d[k, i, x].reshape(32, LAT).astype(F32) * cols(1 + x, i - its[0])
            y = y.astype(BF16).reshape(4, 8, LAT)
            for p in RING:
                r1m[k, p, i] = y[p]
        for o in (2, 1, 3):
            p = (ac[a2] + o) % 4
            sl = pl.ds(its[0], len(its))
            send(r1m.at[k, p, sl], r2d.at[k, o - 1, sl], r2_s, r2_r.at[w, k], ring(a2, o))

    def merge2(w, k):
        a1, a2, a3 = ORDERS[k]
        its = members(w, k)
        n = len(its)
        j0 = place(k)
        wait(r2l.at[w, k], r2l_r.at[w, k])
        ws, l2 = _merge_weights([lse1[w, k]] + [r2l[w, k, x] for x in KS])
        g = ac[a3] * 4 + ac[a2]
        lt = pltpu.roll(l2, ((16 - g) % 16) * 8, 1)
        s3l[w, k] = jnp.concatenate([lt] * 16, axis=0).T[0:8].reshape(8, 1, LANES)
        cols = columns(ws, g * 8, 8)
        for off in LINE_OFFS:
            j = (j0 + off) % 8
            send(s3l.at[w, k, j], r3l.at[w, k, j0], r3l_s, r3l_r.at[w, k], line(a1, j))
        wait(obuf.at[pl.ds(0, 3 * n)], r2_r.at[w, k])
        ys = []
        for i in its:
            y = r1m[k, ac[a2], i].astype(F32) * cols(0, i - its[0])
            for x in KS:
                y = y + r2d[k, x, i].astype(F32) * cols(1 + x, i - its[0])
            ys.append(y)
        y = jnp.concatenate(ys, axis=0).astype(BF16)
        pm = _perm(64, 8 * n, lambda r, c: (c == (r % 8) * 8 + r // 8) & (r % 8 < n))
        s3src[w, k] = jnp.dot(pm, y, preferred_element_type=F32).astype(BF16).reshape(8, 8, LAT)
        for off in LINE_OFFS:
            j = (j0 + off) % 8
            send(s3src.at[w, k, j], r3d.at[w, k, j0], r3_s, r3_r.at[w, k], line(a1, j))
        r3d[w, k, j0] = s3src[w, k, j0]
        r3l[w, k, j0] = s3l[w, k, j0]

    rows = {}

    def merge3(w, k):
        wait(r3l.at[w, k, pl.ds(0, 7)], r3l_r.at[w, k])
        wait(r3d.at[w, k, pl.ds(0, 7)], r3_r.at[w, k])
        ls = [r3l[w, k, j] for j in range(8)]
        ws = [None] * 8
        for h in DIRS:
            ws[h::2], _ = _merge_weights(ls[h::2])
        cols = jnp.concatenate(ws, axis=0).T[0:8]
        for h in DIRS:
            ts = [r3d[w, k, j].astype(F32) * cols[:, j:j + 1] for j in range(h, 8, 2)]
            rows[w, h, k] = functools.reduce(jnp.add, ts)

    for k in KS:
        merge1(0, k)
    for k in KS:
        merge1(1, k)
    for k in KS:
        merge2(0, k)
    wait(cbuf.at[pl.ds(0, 8)], c_s)
    for k in KS:
        wait(s1buf.at[k, pl.ds(0, 7)], s1_s.at[k])
    for par in DIRS:
        its = [i for i in range(NI) for _ in ks_of(i) if i % 2 == par]
        wait(q_of(par).at[pl.ds(0, 3 * len(its))], s2_s.at[par])
        wait(q_of(par).at[pl.ds(0, sum(12 if i < RELAYED else 8 for i in its))], s3_s.at[par])
        wait(q_of(par).at[pl.ds(0, sum(0 if i < RELAYED else 4 for i in its))], sf_s.at[par])
    for k in KS:
        merge2(1, k)
    for k in KS:
        merge3(0, k)
    wait(obuf.at[pl.ds(0, 192)], r1_s)
    wait(r1l, r1l_s)
    wait(obuf.at[pl.ds(0, 48)], r2_s)
    wait(r2l, r2l_s)
    for k in KS:
        merge3(1, k)
    flat = jnp.concatenate([rows[w, h, k] for w in DIRS for h in DIRS for k in KS], axis=0).astype(BF16)

    def pick(r, c):
        w, h, k, i = c // 48, (c // 24) % 2, (c // 8) % 3, c % 8
        s = 3 * (i + w * SPLIT) + k
        return (r == 16 * h + s) & (s < 16) & (i < SPLIT)

    o_ref[...] = jnp.dot(_perm(32, 96, pick), flat, preferred_element_type=F32).astype(BF16)

    for w in DIRS:
        for k in KS:
            wait(r3d.at[w, k, pl.ds(0, 7)], r3_s)
            wait(r3l.at[w, k, pl.ds(0, 7)], r3l_s)


def solution(mesh):
    def local(q, cache, lens):
        dma = pltpu.SemaphoreType.DMA
        V = pltpu.VMEM
        anyspace = pl.BlockSpec(memory_space=pl.ANY)
        tile, qtile, row = (8, LAT), (8, QW), (8, LANES)
        line = (2, 3, 8)
        scratch = [
            pltpu.SMEM((32,), jnp.int32), V((32, QW), BF16), V((2, 3) + qtile, BF16), V((3, 8) + qtile, BF16),
            V((144, 8, LAT + LANES), BF16), V((144,) + tile, BF16),
            V((16, 64) + qtile, BF16), V((288,) + tile, BF16), V((2, 3) + row, F32), V((LANES, LANES), F32),
            V((3, NI, 3, 4) + tile, BF16), V((2, 3, 3) + row, F32), V((3, 4, NI) + tile, BF16), V((2, 3) + row, F32),
            V((3, 3, NI) + tile, BF16), V((2, 3, 3) + row, F32),
            V(line + tile, BF16), V(line + (1, LANES), F32), V(line + tile, BF16), V(line + (1, LANES), F32),
            dma, dma, dma, dma((NI,)), dma((3,)), dma((3,)), dma((2,)), dma((NI,)),
            dma((2,)), dma((NI,)), dma((NI,)), dma((2,)),
            dma, dma((2, 3)), dma, dma((2, 3)), dma, dma((2, 3)), dma, dma((2, 3)),
            dma, dma((2, 3)), dma, dma((2, 3)),
        ]
        o = pl.pallas_call(
            _kernel,
            out_shape=V((32, LAT), BF16),
            in_specs=[anyspace] * 3,
            out_specs=pl.BlockSpec(memory_space=V),
            scratch_shapes=scratch,
            compiler_params=pltpu.CompilerParams(collective_id=0, has_side_effects=True,
                                                 vmem_limit_bytes=50 * 2 ** 20),
        )(*[pltpu.with_memory_space_constraint(v, pltpu.HBM) for v in (lens, q.reshape(32, QW), cache.reshape(32, 32, 8, QW))])
        return o.reshape(32, 1, LAT)

    return jax.shard_map(local, mesh=mesh,
                         in_specs=(P('dp', 'dcp', None), P('dp', None, 'dcp', None, None), P('dp')),
                         out_specs=P('dp', 'dcp', None), check_vma=False)
```

```python
import functools
import math

import jax
import jax.numpy as jnp
from jax import lax
from jax.experimental import pallas as pl
from jax.experimental.pallas import tpu as pltpu
from jax.sharding import PartitionSpec as P

ROPE = 64
QK_DIM = 192
SCALE2 = QK_DIM ** -0.5 * math.log2(math.e)
NEG = -3.0e38
MESH = pl.DeviceIdType.MESH
F32 = jnp.float32
BF16 = jnp.bfloat16

STRIDE = (2, 8, 32)
ORDERS = ((0, 1, 2), (1, 2, 0), (2, 0, 1))
COUNT = (6, 5, 5)
NI = 6
SPLIT = 3


LAT, QW, LANES = 512, 576, 128
KS, DIRS, RING, RING_OFFS, LINE_OFFS = range(3), range(2), range(4), range(1, 4), range(1, 8)


def _perm(rows, cols, f):
    r = lax.broadcasted_iota(jnp.int32, (rows, cols), 0)
    c = lax.broadcasted_iota(jnp.int32, (rows, cols), 1)
    return f(r, c).astype(F32).astype(BF16)


def _merge_weights(lses):
    top = functools.reduce(jnp.maximum, lses)
    ws = [jnp.exp2(v - top) for v in lses]
    tot = functools.reduce(jnp.add, ws)
    inv = 1.0 / tot
    return [w * inv for w in ws], top + jnp.log2(tot)


def _kernel(lens_h, q_h, c_h, o_ref,
            lens, q_in, s1src, s1buf, q_even, q_odd, cbuf, obuf, lrow, wcol, r1d, r1l, r1m, lse1,
            r2d, r2l, s3src, s3l, r3d, r3l,
            sem_l, sem_q, c_s, c_r, s1_s, s1_r, s2_s, s2_r, s3_s, s3_r,
            r1_s, r1_r, r1l_s, r1l_r, r2_s, r2_r, r2l_s, r2l_r, r3_s, r3_r, r3l_s, r3l_r):
    d = lax.axis_index('dcp')
    core = d % 2
    co = ((d // 2) % 4, (d // 8) % 4, d // 32)
    partner = {'dcp': d + 1 - 2 * core}

    nxt = (1, 2, 0)
    ac = [co[n] + core * (co[nxt[n]] - co[n]) for n in KS]
    stride = [STRIDE[n] + core * (STRIDE[nxt[n]] - STRIDE[n]) for n in KS]

    def ring(axis, off):
        return {'dcp': d + ((ac[axis] + off) % 4 - ac[axis]) * stride[axis]}

    def line(axis, j):
        return {'dcp': d + (j // 2 - ac[axis]) * stride[axis] + (j % 2 - core)}

    def send(src, dst, ss, rs, dev):
        pltpu.make_async_remote_copy(src_ref=src, dst_ref=dst, send_sem=ss, recv_sem=rs,
                                     device_id=dev, device_id_type=MESH).start()

    def wait(ref, sem):
        pltpu.make_async_copy(ref, ref, sem).wait()

    def ks_of(i):
        return KS if i < NI - 1 else range(1)

    load_q = pltpu.make_async_copy(q_h, q_in, sem_q)
    load_q.start()
    load_l = pltpu.make_async_copy(lens_h, lens, sem_l)
    load_l.start()

    def cache_rows(i, half):
        n = len(ks_of(i))
        return c_h.at[pl.ds(16 * half + 3 * i, n)], cbuf.at[pl.ds(3 * i, n), pl.ds(32 * core, 32)]

    for i in range(NI):
        src, dst = cache_rows(i, core)
        pltpu.make_async_copy(src, dst, c_r).start()

    bar = pltpu.get_barrier_semaphore()
    pl.semaphore_signal(bar, inc=1, device_id=partner, device_id_type=MESH)
    for a in KS:
        for off in RING_OFFS:
            for c2 in DIRS:
                peer = d + ((co[a] + off) % 4 - co[a]) * STRIDE[a] + c2 - core
                pl.semaphore_signal(bar, inc=1, device_id={'dcp': peer}, device_id_type=MESH)
    lrow[...] = jnp.zeros_like(lrow)
    load_l.wait()

    def sel(r, c):
        s = 3 * (r % 8) + (r // 8) % 3
        return (c == 16 * (r // 24) + s) & (s < 16)

    load_q.wait()
    qp = jnp.dot(_perm(48, 32, sel), q_in[...], preferred_element_type=F32).astype(BF16)
    s1src[...] = qp.reshape(2, 3, 8, QW)
    pl.semaphore_wait(bar, 19)

    def place(k):
        return ac[ORDERS[k][0]] * 2 + core

    for k in KS:
        n = ORDERS[k][0]
        j0 = place(k)
        oc = co[n] + co[nxt[n]] - ac[n]
        ost = STRIDE[n] + STRIDE[nxt[n]] - stride[n]
        for off in (2, 1, 3):
            send(s1src.at[core, k], s1buf.at[k, j0], s1_s, s1_r, ring(n, off))
        for off in (2, 1, 3, 0):
            peer = {'dcp': d + ((oc + off) % 4 - oc) * ost + 1 - 2 * core}
            send(s1src.at[1 - core, k], s1buf.at[k, oc * 2 + core], s1_s, s1_r, peer)
        s1buf[k, j0] = s1src[core, k]
    for i in range(NI):
        src, dst = cache_rows(i, 1 - core)
        send(src, dst, c_s, c_r, partner)

    def q_of(i):
        return q_odd if i % 2 else q_even

    def q_slot(k, i):
        return (k * 3 + i // 2) * 16

    def slot(k, i):
        return (k * NI + i) * 16

    def blk(k, i, off):
        _, a2, a3 = ORDERS[k]
        return q_of(i).at[q_slot(k, i) + ac[a3] * 4 + (ac[a2] - off) % 4]

    def copy3(k, i, off):
        b = blk(k, i, off)
        a3 = ORDERS[k][2]
        for o in (2, 1, 3):
            send(b, b, s3_s.at[i % 2], s3_r.at[i], ring(a3, o))

    def stage2(k, i):
        b = blk(k, i, 0)
        for off in (2, 1, 3):
            send(b, b, s2_s.at[i % 2], s2_r.at[i], ring(ORDERS[k][1], off))
        copy3(k, i, 0)

    tr = _perm(64, 64, lambda r, c: (r // 8 == c % 8) & (r % 8 == c // 8))
    wait(s1buf.at[:, pl.ds(0, 7)], s1_r)
    turned = [jnp.dot(tr, s1buf[k].reshape(64, QW), preferred_element_type=F32) for k in KS]
    for k in KS:
        rows = turned[k]
        _, a2, a3 = ORDERS[k]
        for i in range(COUNT[k]):
            y = rows[8 * i:8 * i + 8, :LAT if i % 2 else QW]
            if i % 2 == 0:
                y = jnp.concatenate([y, rows[8 * i + 8:8 * i + 16, LAT:]], axis=1)
            q_of(i)[q_slot(k, i) + ac[a3] * 4 + ac[a2]] = y.astype(BF16)
    for i in range(NI):
        for k in ks_of(i):
            stage2(k, i)

    def stage3(i):
        n = len(ks_of(i))
        wait(q_of(i).at[pl.ds(0, 3 * n)], s2_r.at[i])
        for off in (1, 3, 2):
            for k in ks_of(i):
                copy3(k, i, off)

    def arrive(i):
        n = len(ks_of(i))
        if i == 0:
            wait(cbuf, c_r)
        wait(q_of(i).at[pl.ds(0, 12 * n)], s3_r.at[i])

    for i in range(NI):
        stage3(i)

    chip8 = (d // 2) * 16

    j = lax.broadcasted_iota(jnp.int32, (LAT, LANES), 0)
    pos = (j & 7) + ((j >> 3) & 31) * 1024 + (j >> 8) * 8

    def cache_of(k, i):
        return cbuf[3 * i + k].reshape(LAT, QW)

    def scores(k, i):
        cs = cache_of(k, i)
        n = pl.ds(q_slot(k, i), 16)
        lat = q_of(i)[n, :, :LAT].reshape(LANES, LAT)
        rope = q_even[n, :, LAT:].reshape(LANES, LANES)
        rope = rope[:, ROPE:] if i % 2 else rope[:, :ROPE]
        dims = (((1,), (1,)), ((), ()))
        st = lax.dot_general(cs[:, :LAT], lat, dims, preferred_element_type=F32)
        return (st + lax.dot_general(cs[:, LAT:], rope, dims, preferred_element_type=F32)) * SCALE2

    def softmax(st, k, i):
        ok = pos < lens[16 * core + 3 * i + k] - chip8
        st = jnp.where(ok, st, NEG)
        m = jnp.max(st, axis=0, keepdims=True)
        p = jnp.where(ok, jnp.exp2(st - m), 0.0)
        l = jnp.sum(p, axis=0, keepdims=True)
        has = l > 0.0
        ls = jnp.where(has, l, 1.0)
        w = wave(i)
        lrow[w, k, i - w * SPLIT:i - w * SPLIT + 1, :] = jnp.where(has, m + jnp.log2(ls), NEG)
        return (p * (1.0 / ls)).astype(BF16)

    def attend(i):
        ks = ks_of(i)
        sts = [scores(k, i) for k in ks]
        ps = [softmax(st, k, i) for st, k in zip(sts, ks)]
        outs = [lax.dot_general(p, cache_of(k, i)[:, :LAT], (((0,), (0,)), ((), ())), preferred_element_type=F32)
                for p, k in zip(ps, ks)]
        for o, k in zip(outs, ks):
            obuf[pl.ds(slot(k, i), 16)] = o.astype(BF16).reshape(16, 8, LAT)

    def wave(i):
        return 0 if i < SPLIT else 1

    def send1(k, i):
        a3 = ORDERS[k][2]
        for o in (2, 1, 3):
            b = obuf.at[pl.ds(slot(k, i) + ((ac[a3] + o) % 4) * 4, 4)]
            send(b, r1d.at[k, i, o - 1], r1_s, r1_r.at[wave(i)], ring(a3, o))

    def members(w, k):
        return range(SPLIT) if w == 0 else range(SPLIT, COUNT[k])

    def count(w):
        return sum(len(members(w, k)) for k in KS)

    def send1_lse(w):
        for k in KS:
            for o in RING_OFFS:
                send(lrow.at[w, k], r1l.at[w, k, o - 1], r1l_s, r1l_r.at[w], ring(ORDERS[k][2], o))

    for i in range(NI):
        with jax.named_scope(f"arrive{i}"):
            arrive(i)
        with jax.named_scope(f"attend{i}"):
            attend(i)
            if i == NI - 1:
                send1_lse(1)
            for k in ks_of(i):
                send1(k, i)
        with jax.named_scope(f"rest{i}"):
            if i == SPLIT - 1:
                send1_lse(0)


    def columns(ws, k, row, n):
        wcol[k, :, :32] = jnp.concatenate(ws, axis=0).T
        t = wcol[k, pl.ds(row, n), :32]
        return lambda x, i: t[:, 8 * x + i:8 * x + i + 1]

    def weighted(cols, i, parts):
        return functools.reduce(jnp.add, [p.astype(F32) * cols(x, i) for x, p in enumerate(parts)])

    def merge1(w):
        cols = []
        wait(r1l.at[w], r1l_r.at[w])
        for k in KS:
            ws, lse1[w, k] = _merge_weights([lrow[w, k]] + [r1l[w, k, x] for x in KS])
            cols.append(columns(ws, k, ac[ORDERS[k][2]] * 32, 32))
        for k in KS:
            for o in RING_OFFS:
                send(lse1.at[w, k], r2l.at[w, k, o - 1], r2l_s, r2l_r.at[w], ring(ORDERS[k][1], o))
        wait(obuf.at[pl.ds(0, 12 * count(w))], r1_r.at[w])
        for k in KS:
            _, a2, a3 = ORDERS[k]
            its = members(w, k)
            for i in its:
                own = obuf[pl.ds(slot(k, i) + ac[a3] * 4, 4)]
                parts = [v.reshape(32, LAT) for v in [own] + [r1d[k, i, x] for x in KS]]
                y = weighted(cols[k], i - its[0], parts).astype(BF16).reshape(4, 8, LAT)
                for p in RING:
                    r1m[k, p, i] = y[p]
            for o in (2, 1, 3):
                sl = pl.ds(its[0], len(its))
                send(r1m.at[k, (ac[a2] + o) % 4, sl], r2d.at[k, o - 1, sl], r2_s, r2_r.at[w], ring(a2, o))

    def merge2(w):
        cols = []
        wait(r2l.at[w], r2l_r.at[w])
        for k in KS:
            _, a2, a3 = ORDERS[k]
            ws, l2 = _merge_weights([lse1[w, k]] + [r2l[w, k, x] for x in KS])
            g = ac[a3] * 4 + ac[a2]
            lt = pltpu.roll(l2, ((16 - g) % 16) * 8, 1)
            s3l[w, k] = jnp.concatenate([lt] * 16, axis=0).T[0:8].reshape(8, 1, LANES)
            cols.append(columns(ws, k, g * 8, 8))
        for k in KS:
            j0 = place(k)
            for off in LINE_OFFS:
                j = (j0 + off) % 8
                send(s3l.at[w, k, j], r3l.at[w, k, j0], r3l_s, r3l_r.at[w], line(ORDERS[k][0], j))
            r3l[w, k, j0] = s3l[w, k, j0]
        wait(obuf.at[pl.ds(0, 3 * count(w))], r2_r.at[w])
        tiles = []
        for k in KS:
            its = members(w, k)
            ys = [weighted(cols[k], i - its[0], [r1m[k, ac[ORDERS[k][1]], i]] + [r2d[k, x, i] for x in KS]) for i in its]
            n = len(its)
            pm = _perm(64, 8 * n, lambda r, c: (c == (r % 8) * 8 + r // 8) & (r % 8 < n))
            tiles.append(jnp.dot(pm, jnp.concatenate(ys, axis=0).astype(BF16), preferred_element_type=F32))
        for k in KS:
            s3src[w, k] = tiles[k].astype(BF16).reshape(8, 8, LAT)
            j0 = place(k)
            for off in (3, 4, 5, 2, 6, 1, 7):
                j = (j0 + off) % 8
                send(s3src.at[w, k, j], r3d.at[w, k, j0], r3_s, r3_r.at[w], line(ORDERS[k][0], j))
            r3d[w, k, j0] = s3src[w, k, j0]

    rows = {}

    def merge3(w):
        cols = []
        wait(r3l.at[w, :, pl.ds(0, 7)], r3l_r.at[w])
        for k in KS:
            ls = [r3l[w, k, j] for j in range(8)]
            ws = [None] * 8
            for h in DIRS:
                ws[h::2], _ = _merge_weights(ls[h::2])
            cols.append(jnp.concatenate(ws, axis=0).T[0:8])
        wait(r3d.at[w, :, pl.ds(0, 7)], r3_r.at[w])
        for k in KS:
            for h in DIRS:
                ts = [r3d[w, k, j].astype(F32) * cols[k][:, j:j + 1] for j in range(h, 8, 2)]
                rows[w, h, k] = functools.reduce(jnp.add, ts)

    merge1(0)
    merge1(1)
    merge2(0)
    wait(s1buf.at[:, pl.ds(0, 7)], s1_s)
    wait(cbuf.at[pl.ds(0, 8)], c_s)
    for par in DIRS:
        its = [i for i in range(NI) for _ in ks_of(i) if i % 2 == par]
        wait(q_of(par).at[pl.ds(0, 3 * len(its))], s2_s.at[par])
        wait(q_of(par).at[pl.ds(0, 12 * len(its))], s3_s.at[par])
    merge2(1)
    merge3(0)
    wait(obuf.at[pl.ds(0, 192)], r1_s)
    wait(r1l, r1l_s)
    wait(obuf.at[pl.ds(0, 48)], r2_s)
    wait(r2l, r2l_s)
    merge3(1)
    flat = jnp.concatenate([rows[w, h, k] for w in DIRS for h in DIRS for k in KS], axis=0).astype(BF16)

    def pick(r, c):
        w, h, k, i = c // 48, (c // 24) % 2, (c // 8) % 3, c % 8
        s = 3 * (i + w * SPLIT) + k
        return (r == 16 * h + s) & (s < 16) & (i < SPLIT)

    o_ref[...] = jnp.dot(_perm(32, 96, pick), flat, preferred_element_type=F32).astype(BF16)

    wait(r3d.at[:, :, pl.ds(0, 7)], r3_s)
    wait(r3l.at[:, :, pl.ds(0, 7)], r3l_s)


def solution(mesh):
    def local(q, cache, lens):
        dma = pltpu.SemaphoreType.DMA
        V = pltpu.VMEM
        anyspace = pl.BlockSpec(memory_space=pl.ANY)
        tile, qtile, row = (8, LAT), (8, QW), (8, LANES)
        line = (2, 3, 8)
        scratch = [
            pltpu.SMEM((32,), jnp.int32), V((32, QW), BF16), V((2, 3) + qtile, BF16), V((3, 8) + qtile, BF16),
            V((144, 8, LAT + LANES), BF16), V((144,) + tile, BF16),
            V((16, 64) + qtile, BF16), V((288,) + tile, BF16), V((2, 3) + row, F32), V((3, LANES, LANES), F32),
            V((3, NI, 3, 4) + tile, BF16), V((2, 3, 3) + row, F32), V((3, 4, NI) + tile, BF16), V((2, 3) + row, F32),
            V((3, 3, NI) + tile, BF16), V((2, 3, 3) + row, F32),
            V(line + tile, BF16), V(line + (1, LANES), F32), V(line + tile, BF16), V(line + (1, LANES), F32),
            dma, dma, dma, dma, dma, dma, dma((2,)), dma((NI,)), dma((2,)), dma((NI,)),
            dma, dma((2,)), dma, dma((2,)), dma, dma((2,)), dma, dma((2,)), dma, dma((2,)), dma, dma((2,)),
        ]
        o = pl.pallas_call(
            _kernel,
            out_shape=V((32, LAT), BF16),
            in_specs=[anyspace] * 3,
            out_specs=pl.BlockSpec(memory_space=V),
            scratch_shapes=scratch,
            compiler_params=pltpu.CompilerParams(collective_id=0, has_side_effects=True,
                                                 vmem_limit_bytes=50 * 2 ** 20),
        )(*[pltpu.with_memory_space_constraint(v, pltpu.HBM) for v in (lens, q.reshape(32, QW), cache.reshape(32, 32, 8, QW))])
        return o.reshape(32, 1, LAT)

    return jax.shard_map(local, mesh=mesh,
                         in_specs=(P('dp', 'dcp', None), P('dp', None, 'dcp', None, None), P('dp')),
                         out_specs=P('dp', 'dcp', None), check_vma=False)
```

```python
import functools
import math

import jax
import jax.numpy as jnp
from jax import lax
from jax.experimental import pallas as pl
from jax.experimental.pallas import tpu as pltpu
from jax.sharding import PartitionSpec as P

ROPE = 64
QK_DIM = 192
SCALE2 = QK_DIM ** -0.5 * math.log2(math.e)
NEG = -3.0e38
MESH = pl.DeviceIdType.MESH
F32 = jnp.float32
BF16 = jnp.bfloat16

STRIDE = (2, 8, 32)
ORDERS = ((0, 1, 2), (1, 2, 0), (2, 0, 1))
COUNT = (6, 5, 5)
NI = 6
SPLIT = 3
ORDER, RELAYED = (0, 3, 4, 5, 1, 2), (3, 4, 5)


LAT, QW, LANES = 512, 576, 128
KS, DIRS, RING, RING_OFFS, LINE_OFFS = range(3), range(2), range(4), range(1, 4), range(1, 8)


def _perm(rows, cols, f):
    r = lax.broadcasted_iota(jnp.int32, (rows, cols), 0)
    c = lax.broadcasted_iota(jnp.int32, (rows, cols), 1)
    return f(r, c).astype(F32).astype(BF16)


def _merge_weights(lses):
    top = functools.reduce(jnp.maximum, lses)
    ws = [jnp.exp2(v - top) for v in lses]
    tot = functools.reduce(jnp.add, ws)
    inv = 1.0 / tot
    return [w * inv for w in ws], top + jnp.log2(tot)


def _kernel(lens_h, q_h, c_h, o_ref,
            lens, q_in, s1src, s1buf, q_even, q_odd, cbuf, obuf, lrow, wcol, r1d, r1l, r1m, lse1,
            r2d, r2l, s3src, s3l, r3d, r3l,
            sem_l, sem_q, c_s, c_r, s1_s, s1_r, s2_s, s2_r, s3_s, s3_r, sf_r,
            r1_s, r1_r, r1l_s, r1l_r, r2_s, r2_r, r2l_s, r2l_r, r3_s, r3_r, r3l_s, r3l_r):
    d = lax.axis_index('dcp')
    core = d % 2
    co = ((d // 2) % 4, (d // 8) % 4, d // 32)
    partner = {'dcp': d + 1 - 2 * core}

    nxt = (1, 2, 0)
    ac = [co[n] + core * (co[nxt[n]] - co[n]) for n in KS]
    stride = [STRIDE[n] + core * (STRIDE[nxt[n]] - STRIDE[n]) for n in KS]

    def ring(axis, off):
        return {'dcp': d + ((ac[axis] + off) % 4 - ac[axis]) * stride[axis]}

    def line(axis, j):
        return {'dcp': d + (j // 2 - ac[axis]) * stride[axis] + (j % 2 - core)}

    def send(src, dst, ss, rs, dev):
        pltpu.make_async_remote_copy(src_ref=src, dst_ref=dst, send_sem=ss, recv_sem=rs,
                                     device_id=dev, device_id_type=MESH).start()

    def wait(ref, sem):
        pltpu.make_async_copy(ref, ref, sem).wait()

    def ks_of(i):
        return KS if i < NI - 1 else range(1)

    bar = pltpu.get_barrier_semaphore()
    pl.semaphore_signal(bar, inc=1, device_id=partner, device_id_type=MESH)
    for a in KS:
        for off in RING_OFFS:
            for c2 in DIRS:
                peer = d + ((co[a] + off) % 4 - co[a]) * STRIDE[a] + c2 - core
                pl.semaphore_signal(bar, inc=1, device_id={'dcp': peer}, device_id_type=MESH)
    load_q = pltpu.make_async_copy(q_h, q_in, sem_q)
    load_q.start()
    load_l = pltpu.make_async_copy(lens_h, lens, sem_l)
    load_l.start()

    def cache_rows(i, half):
        n = len(ks_of(i))
        return c_h.at[pl.ds(16 * half + 3 * i, n)], cbuf.at[pl.ds(3 * i, n), pl.ds(32 * core, 32)]

    for i in range(NI):
        src, dst = cache_rows(i, core)
        pltpu.make_async_copy(src, dst, c_r).start()

    lrow[...] = jnp.zeros_like(lrow)
    load_l.wait()

    def sel(r, c):
        s = 3 * (r % 8) + (r // 8) % 3
        return (c == 16 * (r // 24) + s) & (s < 16)

    load_q.wait()
    qp = jnp.dot(_perm(48, 32, sel), q_in[...], preferred_element_type=F32).astype(BF16)
    s1src[...] = qp.reshape(2, 3, 8, QW)
    pl.semaphore_wait(bar, 19)

    def place(k):
        return ac[ORDERS[k][0]] * 2 + core

    for k in KS:
        n = ORDERS[k][0]
        j0 = place(k)
        oc = co[n] + co[nxt[n]] - ac[n]
        ost = STRIDE[n] + STRIDE[nxt[n]] - stride[n]
        for off in (2, 1, 3):
            send(s1src.at[core, k], s1buf.at[k, j0], s1_s, s1_r, ring(n, off))
        for off in (2, 1, 3, 0):
            peer = {'dcp': d + ((oc + off) % 4 - oc) * ost + 1 - 2 * core}
            send(s1src.at[1 - core, k], s1buf.at[k, oc * 2 + core], s1_s, s1_r, peer)
        s1buf[k, j0] = s1src[core, k]
    for i in range(NI):
        src, dst = cache_rows(i, 1 - core)
        send(src, dst, c_s, c_r, partner)

    def q_of(i):
        return q_odd if i % 2 else q_even

    def q_slot(k, i):
        return (k * 3 + i // 2) * 16

    def slot(k, i):
        return (k * NI + i) * 16

    def blk(k, i, off):
        _, a2, a3 = ORDERS[k]
        return q_of(i).at[q_slot(k, i) + ac[a3] * 4 + (ac[a2] - off) % 4]

    def copy3(k, i, off):
        b = blk(k, i, off)
        a3 = ORDERS[k][2]
        for o in (1, 3) if i in RELAYED else (2, 1, 3):
            onward = i in RELAYED and off // 2 == o // 2
            send(b, b, s3_s.at[i % 2], sf_r.at[i] if onward else s3_r.at[i], ring(a3, o))

    def stage2(k, i):
        b = blk(k, i, 0)
        for off in (2, 1, 3):
            send(b, b, s2_s.at[i % 2], s2_r.at[i], ring(ORDERS[k][1], off))
        copy3(k, i, 0)

    tr = _perm(64, 64, lambda r, c: (r // 8 == c % 8) & (r % 8 == c // 8))
    wait(s1buf.at[:, pl.ds(0, 7)], s1_r)
    turned = [jnp.dot(tr, s1buf[k].reshape(64, QW), preferred_element_type=F32) for k in KS]
    for k in KS:
        rows = turned[k]
        _, a2, a3 = ORDERS[k]
        for i in range(COUNT[k]):
            y = rows[8 * i:8 * i + 8, :LAT if i % 2 else QW]
            if i % 2 == 0:
                y = jnp.concatenate([y, rows[8 * i + 8:8 * i + 16, LAT:]], axis=1)
            q_of(i)[q_slot(k, i) + ac[a3] * 4 + ac[a2]] = y.astype(BF16)
    for i in ORDER:
        for k in ks_of(i):
            stage2(k, i)

    def stage3(i):
        n = len(ks_of(i))
        wait(q_of(i).at[pl.ds(0, 3 * n)], s2_r.at[i])
        for off in (1, 3, 2):
            for k in ks_of(i):
                copy3(k, i, off)

    def forward(i):
        wait(q_of(i).at[pl.ds(0, 4 * len(ks_of(i)))], sf_r.at[i])
        for off in RING:
            for k in ks_of(i):
                _, a2, a3 = ORDERS[k]
                o = 1 if off < 2 else 3
                b = q_of(i).at[q_slot(k, i) + ((ac[a3] - o) % 4) * 4 + (ac[a2] - off) % 4]
                send(b, b, s3_s.at[i % 2], s3_r.at[i], ring(a3, o))

    def arrive(i):
        n = len(ks_of(i))
        if i == 0:
            wait(cbuf, c_r)
        wait(q_of(i).at[pl.ds(0, (8 if i in RELAYED else 12) * n)], s3_r.at[i])

    for i in ORDER:
        stage3(i)

    chip8 = (d // 2) * 16

    j = lax.broadcasted_iota(jnp.int32, (LAT, LANES), 0)
    pos = (j & 7) + ((j >> 3) & 31) * 1024 + (j >> 8) * 8

    def cache_of(k, i):
        return cbuf[3 * i + k].reshape(LAT, QW)

    def scores(k, i):
        cs = cache_of(k, i)
        n = pl.ds(q_slot(k, i), 16)
        lat = q_of(i)[n, :, :LAT].reshape(LANES, LAT)
        rope = q_even[n, :, LAT:].reshape(LANES, LANES)
        rope = rope[:, ROPE:] if i % 2 else rope[:, :ROPE]
        dims = (((1,), (1,)), ((), ()))
        st = lax.dot_general(cs[:, :LAT], lat, dims, preferred_element_type=F32)
        return (st + lax.dot_general(cs[:, LAT:], rope, dims, preferred_element_type=F32)) * SCALE2

    def softmax(st, k, i):
        ok = pos < lens[16 * core + 3 * i + k] - chip8
        st = jnp.where(ok, st, NEG)
        m = jnp.max(st, axis=0, keepdims=True)
        has = m > NEG
        p = jnp.exp2(st - jnp.where(has, m, 0.0))
        ls = jnp.where(has, jnp.sum(p, axis=0, keepdims=True), 1.0)
        w = wave(i)
        lrow[w, k, i - w * SPLIT:i - w * SPLIT + 1, :] = jnp.where(has, m + jnp.log2(ls), NEG)
        return (p * (1.0 / ls)).astype(BF16)

    def attend(batch):
        sts = [scores(k, i) for k, i in batch]
        ps = [softmax(st, k, i) for st, (k, i) in zip(sts, batch)]
        outs = [lax.dot_general(p, cache_of(k, i)[:, :LAT], (((0,), (0,)), ((), ())), preferred_element_type=F32)
                for p, (k, i) in zip(ps, batch)]
        for o, (k, i) in zip(outs, batch):
            obuf[pl.ds(slot(k, i), 16)] = o.astype(BF16).reshape(16, 8, LAT)

    def wave(i):
        return 0 if i < SPLIT else 1

    def send1(k, i):
        a3 = ORDERS[k][2]
        for o in (2, 1, 3):
            b = obuf.at[pl.ds(slot(k, i) + ((ac[a3] + o) % 4) * 4, 4)]
            send(b, r1d.at[k, i, o - 1], r1_s, r1_r.at[wave(i)], ring(a3, o))

    def members(w, k):
        return range(SPLIT) if w == 0 else range(SPLIT, COUNT[k])

    def count(w):
        return sum(len(members(w, k)) for k in KS)

    def send1_lse(w):
        for k in KS:
            for o in RING_OFFS:
                send(lrow.at[w, k], r1l.at[w, k, o - 1], r1l_s, r1l_r.at[w], ring(ORDERS[k][2], o))

    for i in range(NI - 1):
        batch = [(k, i) for k in KS]
        with jax.named_scope(f"arrive{i}"):
            arrive(i)
            if i == NI - 2:
                arrive(i + 1)
                batch.append((0, i + 1))
        with jax.named_scope(f"attend{i}"):
            attend(batch)
        with jax.named_scope(f"rest{i}"):
            if i == 0:
                for x in RELAYED:
                    forward(x)
            if i == SPLIT - 1:
                send1_lse(0)
            if i == NI - 2:
                send1_lse(1)
            for k, x in batch:
                send1(k, x)


    def columns(ws, k, row, n):
        wcol[k, :, :32] = jnp.concatenate(ws, axis=0).T
        t = wcol[k, pl.ds(row, n), :32]
        return lambda x, i: t[:, 8 * x + i:8 * x + i + 1]

    def weighted(cols, i, parts):
        return functools.reduce(jnp.add, [p.astype(F32) * cols(x, i) for x, p in enumerate(parts)])

    def merge1(w):
        cols = []
        wait(r1l.at[w], r1l_r.at[w])
        for k in KS:
            ws, lse1[w, k] = _merge_weights([lrow[w, k]] + [r1l[w, k, x] for x in KS])
            cols.append(columns(ws, k, ac[ORDERS[k][2]] * 32, 32))
        for k in KS:
            for o in RING_OFFS:
                send(lse1.at[w, k], r2l.at[w, k, o - 1], r2l_s, r2l_r.at[w], ring(ORDERS[k][1], o))
        wait(obuf.at[pl.ds(0, 12 * count(w))], r1_r.at[w])
        for k in KS:
            _, a2, a3 = ORDERS[k]
            its = members(w, k)
            for i in its:
                own = obuf[pl.ds(slot(k, i) + ac[a3] * 4, 4)]
                parts = [v.reshape(32, LAT) for v in [own] + [r1d[k, i, x] for x in KS]]
                y = weighted(cols[k], i - its[0], parts).astype(BF16).reshape(4, 8, LAT)
                for p in RING:
                    r1m[k, p, i] = y[p]
            for o in (2, 1, 3):
                sl = pl.ds(its[0], len(its))
                send(r1m.at[k, (ac[a2] + o) % 4, sl], r2d.at[k, o - 1, sl], r2_s, r2_r.at[w], ring(a2, o))

    def merge2(w):
        cols = []
        wait(r2l.at[w], r2l_r.at[w])
        for k in KS:
            _, a2, a3 = ORDERS[k]
            ws, l2 = _merge_weights([lse1[w, k]] + [r2l[w, k, x] for x in KS])
            g = ac[a3] * 4 + ac[a2]
            lt = pltpu.roll(l2, ((16 - g) % 16) * 8, 1)
            s3l[w, k] = jnp.concatenate([lt] * 16, axis=0).T[0:8].reshape(8, 1, LANES)
            cols.append(columns(ws, k, g * 8, 8))
        for k in KS:
            j0 = place(k)
            for off in LINE_OFFS:
                j = (j0 + off) % 8
                send(s3l.at[w, k, j], r3l.at[w, k, j0], r3l_s, r3l_r.at[w], line(ORDERS[k][0], j))
            r3l[w, k, j0] = s3l[w, k, j0]
        wait(obuf.at[pl.ds(0, 3 * count(w))], r2_r.at[w])
        tiles = []
        for k in KS:
            its = members(w, k)
            ys = [weighted(cols[k], i - its[0], [r1m[k, ac[ORDERS[k][1]], i]] + [r2d[k, x, i] for x in KS]) for i in its]
            n = len(its)
            pm = _perm(64, 8 * n, lambda r, c: (c == (r % 8) * 8 + r // 8) & (r % 8 < n))
            tiles.append(jnp.dot(pm, jnp.concatenate(ys, axis=0).astype(BF16), preferred_element_type=F32))
        for k in KS:
            s3src[w, k] = tiles[k].astype(BF16).reshape(8, 8, LAT)
            j0 = place(k)
            for off in (3, 4, 5, 2, 6, 1, 7):
                j = (j0 + off) % 8
                send(s3src.at[w, k, j], r3d.at[w, k, j0], r3_s, r3_r.at[w], line(ORDERS[k][0], j))
            r3d[w, k, j0] = s3src[w, k, j0]

    rows = {}

    def merge3(w):
        cols = []
        wait(r3l.at[w, :, pl.ds(0, 7)], r3l_r.at[w])
        for k in KS:
            ls = [r3l[w, k, j] for j in range(8)]
            ws = [None] * 8
            for h in DIRS:
                ws[h::2], _ = _merge_weights(ls[h::2])
            cols.append(jnp.concatenate(ws, axis=0).T[0:8])
        wait(r3d.at[w, :, pl.ds(0, 7)], r3_r.at[w])
        for k in KS:
            for h in DIRS:
                ts = [r3d[w, k, j].astype(F32) * cols[k][:, j:j + 1] for j in range(h, 8, 2)]
                rows[w, h, k] = functools.reduce(jnp.add, ts)

    merge1(0)
    merge1(1)
    merge2(0)
    wait(s1buf.at[:, pl.ds(0, 7)], s1_s)
    wait(cbuf.at[pl.ds(0, 8)], c_s)
    for par in DIRS:
        its = [i for i in range(NI) for _ in ks_of(i) if i % 2 == par]
        wait(q_of(par).at[pl.ds(0, 3 * len(its))], s2_s.at[par])
        wait(q_of(par).at[pl.ds(0, 12 * len(its))], s3_s.at[par])
    merge2(1)
    merge3(0)
    wait(obuf.at[pl.ds(0, 192)], r1_s)
    wait(r1l, r1l_s)
    wait(obuf.at[pl.ds(0, 48)], r2_s)
    wait(r2l, r2l_s)
    merge3(1)
    flat = jnp.concatenate([rows[w, h, k] for w in DIRS for h in DIRS for k in KS], axis=0).astype(BF16)

    def pick(r, c):
        w, h, k, i = c // 48, (c // 24) % 2, (c // 8) % 3, c % 8
        s = 3 * (i + w * SPLIT) + k
        return (r == 16 * h + s) & (s < 16) & (i < SPLIT)

    o_ref[...] = jnp.dot(_perm(32, 96, pick), flat, preferred_element_type=F32).astype(BF16)

    wait(r3d.at[:, :, pl.ds(0, 7)], r3_s)
    wait(r3l.at[:, :, pl.ds(0, 7)], r3l_s)


def solution(mesh):
    def local(q, cache, lens):
        dma = pltpu.SemaphoreType.DMA
        V = pltpu.VMEM
        anyspace = pl.BlockSpec(memory_space=pl.ANY)
        tile, qtile, row = (8, LAT), (8, QW), (8, LANES)
        line = (2, 3, 8)
        scratch = [
            pltpu.SMEM((32,), jnp.int32), V((32, QW), BF16), V((2, 3) + qtile, BF16), V((3, 8) + qtile, BF16),
            V((144, 8, LAT + LANES), BF16), V((144,) + tile, BF16),
            V((16, 64) + qtile, BF16), V((288,) + tile, BF16), V((2, 3) + row, F32), V((3, LANES, LANES), F32),
            V((3, NI, 3, 4) + tile, BF16), V((2, 3, 3) + row, F32), V((3, 4, NI) + tile, BF16), V((2, 3) + row, F32),
            V((3, 3, NI) + tile, BF16), V((2, 3, 3) + row, F32),
            V(line + tile, BF16), V(line + (1, LANES), F32), V(line + tile, BF16), V(line + (1, LANES), F32),
            dma, dma, dma, dma, dma, dma, dma((2,)), dma((NI,)), dma((2,)), dma((NI,)), dma((NI,)),
            dma, dma((2,)), dma, dma((2,)), dma, dma((2,)), dma, dma((2,)), dma, dma((2,)), dma, dma((2,)),
        ]
        o = pl.pallas_call(
            _kernel,
            out_shape=V((32, LAT), BF16),
            in_specs=[anyspace] * 3,
            out_specs=pl.BlockSpec(memory_space=V),
            scratch_shapes=scratch,
            compiler_params=pltpu.CompilerParams(collective_id=0, has_side_effects=True,
                                                 vmem_limit_bytes=50 * 2 ** 20),
        )(*[pltpu.with_memory_space_constraint(v, pltpu.HBM) for v in (lens, q.reshape(32, QW), cache.reshape(32, 32, 8, QW))])
        return o.reshape(32, 1, LAT)

    return jax.shard_map(local, mesh=mesh,
                         in_specs=(P('dp', 'dcp', None), P('dp', None, 'dcp', None, None), P('dp')),
                         out_specs=P('dp', 'dcp', None), check_vma=False)
```

```python
import functools
import math

import jax
import jax.numpy as jnp
from jax import lax
from jax.experimental import pallas as pl
from jax.experimental.pallas import tpu as pltpu
from jax.sharding import PartitionSpec as P

ROPE = 64
QK_DIM = 192
SCALE2 = QK_DIM ** -0.5 * math.log2(math.e)
NEG = -3.0e38
MESH = pl.DeviceIdType.MESH
F32 = jnp.float32
BF16 = jnp.bfloat16

STRIDE = (2, 8, 32)
ORDERS = ((0, 1, 2), (1, 2, 0), (2, 0, 1))
COUNT = (6, 5, 5)
NI = 6
SPLIT = 4
TILE = (SPLIT, NI - SPLIT)
ORDER, RELAYED = (0, 3, 4, 5, 1, 2), (3, 4, 5)


LAT, QW, LANES = 512, 576, 128
KS, DIRS, RING, RING_OFFS, LINE_OFFS = range(3), range(2), range(4), range(1, 4), range(1, 8)


def _perm(rows, cols, f):
    r = lax.broadcasted_iota(jnp.int32, (rows, cols), 0)
    c = lax.broadcasted_iota(jnp.int32, (rows, cols), 1)
    return f(r, c).astype(F32).astype(BF16)


def _merge_weights(lses):
    top = functools.reduce(jnp.maximum, lses)
    ws = [jnp.exp2(v - top) for v in lses]
    tot = functools.reduce(jnp.add, ws)
    inv = 1.0 / tot
    return [w * inv for w in ws], top + jnp.log2(tot)


def _kernel(lens_h, q_h, c_h, o_ref,
            lens, q_in, s1src, s1buf, q_even, q_odd, cbuf, obuf, lrow, wcol, r1d, r1l, r1m, lse1,
            r2d, r2l, s3a, s3b, s3l, r3a, r3b, r3l, fin,
            sem_l, sem_q, c_s, c_r, s1_s, s1_r, s2_s, s2_r, s3_s, s3_r, sf_r,
            r1_s, r1_r, r1l_s, r1l_r, r2_s, r2_r, r2l_s, r2l_r, r3_s, r3_r, r3l_s, r3l_r):
    d = lax.axis_index('dcp')
    core = d % 2
    co = ((d // 2) % 4, (d // 8) % 4, d // 32)
    partner = {'dcp': d + 1 - 2 * core}

    nxt = (1, 2, 0)
    ac = [co[n] + core * (co[nxt[n]] - co[n]) for n in KS]
    stride = [STRIDE[n] + core * (STRIDE[nxt[n]] - STRIDE[n]) for n in KS]

    def ring(axis, off):
        return {'dcp': d + ((ac[axis] + off) % 4 - ac[axis]) * stride[axis]}

    def line(axis, j):
        return {'dcp': d + (j // 2 - ac[axis]) * stride[axis] + (j % 2 - core)}

    def send(src, dst, ss, rs, dev):
        pltpu.make_async_remote_copy(src_ref=src, dst_ref=dst, send_sem=ss, recv_sem=rs,
                                     device_id=dev, device_id_type=MESH).start()

    def wait(ref, sem):
        pltpu.make_async_copy(ref, ref, sem).wait()

    def ks_of(i):
        return KS if i < NI - 1 else range(1)

    bar = pltpu.get_barrier_semaphore()
    pl.semaphore_signal(bar, inc=1, device_id=partner, device_id_type=MESH)
    for a in KS:
        for off in RING_OFFS:
            for c2 in DIRS:
                peer = d + ((co[a] + off) % 4 - co[a]) * STRIDE[a] + c2 - core
                pl.semaphore_signal(bar, inc=1, device_id={'dcp': peer}, device_id_type=MESH)
    load_q = pltpu.make_async_copy(q_h, q_in, sem_q)
    load_q.start()
    load_l = pltpu.make_async_copy(lens_h, lens, sem_l)
    load_l.start()

    def cache_rows(i, half):
        n = len(ks_of(i))
        return c_h.at[pl.ds(16 * half + 3 * i, n)], cbuf.at[pl.ds(3 * i, n), pl.ds(32 * core, 32)]

    for i in range(NI):
        src, dst = cache_rows(i, core)
        pltpu.make_async_copy(src, dst, c_r).start()

    lrow[...] = jnp.zeros_like(lrow)
    fin[...] = jnp.zeros_like(fin)
    load_l.wait()

    def sel(r, c):
        s = 3 * (r % 8) + (r // 8) % 3
        return (c == 16 * (r // 24) + s) & (s < 16)

    load_q.wait()
    qp = jnp.dot(_perm(48, 32, sel), q_in[...], preferred_element_type=F32).astype(BF16)
    s1src[...] = qp.reshape(2, 3, 8, QW)
    pl.semaphore_wait(bar, 19)

    def place(k):
        return ac[ORDERS[k][0]] * 2 + core

    for k in KS:
        n = ORDERS[k][0]
        j0 = place(k)
        oc = co[n] + co[nxt[n]] - ac[n]
        ost = STRIDE[n] + STRIDE[nxt[n]] - stride[n]
        for off in (2, 1, 3):
            send(s1src.at[core, k], s1buf.at[k, j0], s1_s, s1_r, ring(n, off))
        for off in (2, 1, 3, 0):
            peer = {'dcp': d + ((oc + off) % 4 - oc) * ost + 1 - 2 * core}
            send(s1src.at[1 - core, k], s1buf.at[k, oc * 2 + core], s1_s, s1_r, peer)
        s1buf[k, j0] = s1src[core, k]
    for i in range(NI):
        src, dst = cache_rows(i, 1 - core)
        send(src, dst, c_s, c_r, partner)

    def q_of(i):
        return q_odd if i % 2 else q_even

    def q_slot(k, i):
        return (k * 3 + i // 2) * 16

    def slot(k, i):
        return (k * NI + i) * 16

    def blk(k, i, off):
        _, a2, a3 = ORDERS[k]
        return q_of(i).at[q_slot(k, i) + ac[a3] * 4 + (ac[a2] - off) % 4]

    def copy3(k, i, off):
        b = blk(k, i, off)
        a3 = ORDERS[k][2]
        for o in (1, 3) if i in RELAYED else (2, 1, 3):
            onward = i in RELAYED and off // 2 == o // 2
            send(b, b, s3_s.at[i % 2], sf_r.at[i] if onward else s3_r.at[i], ring(a3, o))

    def stage2(k, i):
        b = blk(k, i, 0)
        for off in (2, 1, 3):
            send(b, b, s2_s.at[i % 2], s2_r.at[i], ring(ORDERS[k][1], off))
        copy3(k, i, 0)

    tr = _perm(64, 64, lambda r, c: (r // 8 == c % 8) & (r % 8 == c // 8))
    wait(s1buf.at[:, pl.ds(0, 7)], s1_r)
    turned = [jnp.dot(tr, s1buf[k].reshape(64, QW), preferred_element_type=F32) for k in KS]
    for k in KS:
        rows = turned[k]
        _, a2, a3 = ORDERS[k]
        for i in range(COUNT[k]):
            y = rows[8 * i:8 * i + 8, :LAT if i % 2 else QW]
            if i % 2 == 0:
                y = jnp.concatenate([y, rows[8 * i + 8:8 * i + 16, LAT:]], axis=1)
            q_of(i)[q_slot(k, i) + ac[a3] * 4 + ac[a2]] = y.astype(BF16)
    for i in ORDER:
        for k in ks_of(i):
            stage2(k, i)

    def stage3(i):
        n = len(ks_of(i))
        wait(q_of(i).at[pl.ds(0, 3 * n)], s2_r.at[i])
        for off in (1, 3, 2):
            for k in ks_of(i):
                copy3(k, i, off)

    def forward(i):
        wait(q_of(i).at[pl.ds(0, 4 * len(ks_of(i)))], sf_r.at[i])
        for off in RING:
            for k in ks_of(i):
                _, a2, a3 = ORDERS[k]
                o = 1 if off < 2 else 3
                b = q_of(i).at[q_slot(k, i) + ((ac[a3] - o) % 4) * 4 + (ac[a2] - off) % 4]
                send(b, b, s3_s.at[i % 2], s3_r.at[i], ring(a3, o))

    def arrive(i):
        n = len(ks_of(i))
        if i == 0:
            wait(cbuf, c_r)
        wait(q_of(i).at[pl.ds(0, (8 if i in RELAYED else 12) * n)], s3_r.at[i])

    for i in ORDER:
        stage3(i)

    chip8 = (d // 2) * 16

    j = lax.broadcasted_iota(jnp.int32, (LAT, LANES), 0)
    pos = (j & 7) + ((j >> 3) & 31) * 1024 + (j >> 8) * 8

    def cache_of(k, i):
        return cbuf[3 * i + k].reshape(LAT, QW)

    def scores(k, i):
        cs = cache_of(k, i)
        n = pl.ds(q_slot(k, i), 16)
        lat = q_of(i)[n, :, :LAT].reshape(LANES, LAT)
        rope = q_even[n, :, LAT:].reshape(LANES, LANES)
        rope = rope[:, ROPE:] if i % 2 else rope[:, :ROPE]
        dims = (((1,), (1,)), ((), ()))
        st = lax.dot_general(cs[:, :LAT], lat, dims, preferred_element_type=F32)
        return (st + lax.dot_general(cs[:, LAT:], rope, dims, preferred_element_type=F32)) * SCALE2

    def softmax(st, k, i):
        ok = pos < lens[16 * core + 3 * i + k] - chip8
        st = jnp.where(ok, st, NEG)
        m = jnp.max(st, axis=0, keepdims=True)
        has = m > NEG
        p = jnp.exp2(st - jnp.where(has, m, 0.0))
        ls = jnp.where(has, jnp.sum(p, axis=0, keepdims=True), 1.0)
        w = wave(i)
        lrow[w, k, i - w * SPLIT] = jnp.where(has, m + jnp.log2(ls), NEG)
        return (p * (1.0 / ls)).astype(BF16)

    def attend(batch):
        sts = [scores(k, i) for k, i in batch]
        ps = [softmax(st, k, i) for st, (k, i) in zip(sts, batch)]
        outs = [lax.dot_general(p, cache_of(k, i)[:, :LAT], (((0,), (0,)), ((), ())), preferred_element_type=F32)
                for p, (k, i) in zip(ps, batch)]
        for o, (k, i) in zip(outs, batch):
            obuf[pl.ds(slot(k, i), 16)] = o.astype(BF16).reshape(16, 8, LAT)

    def wave(i):
        return 0 if i < SPLIT else 1

    def send1(k, i):
        a3 = ORDERS[k][2]
        for o in (2, 1, 3):
            b = obuf.at[pl.ds(slot(k, i) + ((ac[a3] + o) % 4) * 4, 4)]
            send(b, r1d.at[k, i, o - 1], r1_s, r1_r.at[wave(i)], ring(a3, o))

    def members(w, k):
        return range(SPLIT) if w == 0 else range(SPLIT, COUNT[k])

    def count(w):
        return sum(len(members(w, k)) for k in KS)

    def send1_lse(w):
        for k in KS:
            for o in RING_OFFS:
                n = pl.ds(0, TILE[w])
                send(lrow.at[w, k, n], r1l.at[w, k, o - 1, n], r1l_s.at[w], r1l_r.at[w], ring(ORDERS[k][2], o))

    for i in range(NI - 1):
        batch = [(k, i) for k in KS]
        with jax.named_scope(f"arrive{i}"):
            arrive(i)
            if i == NI - 2:
                arrive(i + 1)
                batch.append((0, i + 1))
        with jax.named_scope(f"attend{i}"):
            attend(batch)
        with jax.named_scope(f"rest{i}"):
            if i == 0:
                for x in RELAYED:
                    forward(x)
            if i == SPLIT - 1:
                send1_lse(0)
            if i == NI - 2:
                send1_lse(1)
            for k, x in batch:
                send1(k, x)


    def columns(ws, k, row, n):
        wcol[k, :, :32] = jnp.concatenate(ws, axis=0).T
        t = wcol[k, pl.ds(row, n), :32]
        return lambda x, i: t[:, 8 * x + i:8 * x + i + 1]

    def weighted(cols, i, parts):
        return functools.reduce(jnp.add, [p.astype(F32) * cols(x, i) for x, p in enumerate(parts)])

    def tile_of(w, ref):
        return jnp.concatenate([ref[i] for i in range(TILE[w])] + [jnp.zeros((8 - TILE[w], LANES), F32)], axis=0)

    def merge1(w):
        cols = []
        n = pl.ds(0, TILE[w])
        wait(r1l.at[w, :, :, n], r1l_r.at[w])
        for k in KS:
            ws, l1 = _merge_weights([tile_of(w, r) for r in [lrow.at[w, k]] + [r1l.at[w, k, x] for x in KS]])
            for i in range(TILE[w]):
                lse1[w, k, i] = l1[i:i + 1]
            cols.append(columns(ws, k, ac[ORDERS[k][2]] * 32, 32))
        for k in KS:
            for o in RING_OFFS:
                send(lse1.at[w, k, n], r2l.at[w, k, o - 1, n], r2l_s.at[w], r2l_r.at[w], ring(ORDERS[k][1], o))
        wait(obuf.at[pl.ds(0, 12 * count(w))], r1_r.at[w])
        for k in KS:
            _, a2, a3 = ORDERS[k]
            its = members(w, k)
            for i in its:
                own = obuf[pl.ds(slot(k, i) + ac[a3] * 4, 4)]
                parts = [v.reshape(32, LAT) for v in [own] + [r1d[k, i, x] for x in KS]]
                y = weighted(cols[k], i - its[0], parts).astype(BF16).reshape(4, 8, LAT)
                for p in RING:
                    r1m[k, p, i] = y[p]
            for o in (2, 1, 3):
                sl = pl.ds(its[0], len(its))
                send(r1m.at[k, (ac[a2] + o) % 4, sl], r2d.at[k, o - 1, sl], r2_s, r2_r.at[w], ring(a2, o))

    def merge2(w):
        cols = []
        wait(r2l.at[w, :, :, pl.ds(0, TILE[w])], r2l_r.at[w])
        for k in KS:
            _, a2, a3 = ORDERS[k]
            ws, l2 = _merge_weights([tile_of(w, r) for r in [lse1.at[w, k]] + [r2l.at[w, k, x] for x in KS]])
            g = ac[a3] * 4 + ac[a2]
            lt = pltpu.roll(l2, ((16 - g) % 16) * 8, 1)
            s3l[w, k] = jnp.concatenate([lt] * 16, axis=0).T[0:8].reshape(8, 1, LANES)
            cols.append(columns(ws, k, g * 8, 8))
        for k in KS:
            j0 = place(k)
            for off in LINE_OFFS:
                j = (j0 + off) % 8
                send(s3l.at[w, k, j], r3l.at[w, k, j0], r3l_s, r3l_r.at[w], line(ORDERS[k][0], j))
            r3l[w, k, j0] = s3l[w, k, j0]
        wait(obuf.at[pl.ds(0, 3 * count(w))], r2_r.at[w])
        tiles = []
        for k in KS:
            its = members(w, k)
            ys = [weighted(cols[k], i - its[0], [r1m[k, ac[ORDERS[k][1]], i]] + [r2d[k, x, i] for x in KS]) for i in its]
            n = len(its)
            t = TILE[w]
            pm = _perm(8 * t, 8 * n, lambda r, c: (c == (r % t) * 8 + r // t) & (r % t < n))
            tiles.append(jnp.dot(pm, jnp.concatenate(ys, axis=0).astype(BF16), preferred_element_type=F32))
        for k in KS:
            t, s3, r3 = TILE[w], (s3a, s3b)[w], (r3a, r3b)[w]
            j0 = place(k)
            for j in range(8):
                s3[k, j] = tiles[k][t * j:t * j + t].astype(BF16)
            for off in (3, 4, 5, 2, 6, 1, 7):
                j = (j0 + off) % 8
                send(s3.at[k, j], r3.at[k, j0], r3_s.at[w], r3_r.at[w], line(ORDERS[k][0], j))
            r3[k, j0] = s3[k, j0]

    def merge3(w):
        cols = []
        wait(r3l.at[w, :, pl.ds(0, 7)], r3l_r.at[w])
        for k in KS:
            ls = [r3l[w, k, j] for j in range(8)]
            ws = [None] * 8
            for h in DIRS:
                ws[h::2], _ = _merge_weights(ls[h::2])
            cols.append(jnp.concatenate(ws, axis=0).T[0:8])
        t, r3 = TILE[w], (r3a, r3b)[w]
        wait(r3.at[:, pl.ds(0, 7)], r3_r.at[w])
        for k in KS:
            for h in DIRS:
                ts = [r3[k, j].astype(F32) * cols[k][:t, j:j + 1] for j in range(h, 8, 2)]
                fin[w, h, k, :t] = functools.reduce(jnp.add, ts)

    merge1(0)
    merge1(1)
    merge2(0)
    wait(s1buf.at[:, pl.ds(0, 7)], s1_s)
    wait(cbuf.at[pl.ds(0, 8)], c_s)
    for par in DIRS:
        its = [i for i in range(NI) for _ in ks_of(i) if i % 2 == par]
        wait(q_of(par).at[pl.ds(0, 3 * len(its))], s2_s.at[par])
        wait(q_of(par).at[pl.ds(0, 12 * len(its))], s3_s.at[par])
    merge2(1)
    merge3(0)
    wait(obuf.at[pl.ds(0, 192)], r1_s)
    for w in DIRS:
        n = pl.ds(0, TILE[w])
        wait(r1l.at[w, :, :, n], r1l_s.at[w])
        wait(r2l.at[w, :, :, n], r2l_s.at[w])
    wait(obuf.at[pl.ds(0, 48)], r2_s)
    merge3(1)
    flat = fin[...].reshape(96, LAT).astype(BF16)

    def pick(r, c):
        w, h, k, i = c // 48, (c // 24) % 2, (c // 8) % 3, c % 8
        s = 3 * (i + w * SPLIT) + k
        return (r == 16 * h + s) & (s < 16) & (i < SPLIT)

    o_ref[...] = jnp.dot(_perm(32, 96, pick), flat, preferred_element_type=F32).astype(BF16)

    wait(r3a.at[:, pl.ds(0, 7)], r3_s.at[0])
    wait(r3b.at[:, pl.ds(0, 7)], r3_s.at[1])
    wait(r3l.at[:, :, pl.ds(0, 7)], r3l_s)


def solution(mesh):
    def local(q, cache, lens):
        dma = pltpu.SemaphoreType.DMA
        V = pltpu.VMEM
        anyspace = pl.BlockSpec(memory_space=pl.ANY)
        tile, qtile = (8, LAT), (8, QW)
        line = (2, 3, 8)
        scratch = [
            pltpu.SMEM((32,), jnp.int32), V((32, QW), BF16), V((2, 3) + qtile, BF16), V((3, 8) + qtile, BF16),
            V((144, 8, LAT + LANES), BF16), V((144,) + tile, BF16),
            V((16, 64) + qtile, BF16), V((288,) + tile, BF16), V((2, 3, SPLIT, 1, LANES), F32), V((3, LANES, LANES), F32),
            V((3, NI, 3, 4) + tile, BF16), V((2, 3, 3, SPLIT, 1, LANES), F32), V((3, 4, NI) + tile, BF16), V((2, 3, SPLIT, 1, LANES), F32),
            V((3, 3, NI) + tile, BF16), V((2, 3, 3, SPLIT, 1, LANES), F32),
            V((3, 8, TILE[0], LAT), BF16), V((3, 8, TILE[1], LAT), BF16), V(line + (1, LANES), F32),
            V((3, 8, TILE[0], LAT), BF16), V((3, 8, TILE[1], LAT), BF16), V(line + (1, LANES), F32),
            V((2, 2, 3) + tile, F32),
            dma, dma, dma, dma, dma, dma, dma((2,)), dma((NI,)), dma((2,)), dma((NI,)), dma((NI,)),
            dma, dma((2,)), dma((2,)), dma((2,)), dma, dma((2,)), dma((2,)), dma((2,)), dma((2,)), dma((2,)), dma, dma((2,)),
        ]
        o = pl.pallas_call(
            _kernel,
            out_shape=V((32, LAT), BF16),
            in_specs=[anyspace] * 3,
            out_specs=pl.BlockSpec(memory_space=V),
            scratch_shapes=scratch,
            compiler_params=pltpu.CompilerParams(collective_id=0, has_side_effects=True,
                                                 vmem_limit_bytes=50 * 2 ** 20),
        )(*[pltpu.with_memory_space_constraint(v, pltpu.HBM) for v in (lens, q.reshape(32, QW), cache.reshape(32, 32, 8, QW))])
        return o.reshape(32, 1, LAT)

    return jax.shard_map(local, mesh=mesh,
                         in_specs=(P('dp', 'dcp', None), P('dp', None, 'dcp', None, None), P('dp')),
                         out_specs=P('dp', 'dcp', None), check_vma=False)
```

```python
import functools
import math

import jax
import jax.numpy as jnp
from jax import lax
from jax.experimental import pallas as pl
from jax.experimental.pallas import tpu as pltpu
from jax.sharding import PartitionSpec as P

ROPE = 64
QK_DIM = 192
SCALE2 = QK_DIM ** -0.5 * math.log2(math.e)
NEG = -3.0e38
MESH = pl.DeviceIdType.MESH
F32 = jnp.float32
BF16 = jnp.bfloat16

STRIDE = (2, 8, 32)
ORDERS = ((0, 1, 2), (1, 2, 0), (2, 0, 1))
BASE = 15
COUNT = (6, 6, 5)
NI = 6
SPLIT = 4
TILE = (SPLIT, NI - SPLIT)
ORDER, RELAYED = (0, 4, 5, 1, 2, 3), (4, 5)


LAT, QW, LANES = 512, 576, 128
KS, DIRS, RING, RING_OFFS, LINE_OFFS = range(3), range(2), range(4), range(1, 4), range(1, 8)


def _perm(rows, cols, f):
    r = lax.broadcasted_iota(jnp.int32, (rows, cols), 0)
    c = lax.broadcasted_iota(jnp.int32, (rows, cols), 1)
    return f(r, c).astype(F32).astype(BF16)


def _merge_weights(lses):
    top = functools.reduce(jnp.maximum, lses)
    ws = [jnp.exp2(v - top) for v in lses]
    tot = functools.reduce(jnp.add, ws)
    inv = 1.0 / tot
    return [w * inv for w in ws], top + jnp.log2(tot)


def _kernel(lens_h, q_h, c_h, o_ref,
            lens, q_in, s1src, s1buf, q_even, q_odd, cbuf, obuf, lrow, wcol, r1d, r1l, r1m, lse1,
            r2d, r2l, s3a, s3b, s3l, r3a, r3b, r3l, fin,
            sem_l, sem_q, c_s, c_r, s1_s, s1_r, s2_s, s2_r, s3_s, s3_r, sf_r,
            r1_s, r1_r, r1l_s, r1l_r, r2_s, r2_r, r2l_s, r2l_r, r3_s, r3_r, r3l_s, r3l_r):
    d = lax.axis_index('dcp')
    core = d % 2
    co = ((d // 2) % 4, (d // 8) % 4, d // 32)
    partner = {'dcp': d + 1 - 2 * core}

    nxt = (1, 2, 0)
    ac = [co[n] + core * (co[nxt[n]] - co[n]) for n in KS]
    stride = [STRIDE[n] + core * (STRIDE[nxt[n]] - STRIDE[n]) for n in KS]

    def ring(axis, off):
        return {'dcp': d + ((ac[axis] + off) % 4 - ac[axis]) * stride[axis]}

    def line(axis, j):
        return {'dcp': d + (j // 2 - ac[axis]) * stride[axis] + (j % 2 - core)}

    def send(src, dst, ss, rs, dev):
        pltpu.make_async_remote_copy(src_ref=src, dst_ref=dst, send_sem=ss, recv_sem=rs,
                                     device_id=dev, device_id_type=MESH).start()

    def wait(ref, sem):
        pltpu.make_async_copy(ref, ref, sem).wait()

    def ks_of(i):
        return KS if i < NI - 1 else DIRS

    def only(i, f):
        if i < NI - 1:
            f()
        else:
            pl.when(core == 1)(f)

    def by_core(f):
        for c in DIRS:
            pl.when(core == c)(functools.partial(f, c))

    bar = pltpu.get_barrier_semaphore()
    pl.semaphore_signal(bar, inc=1, device_id=partner, device_id_type=MESH)
    for off in (2, 1, 3):
        for a in KS:
            for c2 in DIRS:
                peer = d + ((co[a] + off) % 4 - co[a]) * STRIDE[a] + c2 - core
                pl.semaphore_signal(bar, inc=1, device_id={'dcp': peer}, device_id_type=MESH)
    load_q = pltpu.make_async_copy(q_h, q_in, sem_q)
    load_q.start()
    load_l = pltpu.make_async_copy(lens_h, lens, sem_l)
    load_l.start()

    def cache_rows(i, half):
        n = len(ks_of(i))
        return c_h.at[pl.ds(BASE * half + 3 * i, n)], cbuf.at[pl.ds(3 * i, n), pl.ds(32 * core, 32)]

    def load_rows(i, half):
        src, dst = cache_rows(i, half)
        pltpu.make_async_copy(src, dst, c_r).start()

    for i in range(NI - 1):
        load_rows(i, core)
    pl.when(core == 1)(lambda: load_rows(NI - 1, 1))

    lrow[...] = jnp.zeros_like(lrow)
    fin[...] = jnp.zeros_like(fin)

    @pl.when(core == 0)
    def _():
        for k in DIRS:
            obuf[pl.ds((k * NI + NI - 1) * 16, 16)] = jnp.zeros((16, 8, LAT), BF16)
            r1d[k, NI - 1] = jnp.zeros((3, 4, 8, LAT), BF16)
    load_l.wait()

    def sel(r, c):
        s = 3 * (r % 8) + (r // 8) % 3
        return (c == BASE * (r // 24) + s) & (s < BASE + 2 * (r // 24))

    load_q.wait()
    qp = jnp.dot(_perm(48, 32, sel), q_in[...], preferred_element_type=F32).astype(BF16)
    s1src[...] = qp.reshape(2, 3, 8, QW)
    pl.semaphore_wait(bar, 19)

    def place(k):
        return ac[ORDERS[k][0]] * 2 + core

    for k in KS:
        n = ORDERS[k][0]
        j0 = place(k)
        oc = co[n] + co[nxt[n]] - ac[n]
        ost = STRIDE[n] + STRIDE[nxt[n]] - stride[n]
        for off in (2, 1, 3):
            send(s1src.at[core, k], s1buf.at[k, j0], s1_s, s1_r, ring(n, off))
        for off in (2, 1, 3, 0):
            peer = {'dcp': d + ((oc + off) % 4 - oc) * ost + 1 - 2 * core}
            send(s1src.at[1 - core, k], s1buf.at[k, oc * 2 + core], s1_s, s1_r, peer)
        s1buf[k, j0] = s1src[core, k]

    def push_rows(i, half):
        src, dst = cache_rows(i, half)
        send(src, dst, c_s, c_r, partner)

    for i in range(NI - 1):
        push_rows(i, 1 - core)
    pl.when(core == 0)(lambda: push_rows(NI - 1, 1))

    def q_of(i):
        return q_odd if i % 2 else q_even

    def q_slot(k, i):
        return (k * 3 + i // 2) * 16

    def slot(k, i):
        return (k * NI + i) * 16

    def blk(k, i, off):
        _, a2, a3 = ORDERS[k]
        return q_of(i).at[q_slot(k, i) + ac[a3] * 4 + (ac[a2] - off) % 4]

    def copy3(k, i, off):
        b = blk(k, i, off)
        a3 = ORDERS[k][2]
        for o in (1, 3) if i in RELAYED else (2, 1, 3):
            onward = i in RELAYED and off // 2 == o // 2
            send(b, b, s3_s.at[i % 2], sf_r.at[i] if onward else s3_r.at[i], ring(a3, o))

    def stage2(k, i):
        b = blk(k, i, 0)
        for off in (2, 1, 3):
            send(b, b, s2_s.at[i % 2], s2_r.at[i], ring(ORDERS[k][1], off))
        copy3(k, i, 0)

    tr = _perm(64, 64, lambda r, c: (r // 8 == c % 8) & (r % 8 == c // 8))
    wait(s1buf.at[:, pl.ds(0, 7)], s1_r)
    turned = [jnp.dot(tr, s1buf[k].reshape(64, QW), preferred_element_type=F32) for k in KS]
    for k in KS:
        rows = turned[k]
        _, a2, a3 = ORDERS[k]
        for i in range(COUNT[k]):
            y = rows[8 * i:8 * i + 8, :LAT if i % 2 else QW]
            if i % 2 == 0:
                y = jnp.concatenate([y, rows[8 * i + 8:8 * i + 16, LAT:]], axis=1)
            q_of(i)[q_slot(k, i) + ac[a3] * 4 + ac[a2]] = y.astype(BF16)
    def rows2(i):
        for k in ks_of(i):
            stage2(k, i)

    for i in ORDER:
        only(i, functools.partial(rows2, i))

    def stage3(i):
        n = len(ks_of(i))
        wait(q_of(i).at[pl.ds(0, 3 * n)], s2_r.at[i])
        for off in (1, 3, 2):
            for k in ks_of(i):
                copy3(k, i, off)

    def forward(i):
        wait(q_of(i).at[pl.ds(0, 4 * len(ks_of(i)))], sf_r.at[i])
        for off in RING:
            for k in ks_of(i):
                _, a2, a3 = ORDERS[k]
                o = 1 if off < 2 else 3
                b = q_of(i).at[q_slot(k, i) + ((ac[a3] - o) % 4) * 4 + (ac[a2] - off) % 4]
                send(b, b, s3_s.at[i % 2], s3_r.at[i], ring(a3, o))

    def arrive(i):
        n = len(ks_of(i))
        if i == 0:
            by_core(lambda c: wait(cbuf.at[pl.ds(0, BASE + 2 * c)], c_r))
        wait(q_of(i).at[pl.ds(0, (8 if i in RELAYED else 12) * n)], s3_r.at[i])

    for i in ORDER:
        only(i, functools.partial(stage3, i))

    chip8 = (d // 2) * 16

    j = lax.broadcasted_iota(jnp.int32, (LAT, LANES), 0)
    pos = (j & 7) + ((j >> 3) & 31) * 1024 + (j >> 8) * 8

    def cache_of(k, i):
        return cbuf[3 * i + k].reshape(LAT, QW)

    def scores(k, i):
        cs = cache_of(k, i)
        n = pl.ds(q_slot(k, i), 16)
        lat = q_of(i)[n, :, :LAT].reshape(LANES, LAT)
        rope = q_even[n, :, LAT:].reshape(LANES, LANES)
        rope = rope[:, ROPE:] if i % 2 else rope[:, :ROPE]
        dims = (((1,), (1,)), ((), ()))
        st = lax.dot_general(cs[:, :LAT], lat, dims, preferred_element_type=F32)
        return (st + lax.dot_general(cs[:, LAT:], rope, dims, preferred_element_type=F32)) * SCALE2

    def softmax(st, k, i):
        ok = pos < lens[BASE * core + 3 * i + k] - chip8
        st = jnp.where(ok, st, NEG)
        m = jnp.max(st, axis=0, keepdims=True)
        has = m > NEG
        p = jnp.exp2(st - jnp.where(has, m, 0.0))
        ls = jnp.where(has, jnp.sum(p, axis=0, keepdims=True), 1.0)
        w = wave(i)
        lrow[w, k, i - w * SPLIT] = jnp.where(has, m + jnp.log2(ls), NEG)
        return (p * (1.0 / ls)).astype(BF16)

    def attend(batch):
        sts = [scores(k, i) for k, i in batch]
        ps = [softmax(st, k, i) for st, (k, i) in zip(sts, batch)]
        outs = [lax.dot_general(p, cache_of(k, i)[:, :LAT], (((0,), (0,)), ((), ())), preferred_element_type=F32)
                for p, (k, i) in zip(ps, batch)]
        for o, (k, i) in zip(outs, batch):
            obuf[pl.ds(slot(k, i), 16)] = o.astype(BF16).reshape(16, 8, LAT)

    def wave(i):
        return 0 if i < SPLIT else 1

    def send1(batch):
        for o, (k, i) in [(o, x) for o in (2, 1, 3) for x in batch]:
            a3 = ORDERS[k][2]
            b = obuf.at[pl.ds(slot(k, i) + ((ac[a3] + o) % 4) * 4, 4)]
            send(b, r1d.at[k, i, o - 1], r1_s, r1_r.at[wave(i)], ring(a3, o))

    def members(w, k):
        return range(SPLIT) if w == 0 else range(SPLIT, COUNT[k])

    def count(w):
        return sum(len(members(w, k)) for k in KS)

    def send1_lse(w):
        for k in KS:
            for o in RING_OFFS:
                n = pl.ds(0, TILE[w])
                send(lrow.at[w, k, n], r1l.at[w, k, o - 1, n], r1l_s.at[w], r1l_r.at[w], ring(ORDERS[k][2], o))

    for i in range(NI - 2):
        batch = [(k, i) for k in KS]
        with jax.named_scope(f"arrive{i}"):
            arrive(i)
        with jax.named_scope(f"attend{i}"):
            attend(batch)
        with jax.named_scope(f"rest{i}"):
            if i == 0:
                for x in RELAYED:
                    only(x, functools.partial(forward, x))
            if i == SPLIT - 1:
                send1_lse(0)
            send1(batch)


    @by_core
    def _(c):
        last = range(NI - 2, NI - 1 + c)
        for i in last:
            arrive(i)
        batch = [(k, i) for i in last for k in ks_of(i)]
        attend(batch)
        send1_lse(1)
        send1(batch)


    def columns(ws, k, row, n):
        wcol[k, :, :32] = jnp.concatenate(ws, axis=0).T
        t = wcol[k, pl.ds(row, n), :32]
        return lambda x, i: t[:, 8 * x + i:8 * x + i + 1]

    def weighted(cols, i, parts):
        return functools.reduce(jnp.add, [p.astype(F32) * cols(x, i) for x, p in enumerate(parts)])

    def tile_of(w, ref):
        return jnp.concatenate([ref[i] for i in range(TILE[w])] + [jnp.zeros((8 - TILE[w], LANES), F32)], axis=0)

    def merge1(w):
        cols = []
        n = pl.ds(0, TILE[w])
        wait(r1l.at[w, :, :, n], r1l_r.at[w])
        for k in KS:
            ws, l1 = _merge_weights([tile_of(w, r) for r in [lrow.at[w, k]] + [r1l.at[w, k, x] for x in KS]])
            for i in range(TILE[w]):
                lse1[w, k, i] = l1[i:i + 1]
            cols.append(columns(ws, k, ac[ORDERS[k][2]] * 32, 32))
        for k in KS:
            for o in RING_OFFS:
                send(lse1.at[w, k, n], r2l.at[w, k, o - 1, n], r2l_s.at[w], r2l_r.at[w], ring(ORDERS[k][1], o))
        if w == 0:
            wait(obuf.at[pl.ds(0, 12 * count(w))], r1_r.at[w])
        else:
            by_core(lambda c: wait(obuf.at[pl.ds(0, 12 * (count(1) - 2 + 2 * c))], r1_r.at[w]))
        for k in KS:
            _, a2, a3 = ORDERS[k]
            its = members(w, k)
            for i in its:
                own = obuf[pl.ds(slot(k, i) + ac[a3] * 4, 4)]
                parts = [v.reshape(32, LAT) for v in [own] + [r1d[k, i, x] for x in KS]]
                y = weighted(cols[k], i - its[0], parts).astype(BF16).reshape(4, 8, LAT)
                for p in RING:
                    r1m[k, p, i] = y[p]
            for o in (2, 1, 3):
                sl = pl.ds(its[0], len(its))
                send(r1m.at[k, (ac[a2] + o) % 4, sl], r2d.at[k, o - 1, sl], r2_s, r2_r.at[w], ring(a2, o))

    def merge2(w):
        cols = []
        wait(r2l.at[w, :, :, pl.ds(0, TILE[w])], r2l_r.at[w])
        for k in KS:
            _, a2, a3 = ORDERS[k]
            ws, l2 = _merge_weights([tile_of(w, r) for r in [lse1.at[w, k]] + [r2l.at[w, k, x] for x in KS]])
            g = ac[a3] * 4 + ac[a2]
            lt = pltpu.roll(l2, ((16 - g) % 16) * 8, 1)
            s3l[w, k] = jnp.concatenate([lt] * 16, axis=0).T[0:8].reshape(8, 1, LANES)
            cols.append(columns(ws, k, g * 8, 8))
        for k in KS:
            j0 = place(k)
            for off in LINE_OFFS:
                j = (j0 + off) % 8
                send(s3l.at[w, k, j], r3l.at[w, k, j0], r3l_s, r3l_r.at[w], line(ORDERS[k][0], j))
            r3l[w, k, j0] = s3l[w, k, j0]
        wait(obuf.at[pl.ds(0, 3 * count(w))], r2_r.at[w])
        tiles = []
        for k in KS:
            its = members(w, k)
            ys = [weighted(cols[k], i - its[0], [r1m[k, ac[ORDERS[k][1]], i]] + [r2d[k, x, i] for x in KS]) for i in its]
            n = len(its)
            t = TILE[w]
            pm = _perm(8 * t, 8 * n, lambda r, c: (c == (r % t) * 8 + r // t) & (r % t < n))
            tiles.append(jnp.dot(pm, jnp.concatenate(ys, axis=0).astype(BF16), preferred_element_type=F32))
        for k in KS:
            t, s3, r3 = TILE[w], (s3a, s3b)[w], (r3a, r3b)[w]
            j0 = place(k)
            for j in range(8):
                s3[k, j] = tiles[k][t * j:t * j + t].astype(BF16)
            for off in (3, 4, 5, 2, 6, 1, 7):
                j = (j0 + off) % 8
                send(s3.at[k, j], r3.at[k, j0], r3_s.at[w], r3_r.at[w], line(ORDERS[k][0], j))
            r3[k, j0] = s3[k, j0]

    def merge3(w):
        cols = []
        wait(r3l.at[w, :, pl.ds(0, 7)], r3l_r.at[w])
        for k in KS:
            ls = [r3l[w, k, j] for j in range(8)]
            ws = [None] * 8
            for h in DIRS:
                ws[h::2], _ = _merge_weights(ls[h::2])
            cols.append(jnp.concatenate(ws, axis=0).T[0:8])
        t, r3 = TILE[w], (r3a, r3b)[w]
        wait(r3.at[:, pl.ds(0, 7)], r3_r.at[w])
        for k in KS:
            for h in DIRS:
                ts = [r3[k, j].astype(F32) * cols[k][:t, j:j + 1] for j in range(h, 8, 2)]
                fin[w, h, k, :t] = functools.reduce(jnp.add, ts)

    merge1(0)
    merge1(1)
    merge2(0)
    wait(s1buf.at[:, pl.ds(0, 7)], s1_s)

    @by_core
    def _(c):
        wait(cbuf.at[pl.ds(0, BASE + 2 * (1 - c)), pl.ds(0, 32)], c_s)
        for par in DIRS:
            its = [i for i in range(NI - 1 + c) for _ in ks_of(i) if i % 2 == par]
            wait(q_of(par).at[pl.ds(0, 3 * len(its))], s2_s.at[par])
            wait(q_of(par).at[pl.ds(0, 12 * len(its))], s3_s.at[par])

    merge2(1)
    merge3(0)
    by_core(lambda c: wait(obuf.at[pl.ds(0, 12 * (BASE + 2 * c))], r1_s))
    for w in DIRS:
        n = pl.ds(0, TILE[w])
        wait(r1l.at[w, :, :, n], r1l_s.at[w])
        wait(r2l.at[w, :, :, n], r2l_s.at[w])
    wait(obuf.at[pl.ds(0, 51)], r2_s)
    merge3(1)
    flat = fin[...].reshape(96, LAT).astype(BF16)

    def pick(r, c):
        w, h, k, i = c // 48, (c // 24) % 2, (c // 8) % 3, c % 8
        s = 3 * (i + w * SPLIT) + k
        return (r == BASE * h + s) & (s < BASE + 2 * h) & (i < SPLIT)

    o_ref[...] = jnp.dot(_perm(32, 96, pick), flat, preferred_element_type=F32).astype(BF16)

    wait(r3a.at[:, pl.ds(0, 7)], r3_s.at[0])
    wait(r3b.at[:, pl.ds(0, 7)], r3_s.at[1])
    wait(r3l.at[:, :, pl.ds(0, 7)], r3l_s)


def solution(mesh):
    def local(q, cache, lens):
        dma = pltpu.SemaphoreType.DMA
        V = pltpu.VMEM
        anyspace = pl.BlockSpec(memory_space=pl.ANY)
        tile, qtile = (8, LAT), (8, QW)
        line = (2, 3, 8)
        scratch = [
            pltpu.SMEM((32,), jnp.int32), V((32, QW), BF16), V((2, 3) + qtile, BF16), V((3, 8) + qtile, BF16),
            V((144, 8, LAT + LANES), BF16), V((144,) + tile, BF16),
            V((BASE + 2, 64) + qtile, BF16), V((288,) + tile, BF16), V((2, 3, SPLIT, 1, LANES), F32), V((3, LANES, LANES), F32),
            V((3, NI, 3, 4) + tile, BF16), V((2, 3, 3, SPLIT, 1, LANES), F32), V((3, 4, NI) + tile, BF16), V((2, 3, SPLIT, 1, LANES), F32),
            V((3, 3, NI) + tile, BF16), V((2, 3, 3, SPLIT, 1, LANES), F32),
            V((3, 8, TILE[0], LAT), BF16), V((3, 8, TILE[1], LAT), BF16), V(line + (1, LANES), F32),
            V((3, 8, TILE[0], LAT), BF16), V((3, 8, TILE[1], LAT), BF16), V(line + (1, LANES), F32),
            V((2, 2, 3) + tile, F32),
            dma, dma, dma, dma, dma, dma, dma((2,)), dma((NI,)), dma((2,)), dma((NI,)), dma((NI,)),
            dma, dma((2,)), dma((2,)), dma((2,)), dma, dma((2,)), dma((2,)), dma((2,)), dma((2,)), dma((2,)), dma, dma((2,)),
        ]
        o = pl.pallas_call(
            _kernel,
            out_shape=V((32, LAT), BF16),
            in_specs=[anyspace] * 3,
            out_specs=pl.BlockSpec(memory_space=V),
            scratch_shapes=scratch,
            compiler_params=pltpu.CompilerParams(collective_id=0, has_side_effects=True,
                                                 vmem_limit_bytes=50 * 2 ** 20),
        )(*[pltpu.with_memory_space_constraint(v, pltpu.HBM) for v in (lens, q.reshape(32, QW), cache.reshape(32, 32, 8, QW))])
        return o.reshape(32, 1, LAT)

    return jax.shard_map(local, mesh=mesh,
                         in_specs=(P('dp', 'dcp', None), P('dp', None, 'dcp', None, None), P('dp')),
                         out_specs=P('dp', 'dcp', None), check_vma=False)
```

```python
import functools
import math

import jax
import jax.numpy as jnp
from jax import lax
from jax.experimental import pallas as pl
from jax.experimental.pallas import tpu as pltpu
from jax.sharding import PartitionSpec as P

ROPE = 64
QK_DIM = 192
SCALE2 = QK_DIM ** -0.5 * math.log2(math.e)
NEG = -3.0e38
MESH = pl.DeviceIdType.MESH
F32 = jnp.float32
BF16 = jnp.bfloat16

STRIDE = (2, 8, 32)
ORDERS = ((0, 1, 2), (1, 2, 0), (2, 0, 1))
BASE = 15
COUNT = (6, 6, 5)
NI = 6
SPLIT = 4
TILE = (SPLIT, NI - SPLIT)
ORDER, RELAYED = (0, 4, 5, 1, 2, 3), (4, 5)


LAT, QW, LANES = 512, 576, 128
KS, DIRS, RING, RING_OFFS, LINE_OFFS = range(3), range(2), range(4), range(1, 4), range(1, 8)


def _perm(rows, cols, f):
    r = lax.broadcasted_iota(jnp.int32, (rows, cols), 0)
    c = lax.broadcasted_iota(jnp.int32, (rows, cols), 1)
    return f(r, c).astype(F32).astype(BF16)


def _merge_weights(lses):
    top = functools.reduce(jnp.maximum, lses)
    ws = [jnp.exp2(v - top) for v in lses]
    tot = functools.reduce(jnp.add, ws)
    inv = 1.0 / tot
    return [w * inv for w in ws], top + jnp.log2(tot)


def _kernel(lens_h, q_h, c_h, o_ref,
            lens, q_in, s1a, s1b, b1a, b1b, q_even, q_odd, cbuf, obuf, lrow, wcol, r1d, r1l, r1m, lse1,
            r2d, r2l, s3a, s3b, s3l, r3a, r3b, r3l, fin,
            sem_l, sem_q, c_s, c_r, s1_s, s1_r, s2_s, s2_r, s3_s, s3_r, sf_r,
            r1_s, r1_r, r1l_s, r1l_r, r2_s, r2_r, r2l_s, r2l_r, r3_s, r3_r, r3l_s, r3l_r):
    d = lax.axis_index('dcp')
    core = d % 2
    co = ((d // 2) % 4, (d // 8) % 4, d // 32)
    partner = {'dcp': d + 1 - 2 * core}

    nxt = (1, 2, 0)
    ac = [co[n] + core * (co[nxt[n]] - co[n]) for n in KS]
    stride = [STRIDE[n] + core * (STRIDE[nxt[n]] - STRIDE[n]) for n in KS]

    def ring(axis, off):
        return {'dcp': d + ((ac[axis] + off) % 4 - ac[axis]) * stride[axis]}

    def line(axis, j):
        return {'dcp': d + (j // 2 - ac[axis]) * stride[axis] + (j % 2 - core)}

    def send(src, dst, ss, rs, dev):
        pltpu.make_async_remote_copy(src_ref=src, dst_ref=dst, send_sem=ss, recv_sem=rs,
                                     device_id=dev, device_id_type=MESH).start()

    def wait(ref, sem):
        pltpu.make_async_copy(ref, ref, sem).wait()

    def ks_of(i):
        return KS if i < NI - 1 else DIRS

    def only(i, f):
        if i < NI - 1:
            f()
        else:
            pl.when(core == 1)(f)

    def by_core(f):
        for c in DIRS:
            pl.when(core == c)(functools.partial(f, c))

    bar = pltpu.get_barrier_semaphore()
    pl.semaphore_signal(bar, inc=1, device_id=partner, device_id_type=MESH)
    for off in (2, 1, 3):
        for a in KS:
            for c2 in DIRS:
                peer = d + ((co[a] + off) % 4 - co[a]) * STRIDE[a] + c2 - core
                pl.semaphore_signal(bar, inc=1, device_id={'dcp': peer}, device_id_type=MESH)
    load_q = pltpu.make_async_copy(q_h, q_in, sem_q)
    load_q.start()
    load_l = pltpu.make_async_copy(lens_h, lens, sem_l)
    load_l.start()

    def cache_rows(i, half):
        n = len(ks_of(i))
        return c_h.at[pl.ds(BASE * half + 3 * i, n)], cbuf.at[pl.ds(3 * i, n), pl.ds(32 * core, 32)]

    def load_rows(i, half):
        src, dst = cache_rows(i, half)
        pltpu.make_async_copy(src, dst, c_r).start()

    for i in range(NI - 1):
        load_rows(i, core)
    pl.when(core == 1)(lambda: load_rows(NI - 1, 1))

    lrow[...] = jnp.zeros_like(lrow)
    fin[...] = jnp.zeros_like(fin)

    @pl.when(core == 0)
    def _():
        for k in DIRS:
            obuf[pl.ds((k * NI + NI - 1) * 16, 16)] = jnp.zeros((16, 8, LAT), BF16)
            r1d[k, NI - 1] = jnp.zeros((3, 4, 8, LAT), BF16)
    load_l.wait()

    def sel(r, c):
        s = 3 * (r % 8) + (r // 8) % 3
        return (c == BASE * (r // 24) + s) & (s < BASE + 2 * (r // 24))

    load_q.wait()
    qp = jnp.dot(_perm(48, 32, sel), q_in[...], preferred_element_type=F32)
    for c in DIRS:
        for k in KS:
            r = 8 * (3 * c + k)
            s1a[c, k] = qp[r:r + 2].astype(BF16)
            s1b[c, k] = qp[r + 2:r + 6].astype(BF16)
    pl.semaphore_wait(bar, 19)

    def place(k):
        return ac[ORDERS[k][0]] * 2 + core

    for part, (src, dst) in enumerate(((s1a, b1a), (s1b, b1b))):
        for k in KS:
            n = ORDERS[k][0]
            j0 = place(k)
            oc = co[n] + co[nxt[n]] - ac[n]
            ost = STRIDE[n] + STRIDE[nxt[n]] - stride[n]
            for off in (2, 1, 3):
                send(src.at[core, k], dst.at[k, j0], s1_s.at[part], s1_r.at[part], ring(n, off))
            for off in (2, 1, 3, 0):
                peer = {'dcp': d + ((oc + off) % 4 - oc) * ost + 1 - 2 * core}
                send(src.at[1 - core, k], dst.at[k, oc * 2 + core], s1_s.at[part], s1_r.at[part], peer)
            dst[k, j0] = src[core, k]

    def push_rows(i, half):
        src, dst = cache_rows(i, half)
        send(src, dst, c_s, c_r, partner)

    for i in range(NI - 1):
        push_rows(i, 1 - core)
    pl.when(core == 0)(lambda: push_rows(NI - 1, 1))

    def q_of(i):
        return q_odd if i % 2 else q_even

    def q_slot(k, i):
        return (k * 3 + i // 2) * 16

    def slot(k, i):
        return (k * NI + i) * 16

    def blk(k, i, off):
        _, a2, a3 = ORDERS[k]
        return q_of(i).at[q_slot(k, i) + ac[a3] * 4 + (ac[a2] - off) % 4]

    def copy3(k, i, off):
        b = blk(k, i, off)
        a3 = ORDERS[k][2]
        for o in (1, 3) if i in RELAYED else (2, 1, 3):
            onward = i in RELAYED and off // 2 == o // 2
            send(b, b, s3_s.at[i % 2], sf_r.at[i] if onward else s3_r.at[i], ring(a3, o))

    def stage2(k, i):
        b = blk(k, i, 0)
        for off in (2, 1, 3):
            send(b, b, s2_s.at[i % 2], s2_r.at[i], ring(ORDERS[k][1], off))
        copy3(k, i, 0)

    def rows2(i):
        for k in ks_of(i):
            stage2(k, i)

    def turn(buf, part, first, n):
        wait(buf.at[:, pl.ds(0, 7)], s1_r.at[part])
        tr = _perm(8 * n, 8 * n, lambda r, c: (r // 8 == c % n) & (r % 8 == c // n))
        ins = [jnp.concatenate([buf[k, j].astype(F32) for j in range(8)], axis=0).astype(BF16) for k in KS]
        outs = [jnp.dot(tr, v, preferred_element_type=F32) for v in ins]
        for k in KS:
            _, a2, a3 = ORDERS[k]
            for i in range(first, min(first + n, COUNT[k])):
                r = 8 * (i - first)
                y = outs[k][r:r + 8, :LAT if i % 2 else QW]
                if i % 2 == 0:
                    y = jnp.concatenate([y, outs[k][r + 8:r + 16, LAT:]], axis=1)
                q_of(i)[q_slot(k, i) + ac[a3] * 4 + ac[a2]] = y.astype(BF16)

    turn(b1a, 0, 0, 2)
    for i in range(2):
        rows2(i)
    turn(b1b, 1, 2, 4)
    for i in ORDER:
        if i > 1:
            only(i, functools.partial(rows2, i))

    def stage3(i):
        n = len(ks_of(i))
        wait(q_of(i).at[pl.ds(0, 3 * n)], s2_r.at[i])
        for off in (1, 3, 2):
            for k in ks_of(i):
                copy3(k, i, off)

    def forward(i):
        wait(q_of(i).at[pl.ds(0, 4 * len(ks_of(i)))], sf_r.at[i])
        for off in RING:
            for k in ks_of(i):
                _, a2, a3 = ORDERS[k]
                o = 1 if off < 2 else 3
                b = q_of(i).at[q_slot(k, i) + ((ac[a3] - o) % 4) * 4 + (ac[a2] - off) % 4]
                send(b, b, s3_s.at[i % 2], s3_r.at[i], ring(a3, o))

    def arrive(i):
        n = len(ks_of(i))
        if i == 0:
            by_core(lambda c: wait(cbuf.at[pl.ds(0, BASE + 2 * c)], c_r))
        wait(q_of(i).at[pl.ds(0, (8 if i in RELAYED else 12) * n)], s3_r.at[i])

    for i in ORDER:
        only(i, functools.partial(stage3, i))

    chip8 = (d // 2) * 16

    j = lax.broadcasted_iota(jnp.int32, (LAT, LANES), 0)
    pos = (j & 7) + ((j >> 3) & 31) * 1024 + (j >> 8) * 8

    def cache_of(k, i):
        return cbuf[3 * i + k].reshape(LAT, QW)

    def scores(k, i):
        cs = cache_of(k, i)
        n = pl.ds(q_slot(k, i), 16)
        lat = q_of(i)[n, :, :LAT].reshape(LANES, LAT)
        rope = q_even[n, :, LAT:].reshape(LANES, LANES)
        rope = rope[:, ROPE:] if i % 2 else rope[:, :ROPE]
        dims = (((1,), (1,)), ((), ()))
        st = lax.dot_general(cs[:, :LAT], lat, dims, preferred_element_type=F32)
        return (st + lax.dot_general(cs[:, LAT:], rope, dims, preferred_element_type=F32)) * SCALE2

    def softmax(st, k, i):
        ok = pos < lens[BASE * core + 3 * i + k] - chip8
        st = jnp.where(ok, st, NEG)
        m = jnp.max(st, axis=0, keepdims=True)
        has = m > NEG
        p = jnp.exp2(st - jnp.where(has, m, 0.0))
        ls = jnp.where(has, jnp.sum(p, axis=0, keepdims=True), 1.0)
        w = wave(i)
        lrow[w, k, i - w * SPLIT] = jnp.where(has, m + jnp.log2(ls), NEG)
        return (p * (1.0 / ls)).astype(BF16)

    def attend(batch):
        sts = [scores(k, i) for k, i in batch]
        ps = [softmax(st, k, i) for st, (k, i) in zip(sts, batch)]
        outs = [lax.dot_general(p, cache_of(k, i)[:, :LAT], (((0,), (0,)), ((), ())), preferred_element_type=F32)
                for p, (k, i) in zip(ps, batch)]
        for o, (k, i) in zip(outs, batch):
            obuf[pl.ds(slot(k, i), 16)] = o.astype(BF16).reshape(16, 8, LAT)

    def wave(i):
        return 0 if i < SPLIT else 1

    def send1(batch):
        for o, (k, i) in [(o, x) for o in (2, 1, 3) for x in batch]:
            a3 = ORDERS[k][2]
            b = obuf.at[pl.ds(slot(k, i) + ((ac[a3] + o) % 4) * 4, 4)]
            send(b, r1d.at[k, i, o - 1], r1_s, r1_r.at[wave(i)], ring(a3, o))

    def members(w, k):
        return range(SPLIT) if w == 0 else range(SPLIT, COUNT[k])

    def count(w):
        return sum(len(members(w, k)) for k in KS)

    def send1_lse(w):
        for k in KS:
            for o in RING_OFFS:
                n = pl.ds(0, TILE[w])
                send(lrow.at[w, k, n], r1l.at[w, k, o - 1, n], r1l_s.at[w], r1l_r.at[w], ring(ORDERS[k][2], o))

    for i in range(NI - 2):
        batch = [(k, i) for k in KS]
        with jax.named_scope(f"arrive{i}"):
            arrive(i)
        with jax.named_scope(f"attend{i}"):
            attend(batch)
        with jax.named_scope(f"rest{i}"):
            if i == 0:
                for x in RELAYED:
                    only(x, functools.partial(forward, x))
            if i == SPLIT - 1:
                send1_lse(0)
            send1(batch)


    @by_core
    def _(c):
        last = range(NI - 2, NI - 1 + c)
        for i in last:
            arrive(i)
        batch = [(k, i) for i in last for k in ks_of(i)]
        attend(batch)
        send1_lse(1)
        send1(batch)


    def columns(ws, k, row, n):
        wcol[k, :, :32] = jnp.concatenate(ws, axis=0).T
        t = wcol[k, pl.ds(row, n), :32]
        return lambda x, i: t[:, 8 * x + i:8 * x + i + 1]

    def weighted(cols, i, parts):
        return functools.reduce(jnp.add, [p.astype(F32) * cols(x, i) for x, p in enumerate(parts)])

    def tile_of(w, ref):
        return jnp.concatenate([ref[i] for i in range(TILE[w])] + [jnp.zeros((8 - TILE[w], LANES), F32)], axis=0)

    def merge1(w):
        cols = []
        n = pl.ds(0, TILE[w])
        wait(r1l.at[w, :, :, n], r1l_r.at[w])
        for k in KS:
            ws, l1 = _merge_weights([tile_of(w, r) for r in [lrow.at[w, k]] + [r1l.at[w, k, x] for x in KS]])
            for i in range(TILE[w]):
                lse1[w, k, i] = l1[i:i + 1]
            cols.append(columns(ws, k, ac[ORDERS[k][2]] * 32, 32))
        for k in KS:
            for o in RING_OFFS:
                send(lse1.at[w, k, n], r2l.at[w, k, o - 1, n], r2l_s.at[w], r2l_r.at[w], ring(ORDERS[k][1], o))
        if w == 0:
            wait(obuf.at[pl.ds(0, 12 * count(w))], r1_r.at[w])
        else:
            by_core(lambda c: wait(obuf.at[pl.ds(0, 12 * (count(1) - 2 + 2 * c))], r1_r.at[w]))
        for k in KS:
            _, a2, a3 = ORDERS[k]
            its = members(w, k)
            for i in its:
                own = obuf[pl.ds(slot(k, i) + ac[a3] * 4, 4)]
                parts = [v.reshape(32, LAT) for v in [own] + [r1d[k, i, x] for x in KS]]
                y = weighted(cols[k], i - its[0], parts).astype(BF16).reshape(4, 8, LAT)
                for p in RING:
                    r1m[k, p, i] = y[p]
            for o in (2, 1, 3):
                sl = pl.ds(its[0], len(its))
                send(r1m.at[k, (ac[a2] + o) % 4, sl], r2d.at[k, o - 1, sl], r2_s, r2_r.at[w], ring(a2, o))

    def merge2(w):
        cols = []
        wait(r2l.at[w, :, :, pl.ds(0, TILE[w])], r2l_r.at[w])
        for k in KS:
            _, a2, a3 = ORDERS[k]
            ws, l2 = _merge_weights([tile_of(w, r) for r in [lse1.at[w, k]] + [r2l.at[w, k, x] for x in KS]])
            g = ac[a3] * 4 + ac[a2]
            lt = pltpu.roll(l2, ((16 - g) % 16) * 8, 1)
            s3l[w, k] = jnp.concatenate([lt] * 16, axis=0).T[0:8].reshape(8, 1, LANES)
            cols.append(columns(ws, k, g * 8, 8))
        for k in KS:
            j0 = place(k)
            for off in LINE_OFFS:
                j = (j0 + off) % 8
                send(s3l.at[w, k, j], r3l.at[w, k, j0], r3l_s, r3l_r.at[w], line(ORDERS[k][0], j))
            r3l[w, k, j0] = s3l[w, k, j0]
        wait(obuf.at[pl.ds(0, 3 * count(w))], r2_r.at[w])
        tiles = []
        for k in KS:
            its = members(w, k)
            ys = [weighted(cols[k], i - its[0], [r1m[k, ac[ORDERS[k][1]], i]] + [r2d[k, x, i] for x in KS]) for i in its]
            n = len(its)
            t = TILE[w]
            pm = _perm(8 * t, 8 * n, lambda r, c: (c == (r % t) * 8 + r // t) & (r % t < n))
            tiles.append(jnp.dot(pm, jnp.concatenate(ys, axis=0).astype(BF16), preferred_element_type=F32))
        for k in KS:
            t, s3, r3 = TILE[w], (s3a, s3b)[w], (r3a, r3b)[w]
            j0 = place(k)
            for j in range(8):
                s3[k, j] = tiles[k][t * j:t * j + t].astype(BF16)
            for off in (3, 4, 5, 2, 6, 1, 7):
                j = (j0 + off) % 8
                send(s3.at[k, j], r3.at[k, j0], r3_s.at[w], r3_r.at[w], line(ORDERS[k][0], j))
            r3[k, j0] = s3[k, j0]

    def merge3(w):
        cols = []
        wait(r3l.at[w, :, pl.ds(0, 7)], r3l_r.at[w])
        for k in KS:
            ls = [r3l[w, k, j] for j in range(8)]
            ws = [None] * 8
            for h in DIRS:
                ws[h::2], _ = _merge_weights(ls[h::2])
            cols.append(jnp.concatenate(ws, axis=0).T[0:8])
        t, r3 = TILE[w], (r3a, r3b)[w]
        wait(r3.at[:, pl.ds(0, 7)], r3_r.at[w])
        for k in KS:
            for h in DIRS:
                ts = [r3[k, j].astype(F32) * cols[k][:t, j:j + 1] for j in range(h, 8, 2)]
                fin[w, h, k, :t] = functools.reduce(jnp.add, ts)

    merge1(0)
    merge1(1)
    merge2(0)
    wait(b1a.at[:, pl.ds(0, 7)], s1_s.at[0])
    wait(b1b.at[:, pl.ds(0, 7)], s1_s.at[1])

    @by_core
    def _(c):
        wait(cbuf.at[pl.ds(0, BASE + 2 * (1 - c)), pl.ds(0, 32)], c_s)
        for par in DIRS:
            its = [i for i in range(NI - 1 + c) for _ in ks_of(i) if i % 2 == par]
            wait(q_of(par).at[pl.ds(0, 3 * len(its))], s2_s.at[par])
            wait(q_of(par).at[pl.ds(0, 12 * len(its))], s3_s.at[par])

    merge2(1)
    merge3(0)
    by_core(lambda c: wait(obuf.at[pl.ds(0, 12 * (BASE + 2 * c))], r1_s))
    for w in DIRS:
        n = pl.ds(0, TILE[w])
        wait(r1l.at[w, :, :, n], r1l_s.at[w])
        wait(r2l.at[w, :, :, n], r2l_s.at[w])
    wait(obuf.at[pl.ds(0, 51)], r2_s)
    merge3(1)
    flat = fin[...].reshape(96, LAT).astype(BF16)

    def pick(r, c):
        w, h, k, i = c // 48, (c // 24) % 2, (c // 8) % 3, c % 8
        s = 3 * (i + w * SPLIT) + k
        return (r == BASE * h + s) & (s < BASE + 2 * h) & (i < SPLIT)

    o_ref[...] = jnp.dot(_perm(32, 96, pick), flat, preferred_element_type=F32).astype(BF16)

    wait(r3a.at[:, pl.ds(0, 7)], r3_s.at[0])
    wait(r3b.at[:, pl.ds(0, 7)], r3_s.at[1])
    wait(r3l.at[:, :, pl.ds(0, 7)], r3l_s)


def solution(mesh):
    def local(q, cache, lens):
        dma = pltpu.SemaphoreType.DMA
        V = pltpu.VMEM
        anyspace = pl.BlockSpec(memory_space=pl.ANY)
        tile, qtile = (8, LAT), (8, QW)
        line = (2, 3, 8)
        scratch = [
            pltpu.SMEM((32,), jnp.int32), V((32, QW), BF16), V((2, 3, 2, QW), BF16), V((2, 3, 4, QW), BF16), V((3, 8, 2, QW), BF16), V((3, 8, 4, QW), BF16),
            V((144, 8, LAT + LANES), BF16), V((144,) + tile, BF16),
            V((BASE + 2, 64) + qtile, BF16), V((288,) + tile, BF16), V((2, 3, SPLIT, 1, LANES), F32), V((3, LANES, LANES), F32),
            V((3, NI, 3, 4) + tile, BF16), V((2, 3, 3, SPLIT, 1, LANES), F32), V((3, 4, NI) + tile, BF16), V((2, 3, SPLIT, 1, LANES), F32),
            V((3, 3, NI) + tile, BF16), V((2, 3, 3, SPLIT, 1, LANES), F32),
            V((3, 8, TILE[0], LAT), BF16), V((3, 8, TILE[1], LAT), BF16), V(line + (1, LANES), F32),
            V((3, 8, TILE[0], LAT), BF16), V((3, 8, TILE[1], LAT), BF16), V(line + (1, LANES), F32),
            V((2, 2, 3) + tile, F32),
            dma, dma, dma, dma, dma((2,)), dma((2,)), dma((2,)), dma((NI,)), dma((2,)), dma((NI,)), dma((NI,)),
            dma, dma((2,)), dma((2,)), dma((2,)), dma, dma((2,)), dma((2,)), dma((2,)), dma((2,)), dma((2,)), dma, dma((2,)),
        ]
        o = pl.pallas_call(
            _kernel,
            out_shape=V((32, LAT), BF16),
            in_specs=[anyspace] * 3,
            out_specs=pl.BlockSpec(memory_space=V),
            scratch_shapes=scratch,
            compiler_params=pltpu.CompilerParams(collective_id=0, has_side_effects=True,
                                                 vmem_limit_bytes=50 * 2 ** 20),
        )(*[pltpu.with_memory_space_constraint(v, pltpu.HBM) for v in (lens, q.reshape(32, QW), cache.reshape(32, 32, 8, QW))])
        return o.reshape(32, 1, LAT)

    return jax.shard_map(local, mesh=mesh,
                         in_specs=(P('dp', 'dcp', None), P('dp', None, 'dcp', None, None), P('dp')),
                         out_specs=P('dp', 'dcp', None), check_vma=False)
```

```python
import functools
import math

import jax
import jax.numpy as jnp
from jax import lax
from jax.experimental import pallas as pl
from jax.experimental.pallas import tpu as pltpu
from jax.sharding import PartitionSpec as P

ROPE = 64
QK_DIM = 192
SCALE2 = QK_DIM ** -0.5 * math.log2(math.e)
NEG = -3.0e38
MESH = pl.DeviceIdType.MESH
F32 = jnp.float32
BF16 = jnp.bfloat16

STRIDE = (2, 8, 32)
ORDERS = ((0, 1, 2), (1, 2, 0), (2, 0, 1))
BASE = 15
COUNT = (6, 6, 5)
NI = 6
SPLIT = 4
TILE = (SPLIT, NI - SPLIT)
ORDER, RELAYED = (0, 5, 4, 1, 2, 3), (5, 4)


LAT, QW, LANES = 512, 576, 128
KS, DIRS, RING, RING_OFFS, LINE_OFFS = range(3), range(2), range(4), range(1, 4), range(1, 8)


def _perm(rows, cols, f):
    r = lax.broadcasted_iota(jnp.int32, (rows, cols), 0)
    c = lax.broadcasted_iota(jnp.int32, (rows, cols), 1)
    return f(r, c).astype(F32).astype(BF16)


def _merge_weights(lses):
    top = functools.reduce(jnp.maximum, lses)
    ws = [jnp.exp2(v - top) for v in lses]
    tot = functools.reduce(jnp.add, ws)
    inv = 1.0 / tot
    return [w * inv for w in ws], top + jnp.log2(tot)


def _kernel(lens_h, q_h, c_h, o_ref,
            lens, q_in, s1a, s1b, b1a, b1b, q_even, q_odd, cbuf, obuf, lrow, wcol, r1d, r1l, r1m, lse1,
            r2d, r2l, s3a, s3b, s3l, r3a, r3b, r3l, fin,
            sem_l, sem_q, c_s, c_r, s1_s, s1_r, s2_s, s2_r, s3_s, s3_r, sf_r,
            r1_s, r1_r, r1l_s, r1l_r, r2_s, r2_r, r2l_s, r2l_r, r3_s, r3_r, r3l_s, r3l_r):
    d = lax.axis_index('dcp')
    core = d % 2
    co = ((d // 2) % 4, (d // 8) % 4, d // 32)
    partner = {'dcp': d + 1 - 2 * core}

    nxt = (1, 2, 0)
    ac = [co[n] + core * (co[nxt[n]] - co[n]) for n in KS]
    stride = [STRIDE[n] + core * (STRIDE[nxt[n]] - STRIDE[n]) for n in KS]

    def ring(axis, off):
        return {'dcp': d + ((ac[axis] + off) % 4 - ac[axis]) * stride[axis]}

    def line(axis, j):
        return {'dcp': d + (j // 2 - ac[axis]) * stride[axis] + (j % 2 - core)}

    def send(src, dst, ss, rs, dev):
        pltpu.make_async_remote_copy(src_ref=src, dst_ref=dst, send_sem=ss, recv_sem=rs,
                                     device_id=dev, device_id_type=MESH).start()

    def wait(ref, sem):
        pltpu.make_async_copy(ref, ref, sem).wait()

    def ks_of(i):
        return KS if i < NI - 1 else DIRS

    def only(i, f):
        if i < NI - 1:
            f()
        else:
            pl.when(core == 1)(f)

    def by_core(f):
        for c in DIRS:
            pl.when(core == c)(functools.partial(f, c))

    bar = pltpu.get_barrier_semaphore()
    pl.semaphore_signal(bar, inc=1, device_id=partner, device_id_type=MESH)
    for off in (2, 1, 3):
        for a in KS:
            for c2 in DIRS:
                peer = d + ((co[a] + off) % 4 - co[a]) * STRIDE[a] + c2 - core
                pl.semaphore_signal(bar, inc=1, device_id={'dcp': peer}, device_id_type=MESH)
    load_q = pltpu.make_async_copy(q_h, q_in, sem_q)
    load_q.start()
    load_l = pltpu.make_async_copy(lens_h, lens, sem_l)
    load_l.start()

    def cache_rows(i, half):
        n = len(ks_of(i))
        return c_h.at[pl.ds(BASE * half + 3 * i, n)], cbuf.at[pl.ds(3 * i, n), pl.ds(32 * core, 32)]

    def load_rows(i, half):
        src, dst = cache_rows(i, half)
        pltpu.make_async_copy(src, dst, c_r).start()

    for i in range(NI - 1):
        load_rows(i, core)
    pl.when(core == 1)(lambda: load_rows(NI - 1, 1))

    lrow[...] = jnp.zeros_like(lrow)
    fin[...] = jnp.zeros_like(fin)

    @pl.when(core == 0)
    def _():
        for k in DIRS:
            obuf[pl.ds((k * NI + NI - 1) * 16, 16)] = jnp.zeros((16, 8, LAT), BF16)
            r1d[k, NI - 1] = jnp.zeros((3, 4, 8, LAT), BF16)
    load_l.wait()

    def sel(r, c):
        s = 3 * (r % 8) + (r // 8) % 3
        return (c == BASE * (r // 24) + s) & (s < BASE + 2 * (r // 24))

    load_q.wait()
    qp = jnp.dot(_perm(48, 32, sel), q_in[...], preferred_element_type=F32)
    for c in DIRS:
        for k in KS:
            r = 8 * (3 * c + k)
            s1a[c, k] = qp[r:r + 2].astype(BF16)
            s1b[c, k] = qp[r + 2:r + 6].astype(BF16)
    pl.semaphore_wait(bar, 19)

    def place(k):
        return ac[ORDERS[k][0]] * 2 + core

    for part, (src, dst) in enumerate(((s1a, b1a), (s1b, b1b))):
        for k in KS:
            n = ORDERS[k][0]
            j0 = place(k)
            oc = co[n] + co[nxt[n]] - ac[n]
            ost = STRIDE[n] + STRIDE[nxt[n]] - stride[n]
            for off in (2, 1, 3):
                send(src.at[core, k], dst.at[k, j0], s1_s.at[part], s1_r.at[part], ring(n, off))
            for off in (2, 1, 3, 0):
                peer = {'dcp': d + ((oc + off) % 4 - oc) * ost + 1 - 2 * core}
                send(src.at[1 - core, k], dst.at[k, oc * 2 + core], s1_s.at[part], s1_r.at[part], peer)
            dst[k, j0] = src[core, k]

    def push_rows(i, half):
        src, dst = cache_rows(i, half)
        send(src, dst, c_s, c_r, partner)

    for i in range(NI - 1):
        push_rows(i, 1 - core)
    pl.when(core == 0)(lambda: push_rows(NI - 1, 1))

    def q_of(i):
        return q_odd if i % 2 else q_even

    def q_slot(k, i):
        return (k * 3 + i // 2) * 16

    def slot(k, i):
        return (k * NI + i) * 16

    def blk(k, i, off):
        _, a2, a3 = ORDERS[k]
        return q_of(i).at[q_slot(k, i) + ac[a3] * 4 + (ac[a2] - off) % 4]

    def copy3(k, i, off):
        b = blk(k, i, off)
        a3 = ORDERS[k][2]
        for o in (1, 3) if i in RELAYED else (2, 1, 3):
            onward = i in RELAYED and off // 2 == o // 2
            send(b, b, s3_s.at[i % 2], sf_r.at[i - NI + 2] if onward else s3_r.at[i], ring(a3, o))

    def stage2(k, i):
        b = blk(k, i, 0)
        for off in (2, 1, 3):
            send(b, b, s2_s.at[i % 2], s2_r.at[i], ring(ORDERS[k][1], off))
        copy3(k, i, 0)

    def rows2(i):
        for k in ks_of(i):
            stage2(k, i)

    def turn(buf, part, first, n):
        wait(buf.at[:, pl.ds(0, 7)], s1_r.at[part])
        tr = _perm(8 * n, 8 * n, lambda r, c: (r // 8 == c % n) & (r % 8 == c // n))
        ins = [jnp.concatenate([buf[k, j].astype(F32) for j in range(8)], axis=0).astype(BF16) for k in KS]
        outs = [jnp.dot(tr, v, preferred_element_type=F32) for v in ins]
        for k in KS:
            _, a2, a3 = ORDERS[k]
            for i in range(first, min(first + n, COUNT[k])):
                r = 8 * (i - first)
                y = outs[k][r:r + 8, :LAT if i % 2 else QW]
                if i % 2 == 0:
                    y = jnp.concatenate([y, outs[k][r + 8:r + 16, LAT:]], axis=1)
                q_of(i)[q_slot(k, i) + ac[a3] * 4 + ac[a2]] = y.astype(BF16)

    turn(b1a, 0, 0, 2)
    for i in range(2):
        rows2(i)
    turn(b1b, 1, 2, 4)
    for i in ORDER:
        if i > 1:
            only(i, functools.partial(rows2, i))

    def stage3(i):
        n = len(ks_of(i))
        wait(q_of(i).at[pl.ds(0, 3 * n)], s2_r.at[i])
        for off in (1, 3, 2):
            for k in ks_of(i):
                copy3(k, i, off)

    def forward(i):
        wait(q_of(i).at[pl.ds(0, 4 * len(ks_of(i)))], sf_r.at[i - NI + 2])
        for off in RING:
            for k in ks_of(i):
                _, a2, a3 = ORDERS[k]
                o = 1 if off < 2 else 3
                b = q_of(i).at[q_slot(k, i) + ((ac[a3] - o) % 4) * 4 + (ac[a2] - off) % 4]
                send(b, b, s3_s.at[i % 2], s3_r.at[i], ring(a3, o))

    def arrive(i):
        n = len(ks_of(i))
        if i == 0:
            by_core(lambda c: wait(cbuf.at[pl.ds(0, BASE + 2 * c)], c_r))
        wait(q_of(i).at[pl.ds(0, (8 if i in RELAYED else 12) * n)], s3_r.at[i])

    for i in ORDER:
        only(i, functools.partial(stage3, i))

    chip8 = (d // 2) * 16

    j = lax.broadcasted_iota(jnp.int32, (LAT, LANES), 0)
    pos = (j & 7) + ((j >> 3) & 31) * 1024 + (j >> 8) * 8

    def cache_of(k, i):
        return cbuf[3 * i + k].reshape(LAT, QW)

    def scores(k, i):
        cs = cache_of(k, i)
        n = pl.ds(q_slot(k, i), 16)
        lat = q_of(i)[n, :, :LAT].reshape(LANES, LAT)
        rope = q_even[n, :, LAT:].reshape(LANES, LANES)
        rope = rope[:, ROPE:] if i % 2 else rope[:, :ROPE]
        dims = (((1,), (1,)), ((), ()))
        st = lax.dot_general(cs[:, :LAT], lat, dims, preferred_element_type=F32)
        return (st + lax.dot_general(cs[:, LAT:], rope, dims, preferred_element_type=F32)) * SCALE2

    def softmax(st, k, i):
        ok = pos < lens[BASE * core + 3 * i + k] - chip8
        st = jnp.where(ok, st, NEG)
        m = jnp.max(st, axis=0, keepdims=True)
        has = m > NEG
        p = jnp.exp2(st - jnp.where(has, m, 0.0))
        ls = jnp.where(has, jnp.sum(p, axis=0, keepdims=True), 1.0)
        w = wave(i)
        lrow[w, k, i - w * SPLIT] = jnp.where(has, m + jnp.log2(ls), NEG)
        return (p * (1.0 / ls)).astype(BF16)

    def attend(batch):
        sts = [scores(k, i) for k, i in batch]
        ps = [softmax(st, k, i) for st, (k, i) in zip(sts, batch)]
        outs = [lax.dot_general(p, cache_of(k, i)[:, :LAT], (((0,), (0,)), ((), ())), preferred_element_type=F32)
                for p, (k, i) in zip(ps, batch)]
        for o, (k, i) in zip(outs, batch):
            obuf[pl.ds(slot(k, i), 16)] = o.astype(BF16).reshape(16, 8, LAT)

    def wave(i):
        return 0 if i < SPLIT else 1

    def send1(batch):
        for o, (k, i) in [(o, x) for o in (2, 1, 3) for x in batch]:
            a3 = ORDERS[k][2]
            b = obuf.at[pl.ds(slot(k, i) + ((ac[a3] + o) % 4) * 4, 4)]
            send(b, r1d.at[k, i, o - 1], r1_s, r1_r.at[wave(i)], ring(a3, o))

    def members(w, k):
        return range(SPLIT) if w == 0 else range(SPLIT, COUNT[k])

    def count(w):
        return sum(len(members(w, k)) for k in KS)

    def send1_lse(w):
        for k in KS:
            for o in RING_OFFS:
                n = pl.ds(0, TILE[w])
                send(lrow.at[w, k, n], r1l.at[w, k, o - 1, n], r1l_s.at[w], r1l_r.at[w], ring(ORDERS[k][2], o))

    for i in range(NI - 2):
        batch = [(k, i) for k in KS]
        with jax.named_scope(f"arrive{i}"):
            arrive(i)
        with jax.named_scope(f"attend{i}"):
            attend(batch)
        with jax.named_scope(f"rest{i}"):
            if i == 0:
                for x in RELAYED:
                    only(x, functools.partial(forward, x))
            if i == SPLIT - 1:
                send1_lse(0)
            send1(batch)


    @by_core
    def _(c):
        last = range(NI - 2, NI - 1 + c)
        for i in last:
            arrive(i)
        batch = [(k, i) for i in last for k in ks_of(i)]
        attend(batch)
        send1_lse(1)
        send1(batch)


    def columns(ws, k, row, n):
        wcol[k, :, :32] = jnp.concatenate(ws, axis=0).T
        t = wcol[k, pl.ds(row, n), :32]
        return lambda x, i: t[:, 8 * x + i:8 * x + i + 1]

    def weighted(cols, i, parts):
        return functools.reduce(jnp.add, [p.astype(F32) * cols(x, i) for x, p in enumerate(parts)])

    def tile_of(w, ref):
        return jnp.concatenate([ref[i] for i in range(TILE[w])] + [jnp.zeros((8 - TILE[w], LANES), F32)], axis=0)

    def merge1(w):
        cols = []
        n = pl.ds(0, TILE[w])
        wait(r1l.at[w, :, :, n], r1l_r.at[w])
        for k in KS:
            ws, l1 = _merge_weights([tile_of(w, r) for r in [lrow.at[w, k]] + [r1l.at[w, k, x] for x in KS]])
            for i in range(TILE[w]):
                lse1[w, k, i] = l1[i:i + 1]
            cols.append(columns(ws, k, ac[ORDERS[k][2]] * 32, 32))
        for k in KS:
            for o in RING_OFFS:
                send(lse1.at[w, k, n], r2l.at[w, k, o - 1, n], r2l_s.at[w], r2l_r.at[w], ring(ORDERS[k][1], o))
        if w == 0:
            wait(obuf.at[pl.ds(0, 12 * count(w))], r1_r.at[w])
        else:
            by_core(lambda c: wait(obuf.at[pl.ds(0, 12 * (count(1) - 2 + 2 * c))], r1_r.at[w]))
        for k in KS:
            _, a2, a3 = ORDERS[k]
            its = members(w, k)
            for i in its:
                own = obuf[pl.ds(slot(k, i) + ac[a3] * 4, 4)]
                parts = [v.reshape(32, LAT) for v in [own] + [r1d[k, i, x] for x in KS]]
                y = weighted(cols[k], i - its[0], parts).astype(BF16).reshape(4, 8, LAT)
                for p in RING:
                    r1m[k, p, i] = y[p]
            for o in (2, 1, 3):
                sl = pl.ds(its[0], len(its))
                send(r1m.at[k, (ac[a2] + o) % 4, sl], r2d.at[k, o - 1, sl], r2_s, r2_r.at[w], ring(a2, o))

    def merge2(w):
        cols = []
        wait(r2l.at[w, :, :, pl.ds(0, TILE[w])], r2l_r.at[w])
        for k in KS:
            _, a2, a3 = ORDERS[k]
            ws, l2 = _merge_weights([tile_of(w, r) for r in [lse1.at[w, k]] + [r2l.at[w, k, x] for x in KS]])
            g = ac[a3] * 4 + ac[a2]
            lt = pltpu.roll(l2, ((16 - g) % 16) * 8, 1)
            s3l[w, k] = jnp.concatenate([lt] * 16, axis=0).T[0:8].reshape(8, 1, LANES)
            cols.append(columns(ws, k, g * 8, 8))
        for k in KS:
            j0 = place(k)
            for off in LINE_OFFS:
                j = (j0 + off) % 8
                send(s3l.at[w, k, j], r3l.at[w, k, j0], r3l_s, r3l_r.at[w], line(ORDERS[k][0], j))
            r3l[w, k, j0] = s3l[w, k, j0]
        wait(obuf.at[pl.ds(0, 3 * count(w))], r2_r.at[w])
        tiles = []
        for k in KS:
            its = members(w, k)
            ys = [weighted(cols[k], i - its[0], [r1m[k, ac[ORDERS[k][1]], i]] + [r2d[k, x, i] for x in KS]) for i in its]
            n = len(its)
            t = TILE[w]
            pm = _perm(8 * t, 8 * n, lambda r, c: (c == (r % t) * 8 + r // t) & (r % t < n))
            tiles.append(jnp.dot(pm, jnp.concatenate(ys, axis=0).astype(BF16), preferred_element_type=F32))
        for k in KS:
            t, s3, r3 = TILE[w], (s3a, s3b)[w], (r3a, r3b)[w]
            j0 = place(k)
            for j in range(8):
                s3[k, j] = tiles[k][t * j:t * j + t].astype(BF16)
            for off in (3, 4, 5, 2, 6, 1, 7):
                j = (j0 + off) % 8
                send(s3.at[k, j], r3.at[k, j0], r3_s.at[w], r3_r.at[w], line(ORDERS[k][0], j))
            r3[k, j0] = s3[k, j0]

    def merge3(w):
        cols = []
        wait(r3l.at[w, :, pl.ds(0, 7)], r3l_r.at[w])
        for k in KS:
            ls = [r3l[w, k, j] for j in range(8)]
            ws = [None] * 8
            for h in DIRS:
                ws[h::2], _ = _merge_weights(ls[h::2])
            cols.append(jnp.concatenate(ws, axis=0).T[0:8])
        t, r3 = TILE[w], (r3a, r3b)[w]
        wait(r3.at[:, pl.ds(0, 7)], r3_r.at[w])
        for k in KS:
            for h in DIRS:
                ts = [r3[k, j].astype(F32) * cols[k][:t, j:j + 1] for j in range(h, 8, 2)]
                fin[w, h, k, :t] = functools.reduce(jnp.add, ts)

    merge1(0)
    merge1(1)
    merge2(0)
    wait(b1a.at[:, pl.ds(0, 7)], s1_s.at[0])
    wait(b1b.at[:, pl.ds(0, 7)], s1_s.at[1])

    @by_core
    def _(c):
        wait(cbuf.at[pl.ds(0, BASE + 2 * (1 - c)), pl.ds(0, 32)], c_s)
        for par in DIRS:
            its = [i for i in range(NI - 1 + c) for _ in ks_of(i) if i % 2 == par]
            wait(q_of(par).at[pl.ds(0, 3 * len(its))], s2_s.at[par])
            wait(q_of(par).at[pl.ds(0, 12 * len(its))], s3_s.at[par])

    merge2(1)
    merge3(0)
    by_core(lambda c: wait(obuf.at[pl.ds(0, 12 * (BASE + 2 * c))], r1_s))
    for w in DIRS:
        n = pl.ds(0, TILE[w])
        wait(r1l.at[w, :, :, n], r1l_s.at[w])
        wait(r2l.at[w, :, :, n], r2l_s.at[w])
    wait(obuf.at[pl.ds(0, 51)], r2_s)
    merge3(1)
    flat = fin[...].reshape(96, LAT).astype(BF16)

    def pick(r, c):
        w, h, k, i = c // 48, (c // 24) % 2, (c // 8) % 3, c % 8
        s = 3 * (i + w * SPLIT) + k
        return (r == BASE * h + s) & (s < BASE + 2 * h) & (i < SPLIT)

    o_ref[...] = jnp.dot(_perm(32, 96, pick), flat, preferred_element_type=F32).astype(BF16)

    wait(r3a.at[:, pl.ds(0, 7)], r3_s.at[0])
    wait(r3b.at[:, pl.ds(0, 7)], r3_s.at[1])
    wait(r3l.at[:, :, pl.ds(0, 7)], r3l_s)


def solution(mesh):
    def local(q, cache, lens):
        dma = pltpu.SemaphoreType.DMA
        V = pltpu.VMEM
        anyspace = pl.BlockSpec(memory_space=pl.ANY)
        tile, qtile = (8, LAT), (8, QW)
        line = (2, 3, 8)
        scratch = [
            pltpu.SMEM((32,), jnp.int32), V((32, QW), BF16), V((2, 3, 2, QW), BF16), V((2, 3, 4, QW), BF16), V((3, 8, 2, QW), BF16), V((3, 8, 4, QW), BF16),
            V((144, 8, LAT + LANES), BF16), V((144,) + tile, BF16),
            V((BASE + 2, 64) + qtile, BF16), V((288,) + tile, BF16), V((2, 3, SPLIT, 1, LANES), F32), V((3, LANES, LANES), F32),
            V((3, NI, 3, 4) + tile, BF16), V((2, 3, 3, SPLIT, 1, LANES), F32), V((3, 4, NI) + tile, BF16), V((2, 3, SPLIT, 1, LANES), F32),
            V((3, 3, NI) + tile, BF16), V((2, 3, 3, SPLIT, 1, LANES), F32),
            V((3, 8, TILE[0], LAT), BF16), V((3, 8, TILE[1], LAT), BF16), V(line + (1, LANES), F32),
            V((3, 8, TILE[0], LAT), BF16), V((3, 8, TILE[1], LAT), BF16), V(line + (1, LANES), F32),
            V((2, 2, 3) + tile, F32),
            dma, dma, dma, dma, dma((2,)), dma((2,)), dma((2,)), dma((NI,)), dma((2,)), dma((NI,)), dma((2,)),
            dma, dma((2,)), dma((2,)), dma((2,)), dma, dma((2,)), dma((2,)), dma((2,)), dma((2,)), dma((2,)), dma, dma((2,)),
        ]
        o = pl.pallas_call(
            _kernel,
            out_shape=V((32, LAT), BF16),
            in_specs=[anyspace] * 3,
            out_specs=pl.BlockSpec(memory_space=V),
            scratch_shapes=scratch,
            compiler_params=pltpu.CompilerParams(collective_id=0, has_side_effects=True,
                                                 vmem_limit_bytes=50 * 2 ** 20),
        )(*[pltpu.with_memory_space_constraint(v, pltpu.HBM) for v in (lens, q.reshape(32, QW), cache.reshape(32, 32, 8, QW))])
        return o.reshape(32, 1, LAT)

    return jax.shard_map(local, mesh=mesh,
                         in_specs=(P('dp', 'dcp', None), P('dp', None, 'dcp', None, None), P('dp')),
                         out_specs=P('dp', 'dcp', None), check_vma=False)
```

```python
import functools
import math

import jax
import jax.numpy as jnp
from jax import lax
from jax.experimental import pallas as pl
from jax.experimental.pallas import tpu as pltpu
from jax.sharding import PartitionSpec as P

ROPE = 64
QK_DIM = 192
SCALE2 = QK_DIM ** -0.5 * math.log2(math.e)
NEG = -3.0e38
MESH = pl.DeviceIdType.MESH
F32 = jnp.float32
BF16 = jnp.bfloat16

STRIDE = (2, 8, 32)
ORDERS = ((0, 1, 2), (1, 2, 0), (2, 0, 1))
BASE = 15
COUNT = (6, 6, 5)
NI = 6
SPLIT = 4
TILE = (SPLIT, NI - SPLIT)
ORDER, RELAYED = (0, 5, 4, 1, 2, 3), (5, 4)


LAT, QW, LANES = 512, 576, 128
KS, DIRS, RING, RING_OFFS, LINE_OFFS = range(3), range(2), range(4), range(1, 4), range(1, 8)


def _perm(rows, cols, f):
    r = lax.broadcasted_iota(jnp.int32, (rows, cols), 0)
    c = lax.broadcasted_iota(jnp.int32, (rows, cols), 1)
    return f(r, c).astype(F32).astype(BF16)


def _merge_weights(lses):
    top = functools.reduce(jnp.maximum, lses)
    ws = [jnp.exp2(v - top) for v in lses]
    tot = functools.reduce(jnp.add, ws)
    inv = 1.0 / tot
    return [w * inv for w in ws], top + jnp.log2(tot)


def _kernel(lens_h, q_h, c_h, o_ref,
            lens, q_in, s1a, s1b, b1a, b1b, q_even, q_odd, cbuf, obuf, lrow, wcol, r1d, r1l, r1m, lse1,
            r2d, r2l, s3a, s3b, s3l, r3a, r3b, r3l, fin,
            sem_l, sem_q, c_s, c_r, s1_s, s1_r, s2_s, s2_r, s3_s, s3_r, sf_r,
            r1_s, r1_r, r1l_s, r1l_r, r2_s, r2_r, r2l_s, r2l_r, r3_s, r3_r, r3l_s, r3l_r):
    d = lax.axis_index('dcp')
    core = d % 2
    co = ((d // 2) % 4, (d // 8) % 4, d // 32)
    partner = {'dcp': d + 1 - 2 * core}

    nxt = (1, 2, 0)
    ac = [co[n] + core * (co[nxt[n]] - co[n]) for n in KS]
    stride = [STRIDE[n] + core * (STRIDE[nxt[n]] - STRIDE[n]) for n in KS]

    def ring(axis, off):
        return {'dcp': d + ((ac[axis] + off) % 4 - ac[axis]) * stride[axis]}

    def line(axis, j):
        return {'dcp': d + (j // 2 - ac[axis]) * stride[axis] + (j % 2 - core)}

    def send(src, dst, ss, rs, dev):
        pltpu.make_async_remote_copy(src_ref=src, dst_ref=dst, send_sem=ss, recv_sem=rs,
                                     device_id=dev, device_id_type=MESH).start()

    def wait(ref, sem):
        pltpu.make_async_copy(ref, ref, sem).wait()

    def ks_of(i):
        return KS if i < NI - 1 else DIRS

    def only(i, f):
        if i < NI - 1:
            f()
        else:
            pl.when(core == 1)(f)

    def by_core(f):
        for c in DIRS:
            pl.when(core == c)(functools.partial(f, c))

    bar = pltpu.get_barrier_semaphore()
    pl.semaphore_signal(bar, inc=1, device_id=partner, device_id_type=MESH)
    for off in (2, 1, 3):
        for a in KS:
            for c2 in DIRS:
                peer = d + ((co[a] + off) % 4 - co[a]) * STRIDE[a] + c2 - core
                pl.semaphore_signal(bar, inc=1, device_id={'dcp': peer}, device_id_type=MESH)
    load_q = pltpu.make_async_copy(q_h, q_in, sem_q)
    load_q.start()
    load_l = pltpu.make_async_copy(lens_h, lens, sem_l)
    load_l.start()

    def cache_rows(i, half):
        n = len(ks_of(i))
        return c_h.at[pl.ds(BASE * half + 3 * i, n)], cbuf.at[pl.ds(3 * i, n), pl.ds(32 * core, 32)]

    def load_rows(i, half):
        src, dst = cache_rows(i, half)
        pltpu.make_async_copy(src, dst, c_r).start()

    for i in range(NI - 1):
        load_rows(i, core)
    pl.when(core == 1)(lambda: load_rows(NI - 1, 1))

    lrow[...] = jnp.zeros_like(lrow)
    fin[...] = jnp.zeros_like(fin)

    @pl.when(core == 0)
    def _():
        for k in DIRS:
            obuf[pl.ds((k * NI + NI - 1) * 16, 16)] = jnp.zeros((16, 8, LAT), BF16)
            r1d[k, NI - 1] = jnp.zeros((3, 4, 8, LAT), BF16)
    load_l.wait()

    def sel(r, c):
        s = 3 * (r % 8) + (r // 8) % 3
        return (c == BASE * (r // 24) + s) & (s < BASE + 2 * (r // 24))

    load_q.wait()
    qp = jnp.dot(_perm(48, 32, sel), q_in[...], preferred_element_type=F32)
    for c in DIRS:
        for k in KS:
            r = 8 * (3 * c + k)
            s1a[c, k] = qp[r:r + 2].astype(BF16)
            s1b[c, k] = qp[r + 2:r + 6].astype(BF16)
    pl.semaphore_wait(bar, 19)

    def place(k):
        return ac[ORDERS[k][0]] * 2 + core

    for part, (src, dst) in enumerate(((s1a, b1a), (s1b, b1b))):
        for k in KS:
            n = ORDERS[k][0]
            j0 = place(k)
            oc = co[n] + co[nxt[n]] - ac[n]
            ost = STRIDE[n] + STRIDE[nxt[n]] - stride[n]
            for off in (2, 1, 3, 0):
                peer = {'dcp': d + ((oc + off) % 4 - oc) * ost + 1 - 2 * core}
                send(src.at[1 - core, k], dst.at[k, oc * 2 + core], s1_s.at[part], s1_r.at[part], peer)
            for off in (2, 1, 3):
                send(src.at[core, k], dst.at[k, j0], s1_s.at[part], s1_r.at[part], ring(n, off))
            dst[k, j0] = src[core, k]

    def push_rows(i, half):
        src, dst = cache_rows(i, half)
        send(src, dst, c_s, c_r, partner)

    for i in range(NI - 1):
        push_rows(i, 1 - core)
    pl.when(core == 0)(lambda: push_rows(NI - 1, 1))

    def q_of(i):
        return q_odd if i % 2 else q_even

    def q_slot(k, i):
        return (k * 3 + i // 2) * 16

    def slot(k, i):
        return (k * NI + i) * 16

    def blk(k, i, off):
        _, a2, a3 = ORDERS[k]
        return q_of(i).at[q_slot(k, i) + ac[a3] * 4 + (ac[a2] - off) % 4]

    def copy3(k, i, off):
        b = blk(k, i, off)
        a3 = ORDERS[k][2]
        for o in (1, 3) if i in RELAYED else (2, 1, 3):
            onward = i in RELAYED and off // 2 == o // 2
            send(b, b, s3_s.at[i % 2], sf_r.at[i - NI + 2] if onward else s3_r.at[i], ring(a3, o))

    def stage2(k, i):
        b = blk(k, i, 0)
        for off in (2, 1, 3):
            send(b, b, s2_s.at[i % 2], s2_r.at[i], ring(ORDERS[k][1], off))
        copy3(k, i, 0)

    def rows2(i):
        for k in ks_of(i):
            stage2(k, i)

    def turn(buf, part, first, n):
        tr = _perm(8 * n, 8 * n, lambda r, c: (r // 8 == c % n) & (r % 8 == c // n))
        wait(buf.at[:, pl.ds(0, 7)], s1_r.at[part])
        ins = [jnp.concatenate([buf[k, j].astype(F32) for j in range(8)], axis=0).astype(BF16) for k in KS]
        outs = [jnp.dot(tr, v, preferred_element_type=F32) for v in ins]
        for k in KS:
            _, a2, a3 = ORDERS[k]
            for i in range(first, min(first + n, COUNT[k])):
                r = 8 * (i - first)
                y = outs[k][r:r + 8, :LAT if i % 2 else QW]
                if i % 2 == 0:
                    y = jnp.concatenate([y, outs[k][r + 8:r + 16, LAT:]], axis=1)
                q_of(i)[q_slot(k, i) + ac[a3] * 4 + ac[a2]] = y.astype(BF16)

    turn(b1a, 0, 0, 2)
    for i in range(2):
        rows2(i)
    turn(b1b, 1, 2, 4)
    for i in ORDER:
        if i > 1:
            only(i, functools.partial(rows2, i))

    def stage3(i):
        n = len(ks_of(i))
        wait(q_of(i).at[pl.ds(0, 3 * n)], s2_r.at[i])
        for off in (1, 3, 2):
            for k in ks_of(i):
                copy3(k, i, off)

    def forward(i):
        wait(q_of(i).at[pl.ds(0, 4 * len(ks_of(i)))], sf_r.at[i - NI + 2])
        for off in RING:
            for k in ks_of(i):
                _, a2, a3 = ORDERS[k]
                o = 1 if off < 2 else 3
                b = q_of(i).at[q_slot(k, i) + ((ac[a3] - o) % 4) * 4 + (ac[a2] - off) % 4]
                send(b, b, s3_s.at[i % 2], s3_r.at[i], ring(a3, o))

    def arrive(i):
        n = len(ks_of(i))
        if i == 0:
            by_core(lambda c: wait(cbuf.at[pl.ds(0, BASE + 2 * c)], c_r))
        wait(q_of(i).at[pl.ds(0, (8 if i in RELAYED else 12) * n)], s3_r.at[i])

    for i in ORDER:
        only(i, functools.partial(stage3, i))

    chip8 = (d // 2) * 16

    j = lax.broadcasted_iota(jnp.int32, (LAT, LANES), 0)
    pos = (j & 7) + ((j >> 3) & 31) * 1024 + (j >> 8) * 8

    def cache_of(k, i):
        return cbuf[3 * i + k].reshape(LAT, QW)

    def scores(k, i):
        cs = cache_of(k, i)
        n = pl.ds(q_slot(k, i), 16)
        lat = q_of(i)[n, :, :LAT].reshape(LANES, LAT)
        rope = q_even[n, :, LAT:].reshape(LANES, LANES)
        rope = rope[:, ROPE:] if i % 2 else rope[:, :ROPE]
        dims = (((1,), (1,)), ((), ()))
        st = lax.dot_general(cs[:, :LAT], lat, dims, preferred_element_type=F32)
        return (st + lax.dot_general(cs[:, LAT:], rope, dims, preferred_element_type=F32)) * SCALE2

    def softmax(st, k, i):
        ok = pos < lens[BASE * core + 3 * i + k] - chip8
        st = jnp.where(ok, st, NEG)
        m = jnp.max(st, axis=0, keepdims=True)
        has = m > NEG
        p = jnp.exp2(st - jnp.where(has, m, 0.0))
        ls = jnp.where(has, jnp.sum(p, axis=0, keepdims=True), 1.0)
        w = wave(i)
        lrow[w, k, i - w * SPLIT] = jnp.where(has, m + jnp.log2(ls), NEG)
        return (p * (1.0 / ls)).astype(BF16)

    def attend(batch):
        sts = [scores(k, i) for k, i in batch]
        ps = [softmax(st, k, i) for st, (k, i) in zip(sts, batch)]
        outs = [lax.dot_general(p, cache_of(k, i)[:, :LAT], (((0,), (0,)), ((), ())), preferred_element_type=F32)
                for p, (k, i) in zip(ps, batch)]
        for o, (k, i) in zip(outs, batch):
            obuf[pl.ds(slot(k, i), 16)] = o.astype(BF16).reshape(16, 8, LAT)

    def wave(i):
        return 0 if i < SPLIT else 1

    def send1(batch):
        for o, (k, i) in [(o, x) for o in (2, 1, 3) for x in batch]:
            a3 = ORDERS[k][2]
            b = obuf.at[pl.ds(slot(k, i) + ((ac[a3] + o) % 4) * 4, 4)]
            send(b, r1d.at[k, i, o - 1], r1_s, r1_r.at[wave(i)], ring(a3, o))

    def members(w, k):
        return range(SPLIT) if w == 0 else range(SPLIT, COUNT[k])

    def count(w):
        return sum(len(members(w, k)) for k in KS)

    def send1_lse(w):
        for k in KS:
            for o in RING_OFFS:
                n = pl.ds(0, TILE[w])
                send(lrow.at[w, k, n], r1l.at[w, k, o - 1, n], r1l_s.at[w], r1l_r.at[w], ring(ORDERS[k][2], o))

    for i in range(NI - 2):
        batch = [(k, i) for k in KS]
        with jax.named_scope(f"arrive{i}"):
            arrive(i)
        with jax.named_scope(f"attend{i}"):
            attend(batch)
        with jax.named_scope(f"rest{i}"):
            if i == 0:
                for x in RELAYED:
                    only(x, functools.partial(forward, x))
            if i == SPLIT - 1:
                send1_lse(0)
            send1(batch)


    @by_core
    def _(c):
        last = range(NI - 2, NI - 1 + c)
        for i in last:
            arrive(i)
        batch = [(k, i) for i in last for k in ks_of(i)]
        attend(batch)
        send1_lse(1)
        send1(batch)


    def columns(ws, k, row, n):
        wcol[k, :, :32] = jnp.concatenate(ws, axis=0).T
        t = wcol[k, pl.ds(row, n), :32]
        return lambda x, i: t[:, 8 * x + i:8 * x + i + 1]

    def weighted(cols, i, parts):
        return functools.reduce(jnp.add, [p.astype(F32) * cols(x, i) for x, p in enumerate(parts)])

    def tile_of(w, ref):
        return jnp.concatenate([ref[i] for i in range(TILE[w])] + [jnp.zeros((8 - TILE[w], LANES), F32)], axis=0)

    def merge1(w):
        cols = []
        n = pl.ds(0, TILE[w])
        wait(r1l.at[w, :, :, n], r1l_r.at[w])
        for k in KS:
            ws, l1 = _merge_weights([tile_of(w, r) for r in [lrow.at[w, k]] + [r1l.at[w, k, x] for x in KS]])
            for i in range(TILE[w]):
                lse1[w, k, i] = l1[i:i + 1]
            cols.append(columns(ws, k, ac[ORDERS[k][2]] * 32, 32))
        for k in KS:
            for o in RING_OFFS:
                send(lse1.at[w, k, n], r2l.at[w, k, o - 1, n], r2l_s.at[w], r2l_r.at[w], ring(ORDERS[k][1], o))
        if w == 0:
            wait(obuf.at[pl.ds(0, 12 * count(w))], r1_r.at[w])
        else:
            by_core(lambda c: wait(obuf.at[pl.ds(0, 12 * (count(1) - 2 + 2 * c))], r1_r.at[w]))
        for k in KS:
            _, a2, a3 = ORDERS[k]
            its = members(w, k)
            for i in its:
                own = obuf[pl.ds(slot(k, i) + ac[a3] * 4, 4)]
                parts = [v.reshape(32, LAT) for v in [own] + [r1d[k, i, x] for x in KS]]
                y = weighted(cols[k], i - its[0], parts).astype(BF16).reshape(4, 8, LAT)
                for p in RING:
                    r1m[k, p, i] = y[p]
            for o in (2, 1, 3):
                sl = pl.ds(its[0], len(its))
                send(r1m.at[k, (ac[a2] + o) % 4, sl], r2d.at[k, o - 1, sl], r2_s, r2_r.at[w], ring(a2, o))

    def merge2(w):
        cols = []
        wait(r2l.at[w, :, :, pl.ds(0, TILE[w])], r2l_r.at[w])
        for k in KS:
            _, a2, a3 = ORDERS[k]
            ws, l2 = _merge_weights([tile_of(w, r) for r in [lse1.at[w, k]] + [r2l.at[w, k, x] for x in KS]])
            g = ac[a3] * 4 + ac[a2]
            lt = pltpu.roll(l2, ((16 - g) % 16) * 8, 1)
            s3l[w, k] = jnp.concatenate([lt] * 16, axis=0).T[0:8].reshape(8, 1, LANES)
            cols.append(columns(ws, k, g * 8, 8))
        for k in KS:
            j0 = place(k)
            for off in LINE_OFFS:
                j = (j0 + off) % 8
                send(s3l.at[w, k, j], r3l.at[w, k, j0], r3l_s, r3l_r.at[w], line(ORDERS[k][0], j))
            r3l[w, k, j0] = s3l[w, k, j0]
        t = TILE[w]
        pms = {n: _perm(8 * t, 8 * n, lambda r, c: (c == (r % t) * 8 + r // t) & (r % t < n))
               for n in sorted({len(members(w, k)) for k in KS})}
        wait(obuf.at[pl.ds(0, 3 * count(w))], r2_r.at[w])
        tiles = []
        for k in KS:
            its = members(w, k)
            ys = [weighted(cols[k], i - its[0], [r1m[k, ac[ORDERS[k][1]], i]] + [r2d[k, x, i] for x in KS]) for i in its]
            n = len(its)
            tiles.append(jnp.dot(pms[n], jnp.concatenate(ys, axis=0).astype(BF16), preferred_element_type=F32))
        for k in KS:
            t, s3, r3 = TILE[w], (s3a, s3b)[w], (r3a, r3b)[w]
            j0 = place(k)
            for j in range(8):
                s3[k, j] = tiles[k][t * j:t * j + t].astype(BF16)
            for off in (3, 4, 5, 2, 6, 1, 7):
                j = (j0 + off) % 8
                send(s3.at[k, j], r3.at[k, j0], r3_s.at[w], r3_r.at[w], line(ORDERS[k][0], j))
            r3[k, j0] = s3[k, j0]

    def merge3(w):
        cols = []
        wait(r3l.at[w, :, pl.ds(0, 7)], r3l_r.at[w])
        for k in KS:
            ls = [r3l[w, k, j] for j in range(8)]
            ws = [None] * 8
            for h in DIRS:
                ws[h::2], _ = _merge_weights(ls[h::2])
            cols.append(jnp.concatenate(ws, axis=0).T[0:8])
        t, r3 = TILE[w], (r3a, r3b)[w]
        wait(r3.at[:, pl.ds(0, 7)], r3_r.at[w])
        for k in KS:
            for h in DIRS:
                ts = [r3[k, j].astype(F32) * cols[k][:t, j:j + 1] for j in range(h, 8, 2)]
                fin[w, h, k, :t] = functools.reduce(jnp.add, ts)

    merge1(0)
    merge1(1)
    merge2(0)
    wait(b1a.at[:, pl.ds(0, 7)], s1_s.at[0])
    wait(b1b.at[:, pl.ds(0, 7)], s1_s.at[1])

    @by_core
    def _(c):
        wait(cbuf.at[pl.ds(0, BASE + 2 * (1 - c)), pl.ds(0, 32)], c_s)
        for par in DIRS:
            its = [i for i in range(NI - 1 + c) for _ in ks_of(i) if i % 2 == par]
            wait(q_of(par).at[pl.ds(0, 3 * len(its))], s2_s.at[par])
            wait(q_of(par).at[pl.ds(0, 12 * len(its))], s3_s.at[par])

    merge2(1)
    merge3(0)
    by_core(lambda c: wait(obuf.at[pl.ds(0, 12 * (BASE + 2 * c))], r1_s))
    for w in DIRS:
        n = pl.ds(0, TILE[w])
        wait(r1l.at[w, :, :, n], r1l_s.at[w])
        wait(r2l.at[w, :, :, n], r2l_s.at[w])
    wait(obuf.at[pl.ds(0, 51)], r2_s)
    def pick(r, c):
        w, h, k, i = c // 48, (c // 24) % 2, (c // 8) % 3, c % 8
        s = 3 * (i + w * SPLIT) + k
        return (r == BASE * h + s) & (s < BASE + 2 * h) & (i < SPLIT)

    pm = _perm(32, 96, pick)
    merge3(1)
    flat = fin[...].reshape(96, LAT).astype(BF16)

    o_ref[...] = jnp.dot(pm, flat, preferred_element_type=F32).astype(BF16)

    wait(r3a.at[:, pl.ds(0, 7)], r3_s.at[0])
    wait(r3b.at[:, pl.ds(0, 7)], r3_s.at[1])
    wait(r3l.at[:, :, pl.ds(0, 7)], r3l_s)


def solution(mesh):
    def local(q, cache, lens):
        dma = pltpu.SemaphoreType.DMA
        V = pltpu.VMEM
        anyspace = pl.BlockSpec(memory_space=pl.ANY)
        tile, qtile = (8, LAT), (8, QW)
        line = (2, 3, 8)
        scratch = [
            pltpu.SMEM((32,), jnp.int32), V((32, QW), BF16), V((2, 3, 2, QW), BF16), V((2, 3, 4, QW), BF16), V((3, 8, 2, QW), BF16), V((3, 8, 4, QW), BF16),
            V((144, 8, LAT + LANES), BF16), V((144,) + tile, BF16),
            V((BASE + 2, 64) + qtile, BF16), V((288,) + tile, BF16), V((2, 3, SPLIT, 1, LANES), F32), V((3, LANES, LANES), F32),
            V((3, NI, 3, 4) + tile, BF16), V((2, 3, 3, SPLIT, 1, LANES), F32), V((3, 4, NI) + tile, BF16), V((2, 3, SPLIT, 1, LANES), F32),
            V((3, 3, NI) + tile, BF16), V((2, 3, 3, SPLIT, 1, LANES), F32),
            V((3, 8, TILE[0], LAT), BF16), V((3, 8, TILE[1], LAT), BF16), V(line + (1, LANES), F32),
            V((3, 8, TILE[0], LAT), BF16), V((3, 8, TILE[1], LAT), BF16), V(line + (1, LANES), F32),
            V((2, 2, 3) + tile, F32),
            dma, dma, dma, dma, dma((2,)), dma((2,)), dma((2,)), dma((NI,)), dma((2,)), dma((NI,)), dma((2,)),
            dma, dma((2,)), dma((2,)), dma((2,)), dma, dma((2,)), dma((2,)), dma((2,)), dma((2,)), dma((2,)), dma, dma((2,)),
        ]
        o = pl.pallas_call(
            _kernel,
            out_shape=V((32, LAT), BF16),
            in_specs=[anyspace] * 3,
            out_specs=pl.BlockSpec(memory_space=V),
            scratch_shapes=scratch,
            compiler_params=pltpu.CompilerParams(collective_id=0, has_side_effects=True,
                                                 vmem_limit_bytes=50 * 2 ** 20),
        )(*[pltpu.with_memory_space_constraint(v, pltpu.HBM) for v in (lens, q.reshape(32, QW), cache.reshape(32, 32, 8, QW))])
        return o.reshape(32, 1, LAT)

    return jax.shard_map(local, mesh=mesh,
                         in_specs=(P('dp', 'dcp', None), P('dp', None, 'dcp', None, None), P('dp')),
                         out_specs=P('dp', 'dcp', None), check_vma=False)
```

```python
import functools
import math

import jax
import jax.numpy as jnp
from jax import lax
from jax.experimental import pallas as pl
from jax.experimental.pallas import tpu as pltpu
from jax.sharding import PartitionSpec as P

ROPE = 64
QK_DIM = 192
SCALE2 = QK_DIM ** -0.5 * math.log2(math.e)
NEG = -3.0e38
MESH = pl.DeviceIdType.MESH
F32 = jnp.float32
BF16 = jnp.bfloat16

STRIDE = (2, 8, 32)
ORDERS = ((0, 1, 2), (1, 2, 0), (2, 0, 1))
BASE = 15
COUNT = (6, 6, 5)
NI = 6
SPLIT = 4
TILE = (SPLIT, NI - SPLIT)
ORDER, RELAYED = (0, 5, 4, 1, 2, 3), (5, 4)


LAT, QW, LANES = 512, 576, 128
KS, DIRS, RING, RING_OFFS, LINE_OFFS = range(3), range(2), range(4), range(1, 4), range(1, 8)


def _perm(rows, cols, f):
    r = lax.broadcasted_iota(jnp.int32, (rows, cols), 0)
    c = lax.broadcasted_iota(jnp.int32, (rows, cols), 1)
    return f(r, c).astype(F32).astype(BF16)


def _merge_weights(lses):
    top = functools.reduce(jnp.maximum, lses)
    ws = [jnp.exp2(v - top) for v in lses]
    tot = functools.reduce(jnp.add, ws)
    inv = 1.0 / tot
    return [w * inv for w in ws], top + jnp.log2(tot)


def _kernel(lens_h, q_h, c_h, o_ref,
            lens, q_in, s1a, s1b, b1a, b1b, q_even, q_odd, cbuf, obuf, lrow, wcol, r1d, r1l, r1m, lse1,
            r2d, r2l, s3a, s3b, s3l, r3a, r3b, r3l, fin,
            sem_l, sem_q, c_s, c_r, s1_s, s1_r, s2_s, s2_r, s3_s, s3_r, sf_r,
            r1_s, r1_r, r1l_s, r1l_r, r2_s, r2_r, r2l_s, r2l_r, r3_s, r3_r, r3l_s, r3l_r):
    d = lax.axis_index('dcp')
    core = d % 2
    co = ((d // 2) % 4, (d // 8) % 4, d // 32)
    partner = {'dcp': d + 1 - 2 * core}

    nxt = (1, 2, 0)
    ac = [co[n] + core * (co[nxt[n]] - co[n]) for n in KS]
    stride = [STRIDE[n] + core * (STRIDE[nxt[n]] - STRIDE[n]) for n in KS]

    def ring(axis, off):
        return {'dcp': d + ((ac[axis] + off) % 4 - ac[axis]) * stride[axis]}

    def line(axis, j):
        return {'dcp': d + (j // 2 - ac[axis]) * stride[axis] + (j % 2 - core)}

    def send(src, dst, ss, rs, dev):
        pltpu.make_async_remote_copy(src_ref=src, dst_ref=dst, send_sem=ss, recv_sem=rs,
                                     device_id=dev, device_id_type=MESH).start()

    def wait(ref, sem):
        pltpu.make_async_copy(ref, ref, sem).wait()

    def ks_of(i):
        return KS if i < NI - 1 else DIRS

    def only(i, f):
        if i < NI - 1:
            f()
        else:
            pl.when(core == 1)(f)

    def by_core(f):
        for c in DIRS:
            pl.when(core == c)(functools.partial(f, c))

    bar = pltpu.get_barrier_semaphore()
    pl.semaphore_signal(bar, inc=1, device_id=partner, device_id_type=MESH)
    for off in (2, 1, 3):
        for a in KS:
            for c2 in DIRS:
                peer = d + ((co[a] + off) % 4 - co[a]) * STRIDE[a] + c2 - core
                pl.semaphore_signal(bar, inc=1, device_id={'dcp': peer}, device_id_type=MESH)
    load_q = pltpu.make_async_copy(q_h, q_in, sem_q)
    load_q.start()
    load_l = pltpu.make_async_copy(lens_h, lens, sem_l)
    load_l.start()

    def cache_rows(i, half):
        n = len(ks_of(i))
        return c_h.at[pl.ds(BASE * half + 3 * i, n)], cbuf.at[pl.ds(3 * i, n), pl.ds(32 * core, 32)]

    def load_rows(i, half):
        src, dst = cache_rows(i, half)
        pltpu.make_async_copy(src, dst, c_r).start()

    for i in range(NI - 1):
        load_rows(i, core)
    pl.when(core == 1)(lambda: load_rows(NI - 1, 1))

    lrow[...] = jnp.zeros_like(lrow)
    fin[...] = jnp.zeros_like(fin)

    @pl.when(core == 0)
    def _():
        for k in DIRS:
            obuf[pl.ds((k * NI + NI - 1) * 16, 16)] = jnp.zeros((16, 8, LAT), BF16)
            r1d[k, NI - 1] = jnp.zeros((3, 4, 8, LAT), BF16)
    load_l.wait()

    def sel(r, c):
        s = 3 * (r % 8) + (r // 8) % 3
        return (c == BASE * (r // 24) + s) & (s < BASE + 2 * (r // 24))

    load_q.wait()
    qp = jnp.dot(_perm(48, 32, sel), q_in[...], preferred_element_type=F32)
    for c in DIRS:
        for k in KS:
            r = 8 * (3 * c + k)
            s1a[c, k] = qp[r:r + 2].astype(BF16)
            s1b[c, k] = qp[r + 2:r + 6].astype(BF16)
    pl.semaphore_wait(bar, 19)

    def place(k):
        return ac[ORDERS[k][0]] * 2 + core

    for part, (src, dst) in enumerate(((s1a, b1a), (s1b, b1b))):
        for k in KS:
            n = ORDERS[k][0]
            j0 = place(k)
            oc = co[n] + co[nxt[n]] - ac[n]
            ost = STRIDE[n] + STRIDE[nxt[n]] - stride[n]
            for off in (2, 1, 3):
                send(src.at[core, k], dst.at[k, j0], s1_s.at[part], s1_r.at[part], ring(n, off))
            for off in (2, 1, 3, 0):
                peer = {'dcp': d + ((oc + off) % 4 - oc) * ost + 1 - 2 * core}
                send(src.at[1 - core, k], dst.at[k, oc * 2 + core], s1_s.at[part], s1_r.at[part], peer)
            dst[k, j0] = src[core, k]

    def push_rows(i, half):
        src, dst = cache_rows(i, half)
        send(src, dst, c_s, c_r, partner)

    for i in range(NI - 1):
        push_rows(i, 1 - core)
    pl.when(core == 0)(lambda: push_rows(NI - 1, 1))

    def q_of(i):
        return q_odd if i % 2 else q_even

    def q_slot(k, i):
        return (k * 3 + i // 2) * 16

    def slot(k, i):
        return (k * NI + i) * 16

    def blk(k, i, off):
        _, a2, a3 = ORDERS[k]
        return q_of(i).at[q_slot(k, i) + ac[a3] * 4 + (ac[a2] - off) % 4]

    def copy3(k, i, off):
        b = blk(k, i, off)
        a3 = ORDERS[k][2]
        for o in (1, 3) if i in RELAYED else (2, 1, 3):
            onward = i in RELAYED and off // 2 == o // 2
            send(b, b, s3_s.at[i % 2], sf_r.at[i - NI + 2] if onward else s3_r.at[i], ring(a3, o))

    def stage2(k, i):
        b = blk(k, i, 0)
        for off in (2, 1, 3):
            send(b, b, s2_s.at[i % 2], s2_r.at[i], ring(ORDERS[k][1], off))
        copy3(k, i, 0)

    def rows2(i):
        for k in ks_of(i):
            stage2(k, i)

    def turn(buf, part, first, n):
        tr = _perm(8 * n, 8 * n, lambda r, c: (r // 8 == c % n) & (r % 8 == c // n))
        wait(buf.at[:, pl.ds(0, 7)], s1_r.at[part])
        ins = [jnp.concatenate([buf[k, j].astype(F32) for j in range(8)], axis=0).astype(BF16) for k in KS]
        outs = [jnp.dot(tr, v, preferred_element_type=F32) for v in ins]
        for k in KS:
            _, a2, a3 = ORDERS[k]
            for i in range(first, min(first + n, COUNT[k])):
                r = 8 * (i - first)
                y = outs[k][r:r + 8, :LAT if i % 2 else QW]
                if i % 2 == 0:
                    y = jnp.concatenate([y, outs[k][r + 8:r + 16, LAT:]], axis=1)
                q_of(i)[q_slot(k, i) + ac[a3] * 4 + ac[a2]] = y.astype(BF16)

    turn(b1a, 0, 0, 2)
    for i in range(2):
        rows2(i)
    turn(b1b, 1, 2, 4)
    for i in ORDER:
        if i > 1:
            only(i, functools.partial(rows2, i))

    def stage3(i):
        n = len(ks_of(i))
        wait(q_of(i).at[pl.ds(0, 3 * n)], s2_r.at[i])
        for off in (1, 3, 2):
            for k in ks_of(i):
                copy3(k, i, off)

    def forward(i):
        wait(q_of(i).at[pl.ds(0, 4 * len(ks_of(i)))], sf_r.at[i - NI + 2])
        for off in RING:
            for k in ks_of(i):
                _, a2, a3 = ORDERS[k]
                o = 1 if off < 2 else 3
                b = q_of(i).at[q_slot(k, i) + ((ac[a3] - o) % 4) * 4 + (ac[a2] - off) % 4]
                send(b, b, s3_s.at[i % 2], s3_r.at[i], ring(a3, o))

    def arrive(i):
        n = len(ks_of(i))
        if i == 0:
            by_core(lambda c: wait(cbuf.at[pl.ds(0, BASE + 2 * c)], c_r))
        wait(q_of(i).at[pl.ds(0, (8 if i in RELAYED else 12) * n)], s3_r.at[i])

    for i in ORDER:
        only(i, functools.partial(stage3, i))

    chip8 = (d // 2) * 16

    j = lax.broadcasted_iota(jnp.int32, (LAT, LANES), 0)
    pos = (j & 7) + ((j >> 3) & 31) * 1024 + (j >> 8) * 8

    def cache_of(k, i):
        return cbuf[3 * i + k].reshape(LAT, QW)

    def scores(k, i):
        cs = cache_of(k, i)
        n = pl.ds(q_slot(k, i), 16)
        lat = q_of(i)[n, :, :LAT].reshape(LANES, LAT)
        rope = q_even[n, :, LAT:].reshape(LANES, LANES)
        rope = rope[:, ROPE:] if i % 2 else rope[:, :ROPE]
        dims = (((1,), (1,)), ((), ()))
        st = lax.dot_general(cs[:, :LAT], lat, dims, preferred_element_type=F32)
        return (st + lax.dot_general(cs[:, LAT:], rope, dims, preferred_element_type=F32)) * SCALE2

    def softmax(st, k, i):
        ok = pos < lens[BASE * core + 3 * i + k] - chip8
        st = jnp.where(ok, st, NEG)
        m = jnp.max(st, axis=0, keepdims=True)
        has = m > NEG
        p = jnp.exp2(st - jnp.where(has, m, 0.0))
        ls = jnp.where(has, jnp.sum(p, axis=0, keepdims=True), 1.0)
        w = wave(i)
        lrow[w, k, i - w * SPLIT] = jnp.where(has, m + jnp.log2(ls), NEG)
        return (p * (1.0 / ls)).astype(BF16)

    def attend(batch):
        sts = [scores(k, i) for k, i in batch]
        ps = [softmax(st, k, i) for st, (k, i) in zip(sts, batch)]
        outs = [lax.dot_general(p, cache_of(k, i)[:, :LAT], (((0,), (0,)), ((), ())), preferred_element_type=F32)
                for p, (k, i) in zip(ps, batch)]
        for o, (k, i) in zip(outs, batch):
            obuf[pl.ds(slot(k, i), 16)] = o.astype(BF16).reshape(16, 8, LAT)

    def wave(i):
        return 0 if i < SPLIT else 1

    def send1(batch):
        for o, (k, i) in [(o, x) for o in (2, 1, 3) for x in batch]:
            a3 = ORDERS[k][2]
            b = obuf.at[pl.ds(slot(k, i) + ((ac[a3] + o) % 4) * 4, 4)]
            send(b, r1d.at[k, i, o - 1], r1_s, r1_r.at[wave(i)], ring(a3, o))

    def members(w, k):
        return range(SPLIT) if w == 0 else range(SPLIT, COUNT[k])

    def count(w):
        return sum(len(members(w, k)) for k in KS)

    def send1_lse(w):
        for k in KS:
            for o in RING_OFFS:
                n = pl.ds(0, TILE[w])
                send(lrow.at[w, k, n], r1l.at[w, k, o - 1, n], r1l_s.at[w], r1l_r.at[w], ring(ORDERS[k][2], o))

    for i in range(NI - 2):
        batch = [(k, i) for k in KS]
        with jax.named_scope(f"arrive{i}"):
            arrive(i)
        with jax.named_scope(f"attend{i}"):
            attend(batch)
        with jax.named_scope(f"rest{i}"):
            if i == 0:
                for x in RELAYED:
                    only(x, functools.partial(forward, x))
            if i == SPLIT - 1:
                send1_lse(0)
            send1(batch)


    @by_core
    def _(c):
        last = range(NI - 2, NI - 1 + c)
        for i in last:
            arrive(i)
        batch = [(k, i) for i in last for k in ks_of(i)]
        attend(batch)
        send1_lse(1)
        send1(batch)


    def columns(ws, k, row, n):
        wcol[k, :, :32] = jnp.concatenate(ws, axis=0).T
        t = wcol[k, pl.ds(row, n), :32]
        return lambda x, i: t[:, 8 * x + i:8 * x + i + 1]

    def weighted(cols, i, parts):
        return functools.reduce(jnp.add, [p.astype(F32) * cols(x, i) for x, p in enumerate(parts)])

    def tile_of(w, ref):
        return jnp.concatenate([ref[i] for i in range(TILE[w])] + [jnp.zeros((8 - TILE[w], LANES), F32)], axis=0)

    def merge1(w):
        cols = []
        n = pl.ds(0, TILE[w])
        wait(r1l.at[w, :, :, n], r1l_r.at[w])
        for k in KS:
            ws, l1 = _merge_weights([tile_of(w, r) for r in [lrow.at[w, k]] + [r1l.at[w, k, x] for x in KS]])
            for i in range(TILE[w]):
                lse1[w, k, i] = l1[i:i + 1]
            cols.append(columns(ws, k, ac[ORDERS[k][2]] * 32, 32))
        for k in KS:
            for o in RING_OFFS:
                send(lse1.at[w, k, n], r2l.at[w, k, o - 1, n], r2l_s.at[w], r2l_r.at[w], ring(ORDERS[k][1], o))
        if w == 0:
            wait(obuf.at[pl.ds(0, 12 * count(w))], r1_r.at[w])
        else:
            by_core(lambda c: wait(obuf.at[pl.ds(0, 12 * (count(1) - 2 + 2 * c))], r1_r.at[w]))
        for k in KS:
            _, a2, a3 = ORDERS[k]
            its = members(w, k)
            for i in its:
                own = obuf[pl.ds(slot(k, i) + ac[a3] * 4, 4)]
                parts = [v.reshape(32, LAT) for v in [own] + [r1d[k, i, x] for x in KS]]
                y = weighted(cols[k], i - its[0], parts).astype(BF16).reshape(4, 8, LAT)
                for p in RING:
                    r1m[k, p, i] = y[p]
            for o in (2, 1, 3):
                sl = pl.ds(its[0], len(its))
                send(r1m.at[k, (ac[a2] + o) % 4, sl], r2d.at[k, o - 1, sl], r2_s, r2_r.at[w], ring(a2, o))

    def merge2(w):
        cols = []
        wait(r2l.at[w, :, :, pl.ds(0, TILE[w])], r2l_r.at[w])
        for k in KS:
            _, a2, a3 = ORDERS[k]
            ws, l2 = _merge_weights([tile_of(w, r) for r in [lse1.at[w, k]] + [r2l.at[w, k, x] for x in KS]])
            g = ac[a3] * 4 + ac[a2]
            lt = pltpu.roll(l2, ((16 - g) % 16) * 8, 1)
            s3l[w, k] = jnp.concatenate([lt] * 16, axis=0).T[0:8].reshape(8, 1, LANES)
            cols.append(columns(ws, k, g * 8, 8))
        for k in KS:
            j0 = place(k)
            for off in LINE_OFFS:
                j = (j0 + off) % 8
                send(s3l.at[w, k, j], r3l.at[w, k, j0], r3l_s, r3l_r.at[w], line(ORDERS[k][0], j))
            r3l[w, k, j0] = s3l[w, k, j0]
        t = TILE[w]
        pms = {n: _perm(8 * t, 8 * n, lambda r, c: (c == (r % t) * 8 + r // t) & (r % t < n))
               for n in sorted({len(members(w, k)) for k in KS})}
        wait(obuf.at[pl.ds(0, 3 * count(w))], r2_r.at[w])
        tiles = []
        for k in KS:
            its = members(w, k)
            ys = [weighted(cols[k], i - its[0], [r1m[k, ac[ORDERS[k][1]], i]] + [r2d[k, x, i] for x in KS]) for i in its]
            n = len(its)
            tiles.append(jnp.dot(pms[n], jnp.concatenate(ys, axis=0).astype(BF16), preferred_element_type=F32))
        for k in KS:
            t, s3, r3 = TILE[w], (s3a, s3b)[w], (r3a, r3b)[w]
            j0 = place(k)
            for j in range(8):
                s3[k, j] = tiles[k][t * j:t * j + t].astype(BF16)
            for off in (3, 4, 5, 2, 6, 1, 7):
                j = (j0 + off) % 8
                send(s3.at[k, j], r3.at[k, j0], r3_s.at[w], r3_r.at[w], line(ORDERS[k][0], j))
            r3[k, j0] = s3[k, j0]

    def merge3(w):
        cols = []
        wait(r3l.at[w, :, pl.ds(0, 7)], r3l_r.at[w])
        for k in KS:
            ls = [r3l[w, k, j] for j in range(8)]
            ws = [None] * 8
            for h in DIRS:
                ws[h::2], _ = _merge_weights(ls[h::2])
            cols.append(jnp.concatenate(ws, axis=0).T[0:8])
        t, r3 = TILE[w], (r3a, r3b)[w]
        wait(r3.at[:, pl.ds(0, 7)], r3_r.at[w])
        for k in KS:
            for h in DIRS:
                ts = [r3[k, j].astype(F32) * cols[k][:t, j:j + 1] for j in range(h, 8, 2)]
                fin[w, h, k, :t] = functools.reduce(jnp.add, ts)

    merge1(0)
    merge1(1)
    merge2(0)
    wait(b1a.at[:, pl.ds(0, 7)], s1_s.at[0])
    wait(b1b.at[:, pl.ds(0, 7)], s1_s.at[1])

    @by_core
    def _(c):
        wait(cbuf.at[pl.ds(0, BASE + 2 * (1 - c)), pl.ds(0, 32)], c_s)
        for par in DIRS:
            its = [i for i in range(NI - 1 + c) for _ in ks_of(i) if i % 2 == par]
            wait(q_of(par).at[pl.ds(0, 3 * len(its))], s2_s.at[par])
            wait(q_of(par).at[pl.ds(0, 12 * len(its))], s3_s.at[par])

    merge2(1)
    merge3(0)
    by_core(lambda c: wait(obuf.at[pl.ds(0, 12 * (BASE + 2 * c))], r1_s))
    for w in DIRS:
        n = pl.ds(0, TILE[w])
        wait(r1l.at[w, :, :, n], r1l_s.at[w])
        wait(r2l.at[w, :, :, n], r2l_s.at[w])
    wait(obuf.at[pl.ds(0, 51)], r2_s)
    def pick(r, c):
        w, h, k, i = c // 48, (c // 24) % 2, (c // 8) % 3, c % 8
        s = 3 * (i + w * SPLIT) + k
        return (r == BASE * h + s) & (s < BASE + 2 * h) & (i < SPLIT)

    pm = _perm(32, 96, pick)
    merge3(1)
    flat = fin[...].reshape(96, LAT).astype(BF16)

    o_ref[...] = jnp.dot(pm, flat, preferred_element_type=F32).astype(BF16)

    wait(r3a.at[:, pl.ds(0, 7)], r3_s.at[0])
    wait(r3b.at[:, pl.ds(0, 7)], r3_s.at[1])
    wait(r3l.at[:, :, pl.ds(0, 7)], r3l_s)


def solution(mesh):
    def local(q, cache, lens):
        dma = pltpu.SemaphoreType.DMA
        V = pltpu.VMEM
        anyspace = pl.BlockSpec(memory_space=pl.ANY)
        tile, qtile = (8, LAT), (8, QW)
        line = (2, 3, 8)
        scratch = [
            pltpu.SMEM((32,), jnp.int32), V((32, QW), BF16), V((2, 3, 2, QW), BF16), V((2, 3, 4, QW), BF16), V((3, 8, 2, QW), BF16), V((3, 8, 4, QW), BF16),
            V((144, 8, LAT + LANES), BF16), V((144,) + tile, BF16),
            V((BASE + 2, 64) + qtile, BF16), V((288,) + tile, BF16), V((2, 3, SPLIT, 1, LANES), F32), V((3, LANES, LANES), F32),
            V((3, NI, 3, 4) + tile, BF16), V((2, 3, 3, SPLIT, 1, LANES), F32), V((3, 4, NI) + tile, BF16), V((2, 3, SPLIT, 1, LANES), F32),
            V((3, 3, NI) + tile, BF16), V((2, 3, 3, SPLIT, 1, LANES), F32),
            V((3, 8, TILE[0], LAT), BF16), V((3, 8, TILE[1], LAT), BF16), V(line + (1, LANES), F32),
            V((3, 8, TILE[0], LAT), BF16), V((3, 8, TILE[1], LAT), BF16), V(line + (1, LANES), F32),
            V((2, 2, 3) + tile, F32),
            dma, dma, dma, dma, dma((2,)), dma((2,)), dma((2,)), dma((NI,)), dma((2,)), dma((NI,)), dma((2,)),
            dma, dma((2,)), dma((2,)), dma((2,)), dma, dma((2,)), dma((2,)), dma((2,)), dma((2,)), dma((2,)), dma, dma((2,)),
        ]
        o = pl.pallas_call(
            _kernel,
            out_shape=V((32, LAT), BF16),
            in_specs=[anyspace] * 3,
            out_specs=pl.BlockSpec(memory_space=V),
            scratch_shapes=scratch,
            compiler_params=pltpu.CompilerParams(collective_id=0, has_side_effects=True,
                                                 vmem_limit_bytes=50 * 2 ** 20),
        )(*[pltpu.with_memory_space_constraint(v, pltpu.HBM) for v in (lens, q.reshape(32, QW), cache.reshape(32, 32, 8, QW))])
        return o.reshape(32, 1, LAT)

    return jax.shard_map(local, mesh=mesh,
                         in_specs=(P('dp', 'dcp', None), P('dp', None, 'dcp', None, None), P('dp')),
                         out_specs=P('dp', 'dcp', None), check_vma=False)
```
